32 devices in a mesh: dp: 8 (over z, y), seq: 4 (over x, core).
Axes of the slice: x: 2, y: 2, z: 4, core: 2. Of those that a mesh axis runs over, the one named last changes fastest.
Arguments:
- activations: bfloat16 [160, 4, 49, 512], P(('dp', 'seq')), may hold values from -6 to 6
- counts: int32 [8], P('dp'), may hold values from 10 to 20, as said below
- w_qkv: bfloat16 [2, 512, 3, 512], P(None, 'dp', None, 'seq'), may hold values from -0.25 to 0.25
- w_out: bfloat16 [2, 512, 512], P(None, 'seq', 'dp'), may hold values from -0.75 to 0.75
- w_up: bfloat16 [2, 512, 2048], P(None, 'dp', 'seq'), may hold values from -0.25 to 0.25
- w_down: bfloat16 [2, 2048, 512], P(None, 'seq', 'dp'), may hold values from -0.125 to 0.125
- qv_bias: float32 [2, 2, 512], P(None, None, 'seq'), may hold values from -3 to 3
- rel_table: float32 [2, 169, 16], P(None, None, 'seq'), may hold values from -4 to 4
- up_bias: bfloat16 [2, 2048], P(None, 'seq'), may hold values from -3 to 3
- norm_gain: float32 [2, 2, 512], replicated, may hold values from 0.5 to 1.5
- norm_bias: float32 [2, 2, 512], replicated, may hold values from -2 to 2
- out_bias: float32 [2, 2, 512], replicated, may hold values from -2 to 2
- cotangent: bfloat16 [160, 4, 49, 512], P(('dp', 'seq')), may hold values from -6 to 6
Outputs:
- out: bfloat16 [160, 4, 49, 512], P(('dp', 'seq'))
- grad_input: float32 [160, 4, 49, 512], P(('dp', 'seq'))
- grad_w_qkv: float32 [2, 512, 3, 512], P(None, 'dp', None, 'seq')
- grad_w_out: float32 [2, 512, 512], P(None, 'seq', 'dp')
- grad_w_up: float32 [2, 512, 2048], P(None, 'dp', 'seq')
- grad_w_down: float32 [2, 2048, 512], P(None, 'seq', 'dp')
- grad_qv_bias: float32 [2, 2, 512], P(None, None, 'seq')
- grad_rel_table: float32 [2, 169, 16], P(None, None, 'seq')
- grad_up_bias: float32 [2, 2048], P(None, 'seq')
- grad_norm_gain: float32 [2, 2, 512], replicated
- grad_norm_bias: float32 [2, 2, 512], replicated
- grad_out_bias: float32 [2, 2, 512], replicated
The draws below stay inside these ranges and needn't reach their ends.
Inputs may be any that keep to these rules, and one draw needn't show every extreme that they name: Index i of dp holds images in its first counts[i] slots and none in the rest; one index is full and another holds 10.
All inputs are finite; a program needn't handle non-finite values.
Results may differ from the reference program's by a relative error of at most 0.028.
Values may be sent and summed in bfloat16 or wider, within the bound.
A program may use at most 256 MiB of HBM per device.

```python
import jax
import jax.numpy as jnp
from jax import lax

D = 512
HEADS = 16
FF = 2048
LAYERS = 2
CAP = 20
GROUPS = 8
SLOTS = 160


def draw_counts(key, part):
    spread_key, filled_key, halved_key = jax.random.split(key, 3)
    picked = jax.random.randint(spread_key, (GROUPS,), CAP // 2, CAP + 1)
    filled = jax.random.randint(filled_key, (), 0, GROUPS)
    halved = (filled + 1 + jax.random.randint(halved_key, (), 0, GROUPS - 1)) % GROUPS
    indices = jnp.arange(GROUPS)
    picked = jnp.where(indices == filled, CAP, picked)
    picked = jnp.where(indices == halved, CAP // 2, picked)
    return picked.astype(jnp.int32)


def raised(values, stream_key, source, target, blocks, factor):
    owner, partner = [(jnp.arange(values.shape[axis_at]) // (values.shape[axis_at] // blocks)).reshape([-1 if axis == axis_at else 1 for axis in range(values.ndim)]) for axis_at in (source, target)]
    chosen = jax.random.permutation(stream_key, blocks)[partner]
    strong = (owner == chosen) | (owner == (partner + blocks // 2) % blocks)
    return jnp.where(strong, factor * values, values)


def level_of(rng, dims, cuts, least, top_value):
    def one(dim, parts):
        steps = jax.random.uniform(jax.random.fold_in(jax.random.fold_in(rng, 6), dim), (parts,), jnp.float32, least / len(cuts), top_value / len(cuts))
        return jnp.repeat(jnp.exp(steps), dims[dim] // parts).reshape((-1,) + (1,) * (len(dims) - dim - 1))

    level = one(*cuts[0])
    for cut in cuts[1:]:
        level = level * one(*cut)
    return level


def scatter_about(rng, extent, width, reach, cuts=(), dtype=jnp.bfloat16):
    drawn = width * jax.random.normal(rng, extent, jnp.float32)
    if cuts:
        drawn = drawn * level_of(rng, extent, cuts, -0.22, 0.18)
    return jnp.clip(drawn, -reach, reach).astype(dtype)


def heavy_noise(stream_key, shape, width, most, cuts, heavy, kind=jnp.bfloat16):
    values = width * jax.random.normal(stream_key, shape, jnp.float32)
    if cuts:
        values = values * level_of(stream_key, shape, cuts, -0.22, 0.18)
    return jnp.clip(raised(values, jax.random.fold_in(stream_key, 3), *heavy), -most, most).astype(kind)


def setup_inputs(seed: int = 0) -> dict:
    streams_of = jax.random.split(jax.random.key(seed), 14)
    return {
        "activations": scatter_about(streams_of[0], (SLOTS, 4, 49, D), 1.0, 6.0, ((0, 32),)),
        "counts": draw_counts(jax.random.fold_in(streams_of[13], 71), 0),
        "w_qkv": scatter_about(streams_of[2], (LAYERS, D, 3, D), D ** -0.5, 0.25, ((1, 8), (3, 4))),
        "w_out": scatter_about(streams_of[3], (LAYERS, D, D), (D // 8) ** -0.5, 0.75, ((1, 4), (2, 8))),
        "w_up": scatter_about(streams_of[4], (LAYERS, D, FF), D ** -0.5, 0.25, ((1, 8), (2, 4))),
        "w_down": scatter_about(streams_of[5], (LAYERS, FF, D), FF ** -0.5, 0.125, ((1, 4), (2, 8))),
        "qv_bias": scatter_about(streams_of[6], (LAYERS, 2, D), 0.5, 3.0, ((2, 4),), jnp.float32),
        "rel_table": scatter_about(streams_of[7], (LAYERS, 169, HEADS), 1.0, 4.0, ((2, 4),), jnp.float32),
        "up_bias": scatter_about(streams_of[8], (LAYERS, FF), 0.5, 3.0, ((1, 4),)),
        "norm_gain": jnp.clip(1.0 + 0.1 * jax.random.normal(streams_of[9], (LAYERS, 2, D), jnp.float32), 0.5, 1.5),
        "norm_bias": scatter_about(streams_of[10], (LAYERS, 2, D), 0.3, 2.0, (), jnp.float32),
        "out_bias": scatter_about(streams_of[11], (LAYERS, 2, D), 0.3, 2.0, (), jnp.float32),
        "cotangent": heavy_noise(streams_of[12], (SLOTS, 4, 49, D), 1.0, 6.0, ((0, 32),), (0, 3, 32, 2.75)),
    }


@jax.custom_vjp
def low(v):
    return lax.optimization_barrier(v.astype(jnp.bfloat16)).astype(jnp.float32)

@jax.custom_vjp
def low_back(v):
    return v

def low_keep(v):
    return (low(v), None)

def low_pass(kept, grad):
    return (grad,)

def back_keep(v):
    return (v, None)

def back_low(kept, grad):
    return (low(grad),)
low.defvjp(low_keep, low_pass)
low_back.defvjp(back_keep, back_low)
highest = lax.Precision.HIGHEST

def window_tables():
    places = jnp.arange(49)
    pos_row = places // 7
    pos_col = places % 7
    relative = (pos_row[:, None] - pos_row[None, :] + 6) * 13 + (pos_col[:, None] - pos_col[None, :] + 6)
    frames = jnp.arange(4)
    image_row = frames[:, None] // 2 * 7 + pos_row[None, :]
    image_col = frames[:, None] % 2 * 7 + pos_col[None, :]
    band_row = (image_row >= 7).astype(jnp.int32) + (image_row >= 11).astype(jnp.int32)
    band_col = (image_col >= 7).astype(jnp.int32) + (image_col >= 11).astype(jnp.int32)
    region = band_row * 3 + band_col
    shifted_mask = jnp.where(region[:, :, None] == region[:, None, :], 0.0, -100.0).astype(jnp.float32)
    return (relative, shifted_mask)

def to_image(tensor):
    leading, channels = (tensor.shape[0], tensor.shape[-1])
    return tensor.reshape(leading, 2, 2, 7, 7, channels).transpose(0, 1, 3, 2, 4, 5).reshape(leading, 14, 14, channels)

def to_windows(tensor):
    leading, channels = (tensor.shape[0], tensor.shape[-1])
    return tensor.reshape(leading, 2, 7, 2, 7, channels).transpose(0, 1, 3, 2, 4, 5).reshape(leading, 4, 49, channels)

def roll_tokens(tensor, offset):
    return to_windows(jnp.roll(to_image(tensor), offset, axis=(1, 2)))

def layer_norm(residual, gain_row, shift_bias):
    centered = residual - lax.optimization_barrier(jnp.mean(residual, -1, keepdims=True))
    spread = lax.optimization_barrier(jnp.mean(centered * centered, -1, keepdims=True))
    return centered * lax.rsqrt(spread + 1e-05) * gain_row + shift_bias

def attention(normed, w_query, w_proj, query_value_bias, bias_table, shifted, relative, shifted_mask):
    leading = normed.shape[0]
    head_count = bias_table.shape[1]
    if shifted:
        normed = roll_tokens(normed, -3)
    projected = jnp.einsum('cwpd,dtf->cwptf', normed, w_query, precision=highest)
    queries = low_back(low(projected[:, :, :, 0] + query_value_bias[0])).reshape(leading, 4, 49, head_count, -1)
    key_heads = low_back(low(projected[:, :, :, 1])).reshape(leading, 4, 49, head_count, -1)
    values = low_back(low(projected[:, :, :, 2] + query_value_bias[1])).reshape(leading, 4, 49, head_count, -1)
    head_size = queries.shape[-1]
    bias_heads = jnp.transpose(bias_table[relative], (2, 0, 1))
    scores = jnp.einsum('cwqhe,cwkhe->cwhqk', queries, key_heads, precision=highest) * head_size ** (-0.5) + bias_heads
    if shifted:
        scores = scores + shifted_mask[None, :, None]
    scores = low_back(scores)
    soft_probs = low(jax.nn.softmax(scores, axis=-1))
    attended = jnp.einsum('cwhqk,cwkhe->cwqhe', soft_probs, values, precision=highest).reshape(leading, 4, 49, -1)
    attended = low_back(low(attended))
    if shifted:
        attended = roll_tokens(attended, 3)
    return low_back(jnp.einsum('cwpe,ef->cwpf', attended, w_proj, precision=highest))

def block_forward(params, residual):
    w_qkv, w_out, w_up, w_down, qv_bias, rel_table, up_bias, norm_gain, norm_bias, out_bias = params
    relative, shifted_mask = window_tables()
    for layer_at in range(LAYERS):
        shifted = layer_at % 2 == 1
        normed = low(layer_norm(residual, norm_gain[layer_at, 0], norm_bias[layer_at, 0]))
        branch = attention(normed, w_qkv[layer_at], w_out[layer_at], qv_bias[layer_at], rel_table[layer_at], shifted, relative, shifted_mask)
        middle = residual + branch + out_bias[layer_at, 0]
        normed_two = low(layer_norm(middle, norm_gain[layer_at, 1], norm_bias[layer_at, 1]))
        preact = low_back(jnp.einsum('cwpd,df->cwpf', normed_two, w_up[layer_at], precision=highest) + up_bias[layer_at])
        hidden = low(jax.nn.gelu(preact, approximate=False))
        down_out = low_back(jnp.einsum('cwpf,fd->cwpd', hidden, w_down[layer_at], precision=highest))
        residual = middle + down_out + out_bias[layer_at, 1]
    return residual

def reference(activations, counts, w_qkv, w_out, w_up, w_down, qv_bias, rel_table, up_bias, norm_gain, norm_bias, out_bias, cotangent):
    params = tuple((member.astype(jnp.float32) for member in (w_qkv, w_out, w_up, w_down, qv_bias, rel_table, up_bias, norm_gain, norm_bias, out_bias)))
    groups = counts.shape[0]
    capacity = activations.shape[0] // groups
    inputs = activations.astype(jnp.float32).reshape(groups, capacity, 4, 49, -1)
    live_rows = (jnp.arange(capacity)[None, :] < counts[:, None]).astype(jnp.float32)[:, :, None, None, None]

    def forward(weights, images):
        block_step = jax.checkpoint(lambda image_block: block_forward(weights, image_block))
        return lax.map(block_step, images) * live_rows
    result, pullback = jax.vjp(forward, params, inputs)
    param_grads, grad_inputs = pullback(cotangent.astype(jnp.float32).reshape(inputs.shape))
    return (result.reshape(activations.shape).astype(jnp.bfloat16), grad_inputs.reshape(activations.shape), param_grads[0], param_grads[1], param_grads[2], param_grads[3], param_grads[4], param_grads[5], param_grads[6], param_grads[7], param_grads[8], param_grads[9])
```

```python
import functools

import jax
import jax.numpy as jnp
import numpy as np
from jax import lax
from jax.experimental import pallas as pl
from jax.experimental.pallas import tpu as pltpu
from jax.sharding import PartitionSpec as P

EPS = 1e-05
F32 = jnp.float32
BF16 = jnp.bfloat16
SIDE = 7
GRID = 14
PLACES = 49
WINDOWS = 4
TOKENS = PLACES * WINDOWS
ROWS = 208
KEYS = 64
PADDED = WINDOWS * KEYS
HEAD = 32
LANES = 128
PER_GROUP = LANES // HEAD
WIDE = PER_GROUP * KEYS
BLOCK = 3 * LANES
SCALE = HEAD**-0.5


def place_tables(shift):
    perm = np.zeros((PADDED, ROWS), np.float32)
    region = np.zeros((WINDOWS, PLACES), np.int64)
    for w in range(WINDOWS):
        for p in range(PLACES):
            row, col = SIDE * (w // 2) + p // SIDE, SIDE * (w % 2) + p % SIDE
            band = [int(v >= 7) + int(v >= 11) for v in (row, col)]
            region[w, p] = 3 * band[0] + band[1]
            row, col = (row + shift) % GRID, (col + shift) % GRID
            source_w = 2 * (row // SIDE) + col // SIDE
            source_p = SIDE * (row % SIDE) + col % SIDE
            perm[KEYS * w + p, WINDOWS * source_p + source_w] = 1.0
    mask = np.zeros((WINDOWS, KEYS, KEYS), np.float32)
    if shift:
        mask[:, :PLACES, :PLACES] = np.where(region[:, :, None] == region[:, None, :], 0.0, -100.0)
    mask[:, PLACES:, :] = -1e30
    return perm, np.tile(mask, (1, 1, PER_GROUP))


def place_onehot():
    onehot = np.zeros((KEYS, KEYS, 169), np.float32)
    for k in range(PLACES):
        for q in range(PLACES):
            rel = (q // 7 - k // 7 + 6) * 13 + (q % 7 - k % 7 + 6)
            onehot[k, q, rel] = 1.0
    return onehot.reshape(KEYS * KEYS, 169)


def nn(a, b):
    return lax.dot_general(a, b, (((1,), (0,)), ((), ())), preferred_element_type=F32)


def nt(a, b):
    return lax.dot_general(a, b, (((1,), (1,)), ((), ())), preferred_element_type=F32)


def tn(a, b):
    return lax.dot_general(a, b, (((0,), (0,)), ((), ())), preferred_element_type=F32)


def row_mean(value):
    return jnp.sum(value, axis=-1, keepdims=True) * (1.0 / value.shape[-1])


def normalize(value):
    centered = value - row_mean(value)
    inverse = lax.rsqrt(row_mean(centered * centered) + EPS)
    return centered * inverse, inverse


def spread_heads(tile):
    head = lax.broadcasted_iota(jnp.int32, tile.shape, 1) // HEAD
    zero = jnp.zeros_like(tile)
    return jnp.concatenate([jnp.where(head == h, tile, zero) for h in range(PER_GROUP)], axis=0)


def join_heads(wide):
    head = lax.broadcasted_iota(jnp.int32, (KEYS, LANES), 1) // HEAD
    total = wide[:KEYS]
    for h in range(1, PER_GROUP):
        total = jnp.where(head == h, wide[KEYS * h : KEYS * (h + 1)], total)
    return total


def cols(at, size):
    return pl.ds(pl.multiple_of(at, LANES), size)


def forward_kernel(
    last,
    live_ref,
    x_ref,
    wq_ref,
    wo_ref,
    wu_ref,
    wd_ref,
    bias_ref,
    mask_ref,
    perm_ref,
    back_ref,
    qvb_ref,
    upb_ref,
    gain_ref,
    shift_ref,
    outb_ref,
    out_ref,
    xhat1_ref,
    inv1_ref,
    normed1_ref,
    qkv_ref,
    lse_ref,
    att_ref,
    xhat2_ref,
    inv2_ref,
    normed2_ref,
    hid_ref,
    slope_ref,
    pad_ref,
):
    groups = wo_ref.shape[1] // LANES
    x = x_ref[0].astype(F32)
    xhat, inverse = normalize(x)
    xhat1_ref[0] = xhat.astype(BF16)
    inv1_ref[0] = jnp.broadcast_to(inverse, (ROWS, LANES))
    normed = (xhat * gain_ref[0:1] + shift_ref[0:1]).astype(BF16)
    normed1_ref[0] = normed
    rolled = nn(perm_ref[...], normed).astype(BF16)
    qkv_ref[0] = (nn(rolled, wq_ref[...]) + qvb_ref[...]).astype(BF16)

    def attend(g, carry):
        bias = bias_ref[g]
        for w in range(WINDOWS):
            rows = slice(KEYS * w, KEYS * (w + 1))
            query = qkv_ref[0, rows, cols(BLOCK * g, LANES)]
            key = qkv_ref[0, rows, cols(BLOCK * g + LANES, LANES)]
            val = qkv_ref[0, rows, cols(BLOCK * g + 2 * LANES, LANES)]
            scores = nt(key, spread_heads(query)) * SCALE + bias + mask_ref[w]
            top = jnp.max(scores, axis=0, keepdims=True)
            expo = jnp.exp(scores - top)
            total = jnp.sum(expo, axis=0, keepdims=True)
            probs = (expo * (1.0 / total)).astype(BF16)
            lse_ref[0, pl.ds(WINDOWS * g + w, 1), :] = top + jnp.log(total)
            pad_ref[rows, cols(LANES * g, LANES)] = join_heads(tn(probs, val)).astype(BF16)
        return carry

    lax.fori_loop(0, groups, attend, 0)
    attended = nn(back_ref[...], pad_ref[...]).astype(BF16)
    att_ref[0] = attended
    middle = x + nt(attended, wo_ref[...]) + outb_ref[0:1]
    xhat, inverse = normalize(middle)
    xhat2_ref[0] = xhat.astype(BF16)
    inv2_ref[0] = jnp.broadcast_to(inverse, (ROWS, LANES))
    normed = (xhat * gain_ref[1:2] + shift_ref[1:2]).astype(BF16)
    normed2_ref[0] = normed
    total = middle + outb_ref[1:2]
    step = 512
    for c in range(wu_ref.shape[1] // step):
        at = slice(step * c, step * (c + 1))
        pre = nn(normed, wu_ref[:, at]) + upb_ref[:, at]
        half = 0.5 * (1.0 + lax.erf(pre * 0.7071067811865476))
        hidden = (pre * half).astype(BF16)
        hid_ref[0, :, at] = hidden
        slope_ref[0, :, at] = (half + pre * jnp.exp(-0.5 * pre * pre) * 0.3989422804014327).astype(BF16)
        total = total + nt(hidden, wd_ref[:, at])
    if last:
        total = total * live_ref[pl.program_id(0)]
    out_ref[0] = total.astype(out_ref.dtype)


def norm_back(grad, xhat, inverse, gain):
    scaled = grad * gain
    first = row_mean(scaled)
    second = row_mean(scaled * xhat)
    return inverse * (scaled - first - xhat * second)


def add_rows(ref, row, value):
    ref[row : row + 1, : value.shape[1]] += jnp.sum(value, axis=0, keepdims=True)


def backward_kernel(
    first,
    live_ref,
    g_ref,
    wq_ref,
    wo_ref,
    wu_ref,
    wd_ref,
    bias_ref,
    mask_ref,
    perm_ref,
    back_ref,
    gain_ref,
    xhat1_ref,
    inv1_ref,
    qkv_ref,
    lse_ref,
    xhat2_ref,
    inv2_ref,
    slope_ref,
    gout_ref,
    gm_ref,
    gpre_ref,
    gp_ref,
    gqkv_ref,
    table_ref,
    small_ref,
    gap_ref,
    gpad_ref,
):
    groups = wo_ref.shape[1] // LANES

    @pl.when(pl.program_id(0) == 0)
    def _():
        table_ref[...] = jnp.zeros_like(table_ref)
        small_ref[...] = jnp.zeros_like(small_ref)

    g_res = g_ref[0].astype(F32)
    if first:
        g_res = g_res * live_ref[pl.program_id(0)]
    width = g_res.shape[1]
    add_rows(small_ref, 5, g_res)
    g_m = g_res.astype(BF16)
    gm_ref[0] = g_m
    g_n2 = jnp.zeros_like(g_res)
    step = 512
    for c in range(wu_ref.shape[1] // step):
        at = slice(step * c, step * (c + 1))
        g_pre = (nn(g_m, wd_ref[:, at]) * slope_ref[0, :, at].astype(F32)).astype(BF16)
        gpre_ref[0, :, at] = g_pre
        small_ref[6:7, at] += jnp.sum(g_pre.astype(F32), axis=0, keepdims=True)
        g_n2 = g_n2 + nt(g_pre, wu_ref[:, at])
    xhat = xhat2_ref[0].astype(F32)
    add_rows(small_ref, 2, g_n2 * xhat)
    add_rows(small_ref, 3, g_n2)
    g_mid = g_res + norm_back(g_n2, xhat, inv2_ref[0, :, 0:1], gain_ref[1:2])
    add_rows(small_ref, 4, g_mid)
    g_p = g_mid.astype(BF16)
    gp_ref[0] = g_p
    g_att = nn(g_p, wo_ref[...]).astype(BF16)
    gap_ref[...] = nn(perm_ref[...], g_att).astype(BF16)

    def attend(g, carry):
        bias = bias_ref[g]
        for w in range(WINDOWS):
            rows = slice(KEYS * w, KEYS * (w + 1))
            query = spread_heads(qkv_ref[0, rows, cols(BLOCK * g, LANES)])
            key = qkv_ref[0, rows, cols(BLOCK * g + LANES, LANES)]
            val = qkv_ref[0, rows, cols(BLOCK * g + 2 * LANES, LANES)]
            grad = spread_heads(gap_ref[rows, cols(LANES * g, LANES)])
            scores = nt(key, query) * SCALE + bias + mask_ref[w]
            probs = jnp.exp(scores - lse_ref[0, pl.ds(WINDOWS * g + w, 1), :])
            g_probs = nt(val, grad)
            g_vals = nn(probs.astype(BF16), grad)
            mean = jnp.sum(g_probs * probs, axis=0, keepdims=True)
            g_scores = (probs * (g_probs - mean)).astype(BF16)
            table_ref[g] += g_scores.astype(F32)
            g_keys = nn(g_scores, query) * SCALE
            g_queries = join_heads(tn(g_scores, key)) * SCALE
            gpad_ref[rows, cols(BLOCK * g, LANES)] = g_queries.astype(BF16)
            gpad_ref[rows, cols(BLOCK * g + LANES, LANES)] = g_keys.astype(BF16)
            gpad_ref[rows, cols(BLOCK * g + 2 * LANES, LANES)] = g_vals.astype(BF16)
        return carry

    lax.fori_loop(0, groups, attend, 0)
    g_qkv = nn(back_ref[...], gpad_ref[...]).astype(BF16)
    gqkv_ref[0] = g_qkv
    add_rows(small_ref, 7, g_qkv.astype(F32))
    g_n1 = nt(g_qkv, wq_ref[...])
    xhat = xhat1_ref[0].astype(F32)
    add_rows(small_ref, 0, g_n1 * xhat)
    add_rows(small_ref, 1, g_n1)
    gout_ref[0] = g_mid + norm_back(g_n1, xhat, inv1_ref[0, :, 0:1], gain_ref[0:1])


def whole(array):
    zeros = (0,) * array.ndim
    return pl.BlockSpec(array.shape, lambda i: zeros, pipeline_mode=pl.Buffered(1))


def per_image(shape):
    tail = (0,) * (len(shape) - 1)
    return pl.BlockSpec((1,) + tuple(shape[1:]), lambda i: (i,) + tail)


def fixed(shape):
    zeros = (0,) * len(shape)
    return pl.BlockSpec(shape, lambda i: zeros)


SMEM = pl.BlockSpec(memory_space=pltpu.SMEM)
PARAMS = pltpu.CompilerParams(dimension_semantics=("arbitrary",), vmem_limit_bytes=60000 * 1024)


def forward_layer(last, live, x, weights, tables, rows):
    images = x.shape[0]
    width, units = weights[0].shape[0], weights[2].shape[1]
    total = weights[0].shape[1]
    groups = width // LANES
    shapes = [
        ((images, ROWS, width), BF16 if last else F32),
        ((images, ROWS, width), BF16),
        ((images, ROWS, LANES), F32),
        ((images, ROWS, width), BF16),
        ((images, PADDED, total), BF16),
        ((images, groups * WINDOWS, WIDE), F32),
        ((images, ROWS, width), BF16),
        ((images, ROWS, width), BF16),
        ((images, ROWS, LANES), F32),
        ((images, ROWS, width), BF16),
        ((images, ROWS, units), BF16),
        ((images, ROWS, units), BF16),
    ]
    fixed_args = (*weights, *tables, *rows)
    return pl.pallas_call(
        functools.partial(forward_kernel, last),
        grid=(images,),
        in_specs=[SMEM, per_image(x.shape)] + [whole(a) for a in fixed_args],
        out_specs=[per_image(s) for s, _ in shapes],
        out_shape=[jax.ShapeDtypeStruct(s, d) for s, d in shapes],
        scratch_shapes=[pltpu.VMEM((PADDED, width), BF16)],
        compiler_params=PARAMS,
        name="forward_layer",
    )(live, x, *fixed_args)


def backward_layer(first, live, g, weights, tables, gain, saved):
    images = g.shape[0]
    width, units = weights[0].shape[0], weights[2].shape[1]
    total = weights[0].shape[1]
    groups = width // LANES
    shapes = [
        ((images, ROWS, width), F32),
        ((images, ROWS, width), BF16),
        ((images, ROWS, units), BF16),
        ((images, ROWS, width), BF16),
        ((images, ROWS, total), BF16),
    ]
    sums = [((groups, KEYS, WIDE), F32), ((8, units), F32)]
    fixed_args = (*weights, *tables, gain)
    return pl.pallas_call(
        functools.partial(backward_kernel, first),
        grid=(images,),
        in_specs=[SMEM, per_image(g.shape)]
        + [whole(a) for a in fixed_args]
        + [per_image(a.shape) for a in saved],
        out_specs=[per_image(s) for s, _ in shapes] + [fixed(s) for s, _ in sums],
        out_shape=[jax.ShapeDtypeStruct(s, d) for s, d in shapes + sums],
        scratch_shapes=[pltpu.VMEM((PADDED, width), BF16), pltpu.VMEM((PADDED, total), BF16)],
        compiler_params=PARAMS,
        name="backward_layer",
    )(live, g, *fixed_args, *saved)


def to_rows(images):
    slots, width = images.shape[0], images.shape[3]
    flat = jnp.transpose(images, (0, 2, 1, 3)).reshape(slots, TOKENS, width)
    return jnp.pad(flat, ((0, 0), (0, ROWS - TOKENS), (0, 0)))


def from_rows(rows):
    slots, width = rows.shape[0], rows.shape[2]
    return jnp.transpose(rows[:, :TOKENS].reshape(slots, PLACES, WINDOWS, width), (0, 2, 1, 3))


def split_packed(packed, width, hidden):
    bounds = (0, 3 * width, 4 * width, 4 * width + hidden, 4 * width + 2 * hidden)
    return tuple(packed[..., a:b] for a, b in zip(bounds[:-1], bounds[1:]))


def local(
    activations,
    counts,
    w_qkv,
    w_out,
    w_up,
    w_down,
    qv_bias,
    rel_table,
    up_bias,
    norm_gain,
    norm_bias,
    out_bias,
    cotangent,
):
    slots, width = activations.shape[0], activations.shape[3]
    layers = w_qkv.shape[0]
    shares = lax.axis_size("seq")
    seq = lax.axis_index("seq")
    local_width, local_units = w_qkv.shape[3], w_up.shape[2]
    live = (seq * slots + jnp.arange(slots) < counts[0]).astype(F32)
    onehot = jnp.asarray(place_onehot())

    pieces = [qv_bias.reshape(-1), jnp.transpose(rel_table, (0, 2, 1)).reshape(-1), up_bias.astype(F32).reshape(-1)]
    small = lax.all_gather(jnp.concatenate(pieces), "seq")
    at = np.cumsum([0] + [p.shape[0] for p in pieces])
    all_qv = small[:, at[0] : at[1]].reshape(shares, layers, 2, local_width)
    all_table = small[:, at[1] : at[2]].reshape(shares, layers, -1, 169)
    all_up = small[:, at[2] : at[3]].reshape(shares, layers, local_units)

    packed = jnp.concatenate(
        [
            w_qkv.reshape(layers, -1, 3 * local_width),
            jnp.transpose(w_out, (0, 2, 1)),
            w_up,
            jnp.transpose(w_down, (0, 2, 1)),
        ],
        axis=2,
    )
    weights, tables, rows = [], [], []
    for layer in range(layers):
        full = lax.all_gather(packed[layer], ("seq", "dp"), axis=0, tiled=True).reshape(shares, width, -1)
        parts = split_packed(full, local_width, local_units)
        weights.append(tuple(jnp.transpose(p, (1, 0, 2)).reshape(width, -1) for p in parts))
        perm, mask = place_tables(3 if layer % 2 == 1 else 0)
        lookup = jnp.dot(
            onehot, all_table[:, layer].reshape(-1, 169).T, precision=lax.Precision.HIGHEST
        ).reshape(KEYS, KEYS, -1, PER_GROUP)
        bias = jnp.transpose(lookup, (2, 0, 3, 1)).reshape(-1, KEYS, WIDE)
        tables.append((bias, jnp.asarray(mask), jnp.asarray(perm, BF16), jnp.asarray(perm.T, BF16)))
        qv = all_qv[:, layer]
        qvb = jnp.stack([qv[:, 0], jnp.zeros_like(qv[:, 0]), qv[:, 1]], axis=1).reshape(1, -1)
        upb = all_up[:, layer].reshape(1, -1)
        rows.append((qvb, upb, norm_gain[layer], norm_bias[layer], out_bias[layer]))

    residual = to_rows(activations)
    saved = []
    for layer in range(layers):
        residual, *kept = forward_layer(
            layer == layers - 1, live, residual, weights[layer], tables[layer], rows[layer]
        )
        saved.append(kept)
    out = from_rows(residual)

    grad = to_rows(cotangent)
    grad_weights, sums = [None] * layers, [None] * layers
    for layer in reversed(range(layers)):
        xhat1, inv1, normed1, qkv, lse, att, xhat2, inv2, normed2, hid, slope = saved[layer]
        grad, g_m, g_pre, g_p, g_qkv, table, small = backward_layer(
            layer == layers - 1,
            live,
            grad,
            weights[layer],
            tables[layer],
            norm_gain[layer],
            (xhat1, inv1, qkv, lse, xhat2, inv2, slope),
        )
        parts = []
        for left, right in ((normed1, g_qkv), (g_p, att), (normed2, g_pre), (g_m, hid)):
            product = tn(left.reshape(-1, width), right.reshape(slots * ROWS, -1)).astype(BF16)
            parts.append(jnp.transpose(product.reshape(width, shares, -1), (1, 0, 2)))
        partial = jnp.concatenate(parts, axis=2).reshape(shares * width, -1)
        grad_weights[layer] = lax.psum_scatter(partial, ("seq", "dp"), scatter_dimension=0, tiled=True).astype(F32)
        per_head = jnp.transpose(table.reshape(-1, KEYS, PER_GROUP, KEYS), (0, 2, 1, 3)).reshape(-1, KEYS * KEYS)
        grad_table = jnp.dot(per_head, onehot, precision=lax.Precision.HIGHEST)
        sums[layer] = (small, grad_table)

    small, grad_table = (jnp.stack(s) for s in zip(*sums))
    small, grad_table = lax.psum((small, grad_table), ("dp", "seq"))
    gains = jnp.stack([small[:, 0, :width], small[:, 2, :width]], axis=1)
    shifts = jnp.stack([small[:, 1, :width], small[:, 3, :width]], axis=1)
    outers = small[:, 4:6, :width]
    mine = lambda value, axis, size: lax.dynamic_slice_in_dim(value, seq * size, size, axis)
    grad_up = mine(small[:, 6], 1, local_units)
    grad_qkv = mine(small[:, 7, : 3 * width].reshape(layers, shares, 3, local_width), 1, 1)[:, 0]
    grad_qv = jnp.stack([grad_qkv[:, 0], grad_qkv[:, 2]], axis=1)
    grad_table = jnp.transpose(mine(grad_table, 1, rel_table.shape[2]), (0, 2, 1))
    parts = split_packed(jnp.stack(grad_weights), local_width, local_units)
    return (
        out,
        from_rows(grad),
        parts[0].reshape(layers, -1, 3, local_width),
        jnp.transpose(parts[1], (0, 2, 1)),
        parts[2],
        jnp.transpose(parts[3], (0, 2, 1)),
        grad_qv,
        grad_table,
        grad_up,
        gains,
        shifts,
        outers,
    )


def solution(mesh):
    slots = P(("dp", "seq"), None, None, None)
    return jax.shard_map(
        local,
        mesh=mesh,
        in_specs=(
            slots,
            P("dp"),
            P(None, "dp", None, "seq"),
            P(None, "seq", "dp"),
            P(None, "dp", "seq"),
            P(None, "seq", "dp"),
            P(None, None, "seq"),
            P(None, None, "seq"),
            P(None, "seq"),
            P(),
            P(),
            P(),
            slots,
        ),
        out_specs=(
            slots,
            slots,
            P(None, "dp", None, "seq"),
            P(None, "seq", "dp"),
            P(None, "dp", "seq"),
            P(None, "seq", "dp"),
            P(None, None, "seq"),
            P(None, None, "seq"),
            P(None, "seq"),
            P(),
            P(),
            P(),
        ),
        check_vma=False,
    )
```

```python
import functools

import jax
import jax.numpy as jnp
import numpy as np
from jax import lax
from jax.experimental import pallas as pl
from jax.experimental.pallas import tpu as pltpu
from jax.sharding import PartitionSpec as P

EPS = 1e-05
F32 = jnp.float32
BF16 = jnp.bfloat16
SIDE = 7
GRID = 14
PLACES = 49
WINDOWS = 4
TOKENS = PLACES * WINDOWS
ROWS = 208
KEYS = 64
PADDED = WINDOWS * KEYS
HEAD = 32
LANES = 128
PER_GROUP = LANES // HEAD
WIDE = PER_GROUP * KEYS
BLOCK = 3 * LANES
SCALE = HEAD**-0.5


def place_tables(shift):
    perm = np.zeros((PADDED, ROWS), np.float32)
    region = np.zeros((WINDOWS, PLACES), np.int64)
    for w in range(WINDOWS):
        for p in range(PLACES):
            row, col = SIDE * (w // 2) + p // SIDE, SIDE * (w % 2) + p % SIDE
            band = [int(v >= 7) + int(v >= 11) for v in (row, col)]
            region[w, p] = 3 * band[0] + band[1]
            row, col = (row + shift) % GRID, (col + shift) % GRID
            source_w = 2 * (row // SIDE) + col // SIDE
            source_p = SIDE * (row % SIDE) + col % SIDE
            perm[KEYS * w + p, WINDOWS * source_p + source_w] = 1.0
    mask = np.zeros((WINDOWS, KEYS, KEYS), np.float32)
    if shift:
        mask[:, :PLACES, :PLACES] = np.where(region[:, :, None] == region[:, None, :], 0.0, -100.0)
    mask[:, PLACES:, :] = -1e30
    return perm, np.tile(mask, (1, 1, PER_GROUP))


def place_onehot():
    onehot = np.zeros((KEYS, KEYS, 169), np.float32)
    for k in range(PLACES):
        for q in range(PLACES):
            rel = (q // 7 - k // 7 + 6) * 13 + (q % 7 - k % 7 + 6)
            onehot[k, q, rel] = 1.0
    return onehot.reshape(KEYS * KEYS, 169)


def nn(a, b):
    return lax.dot_general(a, b, (((1,), (0,)), ((), ())), preferred_element_type=F32)


def nt(a, b):
    return lax.dot_general(a, b, (((1,), (1,)), ((), ())), preferred_element_type=F32)


def tn(a, b):
    return lax.dot_general(a, b, (((0,), (0,)), ((), ())), preferred_element_type=F32)


def row_mean(value):
    return jnp.sum(value, axis=-1, keepdims=True) * (1.0 / value.shape[-1])


def normalize(value):
    centered = value - row_mean(value)
    inverse = lax.rsqrt(row_mean(centered * centered) + EPS)
    return centered * inverse, inverse


def spread_heads(tile):
    head = lax.broadcasted_iota(jnp.int32, tile.shape, 1) // HEAD
    zero = jnp.zeros_like(tile)
    return jnp.concatenate([jnp.where(head == h, tile, zero) for h in range(PER_GROUP)], axis=0)


def join_heads(wide):
    head = lax.broadcasted_iota(jnp.int32, (KEYS, LANES), 1) // HEAD
    total = wide[:KEYS]
    for h in range(1, PER_GROUP):
        total = jnp.where(head == h, wide[KEYS * h : KEYS * (h + 1)], total)
    return total


def cols(at, size):
    return pl.ds(pl.multiple_of(at, LANES), size)


def compact(attn_ref, wq_ref, wo_ref):
    @pl.when(pl.program_id(0) == 0)
    def _():
        for g in range(wo_ref.shape[1] // LANES):
            at = 4 * LANES * g
            wq_ref[:, BLOCK * g : BLOCK * (g + 1)] = attn_ref[:, at : at + BLOCK]
            wo_ref[:, LANES * g : LANES * (g + 1)] = attn_ref[:, at + BLOCK : at + 4 * LANES]


def forward_kernel(
    last,
    live_ref,
    x_ref,
    attn_ref,
    mlp_ref,
    bias_ref,
    mask_ref,
    perm_ref,
    back_ref,
    qvb_ref,
    upb_ref,
    gain_ref,
    shift_ref,
    outb_ref,
    out_ref,
    xhat1_ref,
    inv1_ref,
    normed1_ref,
    qkv_ref,
    lse_ref,
    att_ref,
    xhat2_ref,
    inv2_ref,
    normed2_ref,
    hid_ref,
    slope_ref,
    pad_ref,
    wq_ref,
    wo_ref,
):
    groups = wo_ref.shape[1] // LANES
    compact(attn_ref, wq_ref, wo_ref)
    x = x_ref[0].astype(F32)
    xhat, inverse = normalize(x)
    xhat1_ref[0] = xhat.astype(BF16)
    inv1_ref[0] = jnp.broadcast_to(inverse, (ROWS, LANES))
    normed = (xhat * gain_ref[0:1] + shift_ref[0:1]).astype(BF16)
    normed1_ref[0] = normed
    rolled = nn(perm_ref[...], normed).astype(BF16)
    qkv_ref[0] = (nn(rolled, wq_ref[...]) + qvb_ref[...]).astype(BF16)

    def attend(g, carry):
        bias = bias_ref[g]
        for w in range(WINDOWS):
            rows = slice(KEYS * w, KEYS * (w + 1))
            query = qkv_ref[0, rows, cols(BLOCK * g, LANES)]
            key = qkv_ref[0, rows, cols(BLOCK * g + LANES, LANES)]
            val = qkv_ref[0, rows, cols(BLOCK * g + 2 * LANES, LANES)]
            scores = nt(key, spread_heads(query)) * SCALE + bias + mask_ref[w]
            top = jnp.max(scores, axis=0, keepdims=True)
            expo = jnp.exp(scores - top)
            total = jnp.sum(expo, axis=0, keepdims=True)
            probs = (expo * (1.0 / total)).astype(BF16)
            lse_ref[0, pl.ds(WINDOWS * g + w, 1), :] = top + jnp.log(total)
            pad_ref[rows, cols(LANES * g, LANES)] = join_heads(tn(probs, val)).astype(BF16)
        return carry

    lax.fori_loop(0, groups, attend, 0)
    attended = nn(back_ref[...], pad_ref[...]).astype(BF16)
    att_ref[0] = attended
    middle = x + nt(attended, wo_ref[...]) + outb_ref[0:1]
    xhat, inverse = normalize(middle)
    xhat2_ref[0] = xhat.astype(BF16)
    inv2_ref[0] = jnp.broadcast_to(inverse, (ROWS, LANES))
    normed = (xhat * gain_ref[1:2] + shift_ref[1:2]).astype(BF16)
    normed2_ref[0] = normed
    total = middle + outb_ref[1:2]
    step = mlp_ref.shape[1] // (2 * groups)
    for c in range(groups):
        at = slice(step * c, step * (c + 1))
        pre = nn(normed, mlp_ref[:, 2 * step * c : 2 * step * c + step]) + upb_ref[:, at]
        half = 0.5 * (1.0 + lax.erf(pre * 0.7071067811865476))
        hidden = (pre * half).astype(BF16)
        hid_ref[0, :, at] = hidden
        slope_ref[0, :, at] = (half + pre * jnp.exp(-0.5 * pre * pre) * 0.3989422804014327).astype(BF16)
        total = total + nt(hidden, mlp_ref[:, 2 * step * c + step : 2 * step * (c + 1)])
    if last:
        total = total * live_ref[pl.program_id(0)]
    out_ref[0] = total.astype(out_ref.dtype)


def norm_back(grad, xhat, inverse, gain):
    scaled = grad * gain
    first = row_mean(scaled)
    second = row_mean(scaled * xhat)
    return inverse * (scaled - first - xhat * second)


def add_rows(ref, row, value):
    ref[row : row + 1, : value.shape[1]] += jnp.sum(value, axis=0, keepdims=True)


def backward_kernel(
    first,
    live_ref,
    g_ref,
    attn_ref,
    mlp_ref,
    bias_ref,
    mask_ref,
    perm_ref,
    back_ref,
    gain_ref,
    xhat1_ref,
    inv1_ref,
    qkv_ref,
    lse_ref,
    xhat2_ref,
    inv2_ref,
    slope_ref,
    normed1_ref,
    att_ref,
    normed2_ref,
    hid_ref,
    gout_ref,
    table_ref,
    small_ref,
    gattn_ref,
    gmlp_ref,
    gap_ref,
    gpad_ref,
    wq_ref,
    wo_ref,
    gm_ref,
    gpre_ref,
    gp_ref,
    gqkv_ref,
    kept_n1,
    kept_att,
    kept_n2,
    kept_hid,
    sems,
):
    groups = wo_ref.shape[1] // LANES
    image = pl.program_id(0)
    pairs = ((normed1_ref, kept_n1), (att_ref, kept_att), (normed2_ref, kept_n2), (hid_ref, kept_hid))
    loads = [pltpu.make_async_copy(src, dst, sems.at[k]) for k, (src, dst) in enumerate(pairs)]
    compact(attn_ref, wq_ref, wo_ref)

    @pl.when(image == 0)
    def _():
        table_ref[...] = jnp.zeros_like(table_ref)
        small_ref[...] = jnp.zeros_like(small_ref)
        for load in loads:
            load.start()

    g_res = g_ref[0].astype(F32)
    if first:
        g_res = g_res * live_ref[image]
    add_rows(small_ref, 5, g_res)
    g_m = g_res.astype(BF16)
    gm_ref[image] = g_m
    g_n2 = jnp.zeros_like(g_res)
    step = mlp_ref.shape[1] // (2 * groups)
    for c in range(groups):
        at = slice(step * c, step * (c + 1))
        down = mlp_ref[:, 2 * step * c + step : 2 * step * (c + 1)]
        g_pre = (nn(g_m, down) * slope_ref[0, :, at].astype(F32)).astype(BF16)
        gpre_ref[image, :, at] = g_pre
        add_rows(small_ref, 6 + c, g_pre.astype(F32))
        g_n2 = g_n2 + nt(g_pre, mlp_ref[:, 2 * step * c : 2 * step * c + step])
    xhat = xhat2_ref[0].astype(F32)
    add_rows(small_ref, 2, g_n2 * xhat)
    add_rows(small_ref, 3, g_n2)
    g_mid = g_res + norm_back(g_n2, xhat, inv2_ref[0, :, 0:1], gain_ref[1:2])
    add_rows(small_ref, 4, g_mid)
    g_p = g_mid.astype(BF16)
    gp_ref[image] = g_p
    g_att = nn(g_p, wo_ref[...]).astype(BF16)
    gap_ref[...] = nn(perm_ref[...], g_att).astype(BF16)

    def attend(g, carry):
        bias = bias_ref[g]
        for w in range(WINDOWS):
            rows = slice(KEYS * w, KEYS * (w + 1))
            query = spread_heads(qkv_ref[0, rows, cols(BLOCK * g, LANES)])
            key = qkv_ref[0, rows, cols(BLOCK * g + LANES, LANES)]
            val = qkv_ref[0, rows, cols(BLOCK * g + 2 * LANES, LANES)]
            grad = spread_heads(gap_ref[rows, cols(LANES * g, LANES)])
            scores = nt(key, query) * SCALE + bias + mask_ref[w]
            probs = jnp.exp(scores - lse_ref[0, pl.ds(WINDOWS * g + w, 1), :])
            g_probs = nt(val, grad)
            g_vals = nn(probs.astype(BF16), grad)
            mean = jnp.sum(g_probs * probs, axis=0, keepdims=True)
            g_scores = (probs * (g_probs - mean)).astype(BF16)
            table_ref[g] += g_scores.astype(F32)
            g_keys = nn(g_scores, query) * SCALE
            g_queries = join_heads(tn(g_scores, key)) * SCALE
            gpad_ref[rows, cols(BLOCK * g, LANES)] = g_queries.astype(BF16)
            gpad_ref[rows, cols(BLOCK * g + LANES, LANES)] = g_keys.astype(BF16)
            gpad_ref[rows, cols(BLOCK * g + 2 * LANES, LANES)] = g_vals.astype(BF16)
        return carry

    lax.fori_loop(0, groups, attend, 0)
    g_qkv = nn(back_ref[...], gpad_ref[...]).astype(BF16)
    gqkv_ref[image] = g_qkv
    for g in range(groups):
        for row, at in ((10, BLOCK * g), (11, BLOCK * g + 2 * LANES)):
            part = g_qkv[:, at : at + LANES].astype(F32)
            small_ref[row : row + 1, LANES * g : LANES * (g + 1)] += jnp.sum(part, axis=0, keepdims=True)
    g_n1 = nt(g_qkv, wq_ref[...])
    xhat = xhat1_ref[0].astype(F32)
    add_rows(small_ref, 0, g_n1 * xhat)
    add_rows(small_ref, 1, g_n1)
    gout_ref[0] = g_mid + norm_back(g_n1, xhat, inv1_ref[0, :, 0:1], gain_ref[0:1])

    @pl.when(image == pl.num_programs(0) - 1)
    def _():
        for load in loads:
            load.wait()
        flat = lambda ref: ref.reshape(ref.shape[0] * ref.shape[1], ref.shape[2])

        def product(left_ref, right_ref, size, out_ref, stride, start):
            left = flat(left_ref)[...].T
            for g in range(groups):
                right = flat(right_ref)[:, size * g : size * (g + 1)]
                at = stride * g + start
                out_ref[:, at : at + size] = nn(left, right).astype(BF16)

        product(gm_ref, kept_hid, step, gmlp_ref, 2 * step, step)
        product(kept_n2, gpre_ref, step, gmlp_ref, 2 * step, 0)
        product(gp_ref, kept_att, LANES, gattn_ref, 4 * LANES, BLOCK)
        product(kept_n1, gqkv_ref, BLOCK, gattn_ref, 4 * LANES, 0)


def whole(array):
    zeros = (0,) * array.ndim
    return pl.BlockSpec(array.shape, lambda i: zeros, pipeline_mode=pl.Buffered(1))


def per_image(shape):
    tail = (0,) * (len(shape) - 1)
    return pl.BlockSpec((1,) + tuple(shape[1:]), lambda i: (i,) + tail)


def fixed(shape):
    zeros = (0,) * len(shape)
    return pl.BlockSpec(shape, lambda i: zeros)


def of_layer(array, layer):
    tail = (0,) * (array.ndim - 1)
    return pl.BlockSpec((None,) + array.shape[1:], lambda i: (layer,) + tail, pipeline_mode=pl.Buffered(1))


SMEM = pl.BlockSpec(memory_space=pltpu.SMEM)
ANY = pl.BlockSpec(memory_space=pl.ANY)
PARAMS = pltpu.CompilerParams(dimension_semantics=("arbitrary",), vmem_limit_bytes=60000 * 1024)


def forward_layer(layer, last, live, x, attn, mlp, tables, rows):
    images = x.shape[0]
    width, units = attn.shape[1], mlp.shape[2] // 2
    groups = width // LANES
    total = groups * BLOCK
    shapes = [
        ((images, ROWS, width), BF16 if last else F32),
        ((images, ROWS, width), BF16),
        ((images, ROWS, LANES), F32),
        ((images, ROWS, width), BF16),
        ((images, PADDED, total), BF16),
        ((images, groups * WINDOWS, WIDE), F32),
        ((images, ROWS, width), BF16),
        ((images, ROWS, width), BF16),
        ((images, ROWS, LANES), F32),
        ((images, ROWS, width), BF16),
        ((images, ROWS, units), BF16),
        ((images, ROWS, units), BF16),
    ]
    fixed_args = (*tables, *rows)
    return pl.pallas_call(
        functools.partial(forward_kernel, last),
        grid=(images,),
        in_specs=[SMEM, per_image(x.shape), of_layer(attn, layer), of_layer(mlp, layer)]
        + [whole(a) for a in fixed_args],
        out_specs=[per_image(s) for s, _ in shapes],
        out_shape=[jax.ShapeDtypeStruct(s, d) for s, d in shapes],
        scratch_shapes=[
            pltpu.VMEM((PADDED, width), BF16),
            pltpu.VMEM((width, total), BF16),
            pltpu.VMEM((width, width), BF16),
        ],
        compiler_params=PARAMS,
        name="forward_layer",
    )(live, x, attn, mlp, *fixed_args)


def backward_layer(layer, first, live, g, attn, mlp, tables, gain, saved, operands):
    images = g.shape[0]
    width, units = attn.shape[1], mlp.shape[2] // 2
    groups = width // LANES
    total = groups * BLOCK
    sums = [((groups, KEYS, WIDE), F32), ((16, width), F32), (attn.shape[1:], BF16), (mlp.shape[1:], BF16)]
    fixed_args = (*tables, gain)
    return pl.pallas_call(
        functools.partial(backward_kernel, first),
        grid=(images,),
        in_specs=[SMEM, per_image(g.shape), of_layer(attn, layer), of_layer(mlp, layer)]
        + [whole(a) for a in fixed_args]
        + [per_image(a.shape) for a in saved]
        + [ANY] * len(operands),
        out_specs=[per_image(g.shape)] + [fixed(s) for s, _ in sums],
        out_shape=[jax.ShapeDtypeStruct(g.shape, F32)] + [jax.ShapeDtypeStruct(s, d) for s, d in sums],
        scratch_shapes=[
            pltpu.VMEM((PADDED, width), BF16),
            pltpu.VMEM((PADDED, total), BF16),
            pltpu.VMEM((width, total), BF16),
            pltpu.VMEM((width, width), BF16),
            pltpu.VMEM((images, ROWS, width), BF16),
            pltpu.VMEM((images, ROWS, units), BF16),
            pltpu.VMEM((images, ROWS, width), BF16),
            pltpu.VMEM((images, ROWS, total), BF16),
        ]
        + [pltpu.VMEM(a.shape, a.dtype) for a in operands]
        + [pltpu.SemaphoreType.DMA((len(operands),))],
        compiler_params=PARAMS,
        name="backward_layer",
    )(live, g, attn, mlp, *fixed_args, *saved, *operands)


MESH = pl.DeviceIdType.MESH
LINE = 4
PLANES = 2


class Place:
    def __init__(self, rest):
        dp, seq = lax.axis_index("dp"), lax.axis_index("seq")
        self.rest = rest
        self.z, self.u = dp // rest, dp % rest
        self.x, self.c = seq // PLANES, seq % PLANES

    def at(self, z=0, u=0, x=0, c=0):
        dp = (self.z + z) % LINE * self.rest + (self.u + u) % self.rest
        return (dp, (self.x + x) % 2 * PLANES + (self.c + c) % 2)

    def peers(self):
        near = [self.at(z=k) for k in range(1, LINE)] + [self.at(u=k) for k in range(1, self.rest)]
        return near + [self.at(x=1), self.at(c=1)]


def greet(peers):
    barrier = pltpu.get_barrier_semaphore()
    for peer in peers:
        pl.semaphore_signal(barrier, inc=1, device_id=peer, device_id_type=MESH)
    pl.semaphore_wait(barrier, len(peers))


class Copies:
    def __init__(self, send, recv):
        self.send, self.recv, self.used, self.all = send, recv, 0, []

    def start(self, src, dst, peer):
        at = self.used
        self.used += 1
        copy = pltpu.make_async_remote_copy(
            src_ref=src,
            dst_ref=dst,
            send_sem=self.send.at[at],
            recv_sem=self.recv.at[at],
            device_id=peer,
            device_id_type=MESH,
        )
        copy.start()
        self.all.append(copy)
        return copy

    def drain(self):
        for copy in self.all:
            copy.wait_send()


def arrive(copies):
    for copy in copies:
        copy.wait_recv()


def stages(count, steps):
    order = []
    for tick in range(count * 2 + steps):
        for step in reversed(range(steps)):
            chunk2 = tick - step
            if chunk2 >= 0 and chunk2 % 1 == 0 and chunk2 < count:
                order.append((step, chunk2))
    return order


def gather_kernel(rest, small_ref, wq_ref, wo_ref, wu_ref, wd_ref, all_ref, attn_ref, mlp_ref, attn_own, mlp_own, load, send, recv):
    here = Place(rest)
    layers, rows = attn_own.shape[:2]
    half = rows // 2
    loads = []

    def fetch(src, dst):
        copy = pltpu.make_async_copy(src, dst, load.at[len(loads)])
        copy.start()
        loads.append(copy)
        return copy

    fills = []
    for l in range(layers):
        fills.append(
            [fetch(wq_ref.at[l, t], attn_own.at[l, :, pl.ds(LANES * t, LANES)]) for t in range(3)]
            + [fetch(wo_ref.at[l], attn_own.at[l, :, pl.ds(3 * LANES, LANES)])]
        )
        units = wu_ref.shape[2]
        fills.append(
            [
                fetch(wu_ref.at[l], mlp_own.at[l, :, pl.ds(0, units)]),
                fetch(wd_ref.at[l], mlp_own.at[l, :, pl.ds(units, units)]),
            ]
        )
    greet(here.peers() + [here.at(x=1, c=1)])
    copies = Copies(send, recv)
    spot = here.x * PLANES + here.c
    small = [copies.start(small_ref, all_ref.at[spot], peer) for peer in (here.at(c=1), here.at(x=1), here.at(x=1, c=1))]
    keep = fetch(small_ref, all_ref.at[spot])
    first, second = pl.ds(0, half), pl.ds(half, half)
    both = pl.ds(0, rows)
    chunks = []
    for l in range(layers):
        chunks += [(attn_own.at[l], attn_ref.at[l]), (mlp_own.at[l], mlp_ref.at[l])]
    z, u, x, c = here.z, here.u, here.x, here.c
    others = range(1, rest)

    state = []
    for k, (own, full) in enumerate(chunks):
        width = own.shape[1]

        def span(x, c, width=width):
            return pl.ds(pl.multiple_of((c * 2 + x) * width, width), width)

        def pair(c, width=width):
            return pl.ds(pl.multiple_of(c * 2 * width, 2 * width), 2 * width)

        for fill in fills[k]:
            fill.wait()
        mine = full.at[z, u, both, span(x, c)]
        local = fetch(own, mine)
        line = [copies.start(own, mine, here.at(z=d)) for d in range(1, LINE)]
        state.append(dict(full=full, span=span, pair=pair, local=local, line=line, swap=[]))

    def step_one(s):
        full, span = s["full"], s["span"]
        s["local"].wait()
        arrive(s["line"])
        cols = span(x, c)
        block = full.at[:, u, first, cols]
        s["a"] = [copies.start(block, block, here.at(x=1))]
        block = full.at[:, u, second, cols]
        s["b"] = [copies.start(block, block, here.at(u=d)) for d in others]
        block = full.at[:, u, both, cols]
        s["swap"] += [copies.start(block, block, here.at(c=1))]

    def step_two(s):
        full, span, pair = s["full"], s["span"], s["pair"]
        arrive(s["a"])
        block = full.at[:, u, first, pair(c)]
        s["a"] = [copies.start(block, block, here.at(u=d)) for d in others]
        arrive(s["b"])
        block = full.at[:, :, second, span(x, c)]
        s["b"] = [copies.start(block, block, here.at(x=1))]
        block = full.at[:, u, first, span(1 - x, c)]
        s["swap"] += [copies.start(block, block, here.at(c=1))]
        for d in others:
            block = full.at[:, (u + d) % rest, second, span(x, c)]
            s["swap"] += [copies.start(block, block, here.at(c=1))]

    def step_three(s):
        full, span, pair = s["full"], s["span"], s["pair"]
        arrive(s["a"])
        for d in others:
            block = full.at[:, (u + d) % rest, first, pair(c)]
            s["swap"] += [copies.start(block, block, here.at(c=1))]
        arrive(s["b"])
        block = full.at[:, :, second, span(1 - x, c)]
        s["swap"] += [copies.start(block, block, here.at(c=1))]

    steps = (step_one, step_two, step_three)
    for step, k in stages(len(chunks), len(steps)):
        steps[step](state[k])
    for s in state:
        arrive(s["swap"])
    arrive(small)
    keep.wait()
    copies.drain()


def gather_copies(layers, rest):
    return 3 + 2 * layers * (LINE - 1 + 1 + (rest - 1) + 1 + (rest - 1) + 1 + 1 + (rest - 1) + 1 + (rest - 1) + 1)


def gather_weights(small, wq, wo, wu, wd):
    layers, rows, units = wu.shape
    shares = lax.axis_size("seq")
    rest = lax.axis_size("dp") // LINE
    count = gather_copies(layers, rest)
    attn = jax.ShapeDtypeStruct((layers, LINE, rest, rows, shares * 4 * LANES), BF16)
    mlp = jax.ShapeDtypeStruct((layers, LINE, rest, rows, shares * 2 * units), BF16)
    every = jax.ShapeDtypeStruct((shares,) + small.shape, F32)
    spot = pl.BlockSpec(memory_space=pl.ANY)
    every, attn, mlp = pl.pallas_call(
        functools.partial(gather_kernel, rest),
        in_specs=[spot] * 5,
        out_specs=[spot] * 3,
        out_shape=[every, attn, mlp],
        scratch_shapes=[
            pltpu.VMEM((layers, rows, 4 * LANES), BF16),
            pltpu.VMEM((layers, rows, 2 * units), BF16),
            pltpu.SemaphoreType.DMA((layers * 8 + 1,)),
            pltpu.SemaphoreType.DMA((count,)),
            pltpu.SemaphoreType.DMA((count,)),
        ],
        compiler_params=pltpu.CompilerParams(collective_id=0, has_side_effects=True),
        name="gather_weights",
    )(small, wq, wo, wu, wd)
    width = LINE * rest * rows
    return every, attn.reshape(layers, width, -1), mlp.reshape(layers, width, -1)


def scatter_kernel(rest, layers, *refs):
    small_ref, *refs = refs
    attn_ref, mlp_ref, refs = refs[:layers], refs[layers : 2 * layers], refs[2 * layers :]
    (sum_ref, attn_out, mlp_out, attn_acc, attn_swap, attn_x, attn_u, attn_x2, attn_u2, attn_z, mlp_acc, mlp_swap, mlp_x, mlp_u, mlp_x2, mlp_u2, mlp_z, small_at, small_in, small_u, small_z, load, send, recv) = refs
    here = Place(rest)
    rows = attn_out.shape[1]
    half = rows // 2
    z, u, x, c = here.z, here.u, here.x, here.c
    first, second, both = pl.ds(0, half), pl.ds(half, half), pl.ds(0, rows)
    others = range(1, rest)
    chunks = []
    for l in reversed(range(layers)):
        chunks.append((mlp_ref[l], mlp_out.at[l], *(b.at[l] for b in (mlp_acc, mlp_swap, mlp_x, mlp_u, mlp_x2, mlp_u2, mlp_z))))
    for l in reversed(range(layers)):
        chunks.append((attn_ref[l], attn_out.at[l], *(b.at[l] for b in (attn_acc, attn_swap, attn_x, attn_u, attn_x2, attn_u2, attn_z))))
    loads = []

    def fetch(src, dst):
        copy = pltpu.make_async_copy(src, dst, load.at[len(loads)])
        copy.start()
        loads.append(copy)
        return copy

    state = []
    for full, out, acc, swap, xbuf, ubuf, xbuf2, ubuf2, zbuf in chunks:
        width = out.shape[1]

        def pair(c, width=width):
            return pl.ds(pl.multiple_of(c * 2 * width, 2 * width), 2 * width)

        def span(x, width=width):
            return pl.ds(pl.multiple_of(x * width, width), width)

        own = fetch(full.at[:, :, :, pair(c)], acc)
        state.append(dict(full=full, out=out, acc=acc, swap=swap, x=xbuf, u=ubuf, x2=xbuf2, u2=ubuf2, z=zbuf, span=span, pair=pair, own=own))
    greet(here.peers())
    copies = Copies(send, recv)
    keep = fetch(small_ref, small_at.at[0])
    little = [copies.start(small_ref, small_in.at[0], here.at(c=1))]
    for s in state:
        s["wait"] = [copies.start(s["full"].at[:, :, :, s["pair"](1 - c)], s["swap"], here.at(c=1))]

    def each(count, body):
        def step(i, carry):
            body(i)
            return carry

        lax.fori_loop(0, count, step, 0)

    def plus(ref, at, *others_):
        total = ref[at].astype(F32)
        for other in others_:
            total = total + other.astype(F32)
        ref[at] = total.astype(BF16)

    def step_one(s):
        s["own"].wait()
        arrive(s["wait"])
        acc, swap, span = s["acc"], s["swap"], s["span"]

        def add(i):
            a, b = i // rest, i % rest
            plus(acc, (a, b), swap[a, b])

        each(LINE * rest, add)
        s["wait"] = [copies.start(acc.at[:, :, first, span(1 - x)], s["x"], here.at(x=1))]
        for d in others:
            s["wait"].append(copies.start(acc.at[:, (u + d) % rest, second, :], s["u"].at[d - 1], here.at(u=d)))

    def step_two(s):
        arrive(s["wait"])
        acc, span = s["acc"], s["span"]
        mine = span(x)

        def add(i):
            a, b = i // rest, i % rest
            plus(acc, (a, b, first, mine), s["x"][a, b])

        each(LINE * rest, add)

        def add_u(a):
            plus(acc, (a, u, second), *(s["u"][d - 1, a] for d in others))

        each(LINE, add_u)
        s["wait"] = [copies.start(acc.at[:, u, second, span(1 - x)], s["x2"], here.at(x=1))]
        for d in others:
            s["wait"].append(copies.start(acc.at[:, (u + d) % rest, first, mine], s["u2"].at[d - 1], here.at(u=d)))

    def step_three(s):
        arrive(s["wait"])
        acc, span = s["acc"], s["span"]
        mine = span(x)

        def add(a):
            plus(acc, (a, u, second, mine), s["x2"][a])
            plus(acc, (a, u, first, mine), *(s["u2"][d - 1, a] for d in others))

        each(LINE, add)
        s["wait"] = [copies.start(acc.at[(z + d) % LINE, u, both, mine], s["z"].at[d - 1], here.at(z=d)) for d in range(1, LINE)]

    def step_four(s):
        arrive(s["wait"])
        total = s["acc"][z, u, both, s["span"](x)].astype(F32)
        for d in range(1, LINE):
            total = total + s["z"][d - 1].astype(F32)
        s["out"][...] = total

    def little_one():
        keep.wait()
        arrive(little)
        small_at[1] = small_at[0] + small_in[0]
        little[:] = [copies.start(small_at.at[1], small_in.at[1], here.at(x=1))]

    def little_two():
        arrive(little)
        small_u[u] = small_at[1] + small_in[1]
        little[:] = [copies.start(small_u.at[u], small_u.at[u], here.at(u=d)) for d in others]

    def little_three():
        arrive(little)
        total = small_u[0]
        for d in others:
            total = total + small_u[d]
        small_z[z] = total
        little[:] = [copies.start(small_z.at[z], small_z.at[z], here.at(z=d)) for d in range(1, LINE)]

    def little_four():
        arrive(little)
        total = small_z[0]
        for d in range(1, LINE):
            total = total + small_z[d]
        sum_ref[...] = total

    steps = (step_one, step_two, step_three, step_four)
    smalls = [little_one, little_two, little_three, little_four]
    for step, k in stages(len(chunks), len(steps)):
        steps[step](state[k])
        if smalls and step == 0:
            smalls.pop(0)()
    for step in smalls:
        step()
    copies.drain()


def scatter_weights(small, attn, mlp):
    layers, width = len(attn), attn[0].shape[0]
    shares = lax.axis_size("seq")
    rest = lax.axis_size("dp") // LINE
    rows = width // (LINE * rest)
    half = rows // 2
    wides = [attn[0].shape[1] // shares, mlp[0].shape[1] // shares]
    count = layers * 2 * (1 + 2 * rest + LINE - 1) + 2 + rest - 1 + LINE - 1
    spot = pl.BlockSpec(memory_space=pl.ANY)
    vmem = pl.BlockSpec(memory_space=pltpu.VMEM)
    buffers = []
    for w in wides:
        for shape in (
            (LINE, rest, rows, 2 * w),
            (LINE, rest, rows, 2 * w),
            (LINE, rest, half, w),
            (rest - 1, LINE, half, 2 * w),
            (LINE, half, w),
            (rest - 1, LINE, half, w),
            (LINE - 1, rows, w),
        ):
            buffers.append(pltpu.VMEM((layers,) + shape, BF16))
    little = [pltpu.VMEM((n,) + small.shape, F32) for n in (2, 2, rest, LINE)]
    four = lambda a: a.reshape(LINE, rest, rows, -1)
    return pl.pallas_call(
        functools.partial(scatter_kernel, rest, layers),
        in_specs=[spot] * (1 + 2 * layers),
        out_specs=[vmem] * 3,
        out_shape=[jax.ShapeDtypeStruct(small.shape, F32)] + [jax.ShapeDtypeStruct((layers, rows, w), F32) for w in wides],
        scratch_shapes=buffers
        + little
        + [
            pltpu.SemaphoreType.DMA((layers * 2 + 1,)),
            pltpu.SemaphoreType.DMA((count,)),
            pltpu.SemaphoreType.DMA((count,)),
        ],
        compiler_params=pltpu.CompilerParams(collective_id=1, has_side_effects=True, vmem_limit_bytes=60000 * 1024),
        name="scatter_weights",
    )(small, *(four(a) for a in (*attn, *mlp)))


def to_rows(images):
    slots, width = images.shape[0], images.shape[3]
    flat = jnp.transpose(images, (0, 2, 1, 3)).reshape(slots, TOKENS, width)
    return jnp.pad(flat, ((0, 0), (0, ROWS - TOKENS), (0, 0)))


def from_rows(rows):
    slots, width = rows.shape[0], rows.shape[2]
    return jnp.transpose(rows[:, :TOKENS].reshape(slots, PLACES, WINDOWS, width), (0, 2, 1, 3))


def local(
    activations,
    counts,
    w_qkv,
    w_out,
    w_up,
    w_down,
    qv_bias,
    rel_table,
    up_bias,
    norm_gain,
    norm_bias,
    out_bias,
    cotangent,
):
    slots, width = activations.shape[0], activations.shape[3]
    layers = w_qkv.shape[0]
    shares = lax.axis_size("seq")
    seq = lax.axis_index("seq")
    spot = seq % PLANES * 2 + seq // PLANES
    units = w_up.shape[2]
    heads = rel_table.shape[2]
    live = (seq * slots + jnp.arange(slots) < counts[0]).astype(F32)
    onehot = jnp.asarray(place_onehot())

    table = jnp.pad(jnp.transpose(rel_table, (0, 2, 1)), ((0, 0), (0, 0), (0, 2 * LANES - 169)))
    pieces = [p.astype(F32).reshape(-1, LANES) for p in (qv_bias, up_bias, table)]
    at = np.cumsum([0] + [p.shape[0] for p in pieces])
    every, attn, mlp = gather_weights(
        jnp.concatenate(pieces),
        jnp.transpose(w_qkv, (0, 2, 1, 3)),
        jnp.transpose(w_out, (0, 2, 1)),
        w_up,
        jnp.transpose(w_down, (0, 2, 1)),
    )
    every = jnp.stack([every[PLANES * (p % 2) + p // 2] for p in range(shares)])
    all_qv = every[:, at[0] : at[1]].reshape(shares, layers, 2, LANES)
    all_up = every[:, at[1] : at[2]].reshape(shares, layers, units)
    all_table = every[:, at[2] : at[3]].reshape(shares, layers, heads, 2 * LANES)[..., :169]

    tables, rows = [], []
    for layer in range(layers):
        perm, mask = place_tables(3 if layer % 2 == 1 else 0)
        lookup = jnp.dot(
            onehot, all_table[:, layer].reshape(-1, 169).T, precision=lax.Precision.HIGHEST
        ).reshape(KEYS, KEYS, -1, PER_GROUP)
        bias = jnp.transpose(lookup, (2, 0, 3, 1)).reshape(-1, KEYS, WIDE)
        tables.append((bias, jnp.asarray(mask), jnp.asarray(perm, BF16), jnp.asarray(perm.T, BF16)))
        qv = all_qv[:, layer]
        qvb = jnp.stack([qv[:, 0], jnp.zeros_like(qv[:, 0]), qv[:, 1]], axis=1).reshape(1, -1)
        upb = all_up[:, layer].reshape(1, -1)
        rows.append((qvb, upb, norm_gain[layer], norm_bias[layer], out_bias[layer]))

    residual = to_rows(activations)
    saved = []
    for layer in range(layers):
        last = layer == layers - 1
        residual, *kept = forward_layer(layer, last, live, residual, attn, mlp, tables[layer], rows[layer])
        saved.append(kept)
    out = from_rows(residual)

    grad = to_rows(cotangent)
    smalls, grads_attn, grads_mlp = [None] * layers, [None] * layers, [None] * layers
    for layer in reversed(range(layers)):
        xhat1, inv1, normed1, qkv, lse, att, xhat2, inv2, normed2, hid, slope = saved[layer]
        grad, table, small, grads_attn[layer], grads_mlp[layer] = backward_layer(
            layer,
            layer == layers - 1,
            live,
            grad,
            attn,
            mlp,
            tables[layer],
            norm_gain[layer],
            (xhat1, inv1, qkv, lse, xhat2, inv2, slope),
            (normed1, att, normed2, hid),
        )
        per_head = jnp.transpose(table.reshape(-1, KEYS, PER_GROUP, KEYS), (0, 2, 1, 3)).reshape(-1, KEYS * KEYS)
        grad_table = jnp.dot(per_head, onehot, precision=lax.Precision.HIGHEST)
        grad_table = jnp.pad(grad_table, ((0, 0), (0, 2 * LANES - 169))).reshape(-1, width)
        smalls[layer] = jnp.concatenate([small, grad_table])

    total, grad_attn, grad_mlp = scatter_weights(jnp.stack(smalls), grads_attn, grads_mlp)
    mine = lambda value, axis, size: lax.dynamic_slice_in_dim(value, spot * size, size, axis)
    grad_table = mine(total[:, 16:].reshape(layers, -1, 2 * LANES), 1, heads)[..., :169]
    return (
        out,
        from_rows(grad),
        jnp.transpose(grad_attn[..., :BLOCK].reshape(layers, -1, 3, LANES), (0, 1, 2, 3)),
        jnp.transpose(grad_attn[..., BLOCK:], (0, 2, 1)),
        grad_mlp[..., :units],
        jnp.transpose(grad_mlp[..., units:], (0, 2, 1)),
        mine(total[:, 10:12], 2, LANES),
        jnp.transpose(grad_table, (0, 2, 1)),
        mine(total[:, 6:10], 1, 1)[:, 0],
        total[:, 0:3:2],
        total[:, 1:4:2],
        total[:, 4:6],
    )


def solution(mesh):
    slots = P(("dp", "seq"), None, None, None)
    return jax.shard_map(
        local,
        mesh=mesh,
        in_specs=(
            slots,
            P("dp"),
            P(None, "dp", None, "seq"),
            P(None, "seq", "dp"),
            P(None, "dp", "seq"),
            P(None, "seq", "dp"),
            P(None, None, "seq"),
            P(None, None, "seq"),
            P(None, "seq"),
            P(),
            P(),
            P(),
            slots,
        ),
        out_specs=(
            slots,
            slots,
            P(None, "dp", None, "seq"),
            P(None, "seq", "dp"),
            P(None, "dp", "seq"),
            P(None, "seq", "dp"),
            P(None, None, "seq"),
            P(None, None, "seq"),
            P(None, "seq"),
            P(),
            P(),
            P(),
        ),
        check_vma=False,
    )
```

```python
import functools

import jax
import jax.numpy as jnp
import numpy as np
from jax import lax
from jax.experimental import pallas as pl
from jax.experimental.pallas import tpu as pltpu
from jax.sharding import PartitionSpec as P

EPS = 1e-05
F32 = jnp.float32
BF16 = jnp.bfloat16
SIDE = 7
GRID = 14
PLACES = 49
WINDOWS = 4
TOKENS = PLACES * WINDOWS
ROWS = 208
KEYS = 64
PADDED = WINDOWS * KEYS
HEAD = 32
LANES = 128
PER_GROUP = LANES // HEAD
WIDE = PER_GROUP * KEYS
BLOCK = 3 * LANES
SCALE = HEAD**-0.5


def place_tables(shift):
    perm = np.zeros((PADDED, ROWS), np.float32)
    region = np.zeros((WINDOWS, PLACES), np.int64)
    for w in range(WINDOWS):
        for p in range(PLACES):
            row, col = SIDE * (w // 2) + p // SIDE, SIDE * (w % 2) + p % SIDE
            band = [int(v >= 7) + int(v >= 11) for v in (row, col)]
            region[w, p] = 3 * band[0] + band[1]
            row, col = (row + shift) % GRID, (col + shift) % GRID
            source_w = 2 * (row // SIDE) + col // SIDE
            source_p = SIDE * (row % SIDE) + col % SIDE
            perm[KEYS * w + p, WINDOWS * source_p + source_w] = 1.0
    mask = np.zeros((WINDOWS, KEYS, KEYS), np.float32)
    if shift:
        mask[:, :PLACES, :PLACES] = np.where(region[:, :, None] == region[:, None, :], 0.0, -100.0)
    mask[:, PLACES:, :] = -1e30
    return perm, np.tile(mask, (1, 1, PER_GROUP))


def place_onehot():
    onehot = np.zeros((KEYS, KEYS, 169), np.float32)
    for k in range(PLACES):
        for q in range(PLACES):
            rel = (q // 7 - k // 7 + 6) * 13 + (q % 7 - k % 7 + 6)
            onehot[k, q, rel] = 1.0
    return onehot.reshape(KEYS * KEYS, 169)


def nn(a, b):
    return lax.dot_general(a, b, (((1,), (0,)), ((), ())), preferred_element_type=F32)


def nt(a, b):
    return lax.dot_general(a, b, (((1,), (1,)), ((), ())), preferred_element_type=F32)


def tn(a, b):
    return lax.dot_general(a, b, (((0,), (0,)), ((), ())), preferred_element_type=F32)


def row_mean(value):
    return jnp.sum(value, axis=-1, keepdims=True) * (1.0 / value.shape[-1])


def normalize(value):
    centered = value - row_mean(value)
    inverse = lax.rsqrt(row_mean(centered * centered) + EPS)
    return centered * inverse, inverse


def spread_heads(tile):
    head = lax.broadcasted_iota(jnp.int32, tile.shape, 1) // HEAD
    zero = jnp.zeros_like(tile)
    return jnp.concatenate([jnp.where(head == h, tile, zero) for h in range(PER_GROUP)], axis=0)


def join_heads(wide):
    head = lax.broadcasted_iota(jnp.int32, (KEYS, LANES), 1) // HEAD
    total = wide[:KEYS]
    for h in range(1, PER_GROUP):
        total = jnp.where(head == h, wide[KEYS * h : KEYS * (h + 1)], total)
    return total


def cols(at, size):
    return pl.ds(pl.multiple_of(at, LANES), size)


SMEM = pl.BlockSpec(memory_space=pltpu.SMEM)
ANY = pl.BlockSpec(memory_space=pl.ANY)

MESH = pl.DeviceIdType.MESH
LINE = 4
PLANES = 2


class Place:
    def __init__(self, rest):
        dp, seq = lax.axis_index("dp"), lax.axis_index("seq")
        self.rest = rest
        self.z, self.u = dp // rest, dp % rest
        self.x, self.c = seq // PLANES, seq % PLANES

    def at(self, z=0, u=0, x=0, c=0):
        dp = (self.z + z) % LINE * self.rest + (self.u + u) % self.rest
        return (dp, (self.x + x) % 2 * PLANES + (self.c + c) % 2)

    def greet(self, *more):
        near = [self.at(z=k) for k in range(1, LINE)] + [self.at(u=k) for k in range(1, self.rest)]
        peers = near + [self.at(x=1), self.at(c=1), *more]
        barrier = pltpu.get_barrier_semaphore()
        for peer in peers:
            pl.semaphore_signal(barrier, inc=1, device_id=peer, device_id_type=MESH)
        pl.semaphore_wait(barrier, len(peers))


class Copies:
    def __init__(self, load, send, recv):
        self.load, self.send, self.recv = load, send, recv
        self.loads, self.sent = 0, []

    def local(self, src, dst):
        self.loads += 1
        return pltpu.make_async_copy(src, dst, self.load.at[self.loads - 1])

    def remote(self, src, dst, peer):
        at = len(self.sent)
        copy = pltpu.make_async_remote_copy(
            src_ref=src,
            dst_ref=dst,
            send_sem=self.send.at[at],
            recv_sem=self.recv.at[at],
            device_id=peer,
            device_id_type=MESH,
        )
        self.sent.append(copy)
        return copy

    def drain(self):
        for copy in self.sent:
            copy.wait_send()


def start(copies):
    for copy in copies:
        copy.start()


def arrive(copies):
    for copy in copies:
        copy.wait_recv()


def schedule(count, begin, steps, lag=3.0):
    free, ready, plan = {}, [(0.0, k, 0) for k in range(count)], []
    transfers = [begin, *steps]
    while ready:
        ready.sort()
        now, k, s = ready.pop(0)
        if s > 0:
            plan.append((now, s - 1, k))
        if s < len(transfers) and transfers[s]:
            link, total = transfers[s]
            free[link] = max(free.get(link, 0.0), now) + total / count
            ready.append((free[link] + lag, k, s + 1))
    return plan


def row_chunks(rows, least):
    count = max(1, rows // least)
    size = rows // count
    return [(k * size, size) for k in range(count)]


ATTN_ROWS, MLP_ROWS = 32, 16


class Gather:
    def __init__(self, here, copies, fills, chunks):
        self.copies, self.items = copies, []
        self.fills = [copies.local(a, b) for a, b in fills]
        z, u, x, c, rest = here.z, here.u, here.x, here.c, here.rest
        others = range(1, rest)
        for own, full, (at, rows) in chunks:
            width = own.shape[1]
            half = rows // 2
            first, second, both = pl.ds(at, half), pl.ds(at + half, half), pl.ds(at, rows)
            span = [pl.ds(pl.multiple_of((c * 2 + (x + d) % 2) * width, width), width) for d in range(2)]
            pair = pl.ds(pl.multiple_of(c * 2 * width, 2 * width), 2 * width)

            def send(index, **offset):
                return copies.remote(full.at[index], full.at[index], here.at(**offset))

            mine = full.at[z, u, both, span[0]]
            shard = own.at[both, :]
            item = dict(
                local=[copies.local(shard, mine)],
                line=[copies.remote(shard, mine, here.at(z=d)) for d in range(1, LINE)],
            )
            every = slice(None)
            item["a1"] = [send((every, u, first, span[0]), x=1)]
            item["b1"] = [send((every, u, second, span[0]), u=d) for d in others]
            item["d1"] = [send((every, u, both, span[0]), c=1)]
            item["a2"] = [send((every, u, first, pair), u=d) for d in others]
            item["b2"] = [send((every, every, second, span[0]), x=1)]
            item["d2"] = [send((every, u, first, span[1]), c=1)]
            item["d2"] += [send((every, (u + d) % rest, second, span[0]), c=1) for d in others]
            item["d3"] = [send((every, (u + d) % rest, first, pair), c=1) for d in others]
            item["d3"] += [send((every, every, second, span[1]), c=1)]
            self.items.append(item)

    def fill(self):
        start(self.fills)

    def begin(self):
        for copy in self.fills:
            copy.wait()
        for item in self.items:
            start(item["local"] + item["line"])

    def events(self):
        def one(item):
            item["local"][0].wait()
            arrive(item["line"])
            start(item["a1"] + item["b1"] + item["d1"])

        def two(item):
            arrive(item["a1"])
            start(item["a2"])
            arrive(item["b1"])
            start(item["b2"] + item["d2"])

        def three(item):
            arrive(item["a2"] + item["b2"])
            start(item["d3"])

        steps = (one, two, three)
        plan = schedule(len(self.items), ("z", 15.0), [("xy", 8.0), ("xy", 16.0), None])
        return [(t, functools.partial(steps[s], self.items[k])) for t, s, k in plan]

    def finish(self):
        for item in self.items:
            arrive(item["d1"] + item["d2"] + item["d3"])


def gather_sems(chunks, rest, more=0):
    count = chunks * (LINE + 4 + 4 * (rest - 1)) + more
    return [pltpu.SemaphoreType.DMA((n,)) for n in (chunks + 7, count, count)]


def shard_chunks(layer, wq_ref, wo_ref, wu_ref, wd_ref, attn_own, mlp_own, attn_ref, mlp_ref):
    units = wu_ref.shape[2]
    part = lambda ref, at, size: ref.at[:, pl.ds(at, size)]
    fills = [(wq_ref.at[layer, t], part(attn_own, LANES * t, LANES)) for t in range(3)]
    fills += [(wo_ref.at[layer], part(attn_own, BLOCK, LANES))]
    fills += [(wu_ref.at[layer], part(mlp_own, 0, units)), (wd_ref.at[layer], part(mlp_own, units, units))]
    rows = attn_own.shape[0]
    chunks = [(attn_own, attn_ref, r) for r in row_chunks(rows, ATTN_ROWS)]
    chunks += [(mlp_own, mlp_ref, r) for r in row_chunks(rows, MLP_ROWS)]
    return fills, chunks


def chunk_count(rows):
    return len(row_chunks(rows, ATTN_ROWS)) + len(row_chunks(rows, MLP_ROWS))


def gather_kernel(rest, small_ref, wq_ref, wo_ref, wu_ref, wd_ref, all_ref, attn_ref, mlp_ref, attn_own, mlp_own, load, send, recv):
    here = Place(rest)
    copies = Copies(load, send, recv)
    gather = Gather(here, copies, *shard_chunks(0, wq_ref, wo_ref, wu_ref, wd_ref, attn_own, mlp_own, attn_ref, mlp_ref))
    gather.fill()
    across = here.at(x=1, c=1)
    here.greet(across)
    spot = here.x * PLANES + here.c
    small = [copies.remote(small_ref, all_ref.at[spot], peer) for peer in (here.at(c=1), here.at(x=1), across)]
    keep = copies.local(small_ref, all_ref.at[spot])
    start(small + [keep])
    gather.begin()
    for _, event in gather.events():
        event()
    gather.finish()
    arrive(small)
    keep.wait()
    copies.drain()


def gather_shapes(rest, shards):
    rows, units = shards[2].shape[1:]
    shares = lax.axis_size("seq")
    widths = (4 * LANES, 2 * units)
    whole_shapes = [jax.ShapeDtypeStruct((LINE, rest, rows, shares * w), BF16) for w in widths]
    return whole_shapes, [pltpu.VMEM((rows, w), BF16) for w in widths]


def flat_rows(matrix):
    return matrix.reshape(-1, matrix.shape[-1])


def gather_weights(small, *shards):
    rest = lax.axis_size("dp") // LINE
    whole_shapes, own = gather_shapes(rest, shards)
    every = jax.ShapeDtypeStruct((lax.axis_size("seq"),) + small.shape, F32)
    every, attn, mlp = pl.pallas_call(
        functools.partial(gather_kernel, rest),
        in_specs=[ANY] * 5,
        out_specs=[ANY] * 3,
        out_shape=[every] + whole_shapes,
        scratch_shapes=own + gather_sems(chunk_count(shards[2].shape[1]), rest, 3),
        compiler_params=pltpu.CompilerParams(collective_id=0, has_side_effects=True),
        name="gather_weights",
    )(small, *shards)
    return every, flat_rows(attn), flat_rows(mlp)


def each(count, body):
    def step(i, carry):
        body(i)
        return carry

    lax.fori_loop(0, count, step, 0)


def plus(ref, at, *others):
    total = ref[at].astype(F32)
    for other in others:
        total = total + other.astype(F32)
    ref[at] = total.astype(BF16)


class Scatter:
    def __init__(self, here, copies, chunks):
        self.here, self.copies, self.items = here, copies, []
        z, u, x, c, rest = here.z, here.u, here.x, here.c, here.rest
        others = range(1, rest)
        for full, out, (at, rows), (acc, swap, x1, u1, x2, u2, line) in chunks:
            width = out.shape[1]
            half = rows // 2
            first, second, both = pl.ds(0, half), pl.ds(half, half), pl.ds(0, rows)
            whole_rows = pl.ds(at, rows)
            pair = [pl.ds(pl.multiple_of((c + d) % 2 * 2 * width, 2 * width), 2 * width) for d in range(2)]
            span = [pl.ds(pl.multiple_of((x + d) % 2 * width, width), width) for d in range(2)]
            every = slice(None)
            item = dict(out=out, rows=whole_rows, acc=acc, swap=swap, x1=x1, u1=u1, x2=x2, u2=u2, line=line)
            item.update(first=first, second=second, both=both, mine=span[0])
            item["own"] = copies.local(full.at[:, :, whole_rows, pair[0]], acc)
            item["to_c"] = [copies.remote(full.at[:, :, whole_rows, pair[1]], swap, here.at(c=1))]
            item["to_1"] = [copies.remote(acc.at[:, :, first, span[1]], x1, here.at(x=1))]
            for d in others:
                there = (u + d) % rest
                item["to_1"].append(copies.remote(acc.at[:, there, second, :], u1.at[d - 1], here.at(u=d)))
            item["to_2"] = [copies.remote(acc.at[:, u, second, span[1]], x2, here.at(x=1))]
            for d in others:
                there = (u + d) % rest
                item["to_2"].append(copies.remote(acc.at[:, there, first, span[0]], u2.at[d - 1], here.at(u=d)))
            item["to_z"] = [
                copies.remote(acc.at[(z + d) % LINE, u, both, span[0]], line.at[d - 1], here.at(z=d))
                for d in range(1, LINE)
            ]
            self.items.append(item)

    def load(self):
        for item in self.items:
            item["own"].start()

    def begin(self):
        for item in self.items:
            start(item["to_c"])

    def events(self):
        z, u, rest = self.here.z, self.here.u, self.here.rest
        others = range(1, rest)

        def one(item):
            item["own"].wait()
            arrive(item["to_c"])

            def add(i):
                a, b = i // rest, i % rest
                plus(item["acc"], (a, b), item["swap"][a, b])

            each(LINE * rest, add)
            start(item["to_1"])

        def two(item):
            arrive(item["to_1"])
            first, second, mine = item["first"], item["second"], item["mine"]

            def add(i):
                a, b = i // rest, i % rest
                plus(item["acc"], (a, b, first, mine), item["x1"][a, b])

            each(LINE * rest, add)

            def add_u(a):
                plus(item["acc"], (a, u, second), *(item["u1"][d - 1, a] for d in others))

            each(LINE, add_u)
            start(item["to_2"])

        def three(item):
            arrive(item["to_2"])
            first, second, mine = item["first"], item["second"], item["mine"]

            def add(a):
                plus(item["acc"], (a, u, second, mine), item["x2"][a])
                plus(item["acc"], (a, u, first, mine), *(item["u2"][d - 1, a] for d in others))

            each(LINE, add)
            start(item["to_z"])

        def four(item):
            arrive(item["to_z"])
            total = item["acc"][z, u, item["both"], item["mine"]].astype(F32)
            for d in range(1, LINE):
                total = total + item["line"][d - 1].astype(F32)
            item["out"][item["rows"], :] = total

        steps = (one, two, three, four)
        plan = schedule(len(self.items), ("c", 5.0), [("xy", 16.0), ("xy", 8.0), ("z", 15.0), None])
        return [(t, functools.partial(steps[s], self.items[k])) for t, s, k in plan]


def scatter_sems(chunks, rest, more=0):
    count = chunks * (LINE + 2 + 2 * (rest - 1)) + more
    return [pltpu.SemaphoreType.DMA((n,)) for n in (chunks + 1, count, count)]


def scatter_buffers(rest, rows, width):
    half = rows // 2
    shapes = (
        (LINE, rest, rows, 2 * width),
        (LINE, rest, rows, 2 * width),
        (LINE, rest, half, width),
        (rest - 1, LINE, half, 2 * width),
        (LINE, half, width),
        (rest - 1, LINE, half, width),
        (LINE - 1, rows, width),
    )
    return [pltpu.VMEM(s, BF16) for s in shapes]


def scatter_chunks(attn_ref, mlp_ref, attn_out, mlp_out, scratch):
    chunks, at = [], 0
    for matrix, out, least in ((mlp_ref, mlp_out, MLP_ROWS), (attn_ref, attn_out, ATTN_ROWS)):
        for rows in row_chunks(out.shape[0], least):
            chunks.append((matrix, out, rows, scratch[at : at + 7]))
            at += 7
    return chunks


def scatter_shapes(rest, attn, mlp):
    shares = lax.axis_size("seq")
    rows = attn.shape[0] // (LINE * rest)
    widths = [m.shape[1] // shares for m in (attn, mlp)]
    outs = [jax.ShapeDtypeStruct((rows, w), F32) for w in widths]
    operands = [m.reshape(LINE, rest, rows, -1) for m in (attn, mlp)]
    buffers = []
    for width, least in ((widths[1], MLP_ROWS), (widths[0], ATTN_ROWS)):
        for _, size in row_chunks(rows, least):
            buffers += scatter_buffers(rest, size, width)
    return operands, outs, buffers


def scatter_kernel(rest, *refs):
    small_ref, attn_ref, mlp_ref, sum_ref, attn_out, mlp_out, *scratch = refs
    *scratch, small_at, small_in, small_u, small_z, load, send, recv = scratch
    here = Place(rest)
    copies = Copies(load, send, recv)
    scatter = Scatter(here, copies, scatter_chunks(attn_ref, mlp_ref, attn_out, mlp_out, scratch))
    scatter.load()
    here.greet()
    keep = copies.local(small_ref, small_at.at[0])
    u, z = here.u, here.z
    to_c = [copies.remote(small_ref, small_in.at[0], here.at(c=1))]
    to_x = [copies.remote(small_at.at[1], small_in.at[1], here.at(x=1))]
    to_u = [copies.remote(small_u.at[u], small_u.at[u], here.at(u=d)) for d in range(1, rest)]
    to_z = [copies.remote(small_z.at[z], small_z.at[z], here.at(z=d)) for d in range(1, LINE)]
    start([keep] + to_c)
    scatter.begin()

    def one():
        keep.wait()
        arrive(to_c)
        small_at[1] = small_at[0] + small_in[0]
        start(to_x)

    def two():
        arrive(to_x)
        small_u[u] = small_at[1] + small_in[1]
        start(to_u)

    def three():
        arrive(to_u)
        total = small_u[0]
        for d in range(1, rest):
            total = total + small_u[d]
        small_z[z] = total
        start(to_z)

    def four():
        arrive(to_z)
        total = small_z[0]
        for d in range(1, LINE):
            total = total + small_z[d]
        sum_ref[...] = total

    little = [one, two, three, four]
    for _, event in scatter.events():
        event()
        if little:
            little.pop(0)()
    copies.drain()


def scatter_weights(small, attn, mlp):
    rest = lax.axis_size("dp") // LINE
    operands, outs, buffers = scatter_shapes(rest, attn, mlp)
    little = [pltpu.VMEM((n,) + small.shape, F32) for n in (2, 2, rest, LINE)]
    vmem = pl.BlockSpec(memory_space=pltpu.VMEM)
    return pl.pallas_call(
        functools.partial(scatter_kernel, rest),
        in_specs=[ANY] * 3,
        out_specs=[vmem] * 3,
        out_shape=[jax.ShapeDtypeStruct(small.shape, F32)] + outs,
        scratch_shapes=buffers + little + scatter_sems(len(buffers) // 7, rest, rest + LINE),
        compiler_params=pltpu.CompilerParams(collective_id=1, has_side_effects=True, vmem_limit_bytes=60000 * 1024),
        name="scatter_weights",
    )(small, *operands)


class Hooks:
    def __init__(self, images, points):
        self.images, self.points, self.table = images, points, {}
        self.image = pl.program_id(0)

    def place(self, share, event):
        slot = min(int(share * self.images * self.points), self.images * self.points - 1)
        self.table.setdefault(slot, []).append(event)

    def __call__(self, point):
        for slot in sorted(self.table):
            if slot % self.points == point:

                @pl.when(self.image == slot // self.points)
                def _(slot=slot):
                    for event in self.table[slot]:
                        event()


def compact(attn_ref, wq_ref, wo_ref):
    @pl.when(pl.program_id(0) == 0)
    def _():
        for g in range(wo_ref.shape[1] // LANES):
            at = 4 * LANES * g
            wq_ref[:, BLOCK * g : BLOCK * (g + 1)] = attn_ref[:, at : at + BLOCK]
            wo_ref[:, LANES * g : LANES * (g + 1)] = attn_ref[:, at + BLOCK : at + 4 * LANES]


def gather_hooks(hook, rest, layer, shards, wholes, attn_own, mlp_own, load, send, recv):
    here = Place(rest)
    copies = Copies(load, send, recv)
    gather = Gather(here, copies, *shard_chunks(layer, *shards, attn_own, mlp_own, *wholes))
    hook.place(0, gather.fill)
    hook.place(0, here.greet)
    hook.place(0, gather.begin)
    for due, event in gather.events():
        hook.place(due / 36.0, event)
    hook.place(1, gather.finish)
    hook.place(1, copies.drain)


def forward_kernel(images, last, following, rest, *refs):
    live_ref, x_ref, attn_ref, mlp_ref, bias_ref, mask_ref, perm_ref, back_ref, *refs = refs
    qvb_ref, upb_ref, gain_ref, shift_ref, outb_ref, *refs = refs
    shards, refs = (refs[:4], refs[4:]) if following else ((), refs)
    out_ref, xhat1_ref, inv1_ref, normed1_ref, qkv_ref, lse_ref, *refs = refs
    att_ref, xhat2_ref, inv2_ref, normed2_ref, hid_ref, slope_ref, *refs = refs
    wholes, refs = (refs[:2], refs[2:]) if following else ((), refs)
    pad_ref, wq_ref, wo_ref, *refs = refs
    hook = Hooks(images, 4)
    if following:
        gather_hooks(hook, rest, following, shards, wholes, *refs)
    hook(0)
    groups = wo_ref.shape[1] // LANES
    compact(attn_ref, wq_ref, wo_ref)
    x = x_ref[0].astype(F32)
    xhat, inverse = normalize(x)
    xhat1_ref[0] = xhat.astype(BF16)
    inv1_ref[0] = jnp.broadcast_to(inverse, (ROWS, LANES))
    normed = (xhat * gain_ref[0:1] + shift_ref[0:1]).astype(BF16)
    normed1_ref[0] = normed
    rolled = nn(perm_ref[...], normed).astype(BF16)
    qkv_ref[0] = (nn(rolled, wq_ref[...]) + qvb_ref[...]).astype(BF16)
    hook(1)

    def attend(g, carry):
        bias = bias_ref[g]
        for w in range(WINDOWS):
            rows = slice(KEYS * w, KEYS * (w + 1))
            query = qkv_ref[0, rows, cols(BLOCK * g, LANES)]
            key = qkv_ref[0, rows, cols(BLOCK * g + LANES, LANES)]
            val = qkv_ref[0, rows, cols(BLOCK * g + 2 * LANES, LANES)]
            scores = nt(key, spread_heads(query)) * SCALE + bias + mask_ref[w]
            top = jnp.max(scores, axis=0, keepdims=True)
            expo = jnp.exp(scores - top)
            total = jnp.sum(expo, axis=0, keepdims=True)
            probs = (expo * (1.0 / total)).astype(BF16)
            lse_ref[0, pl.ds(WINDOWS * g + w, 1), :] = top + jnp.log(total)
            pad_ref[rows, cols(LANES * g, LANES)] = join_heads(tn(probs, val)).astype(BF16)
        return carry

    lax.fori_loop(0, groups, attend, 0)
    hook(2)
    attended = nn(back_ref[...], pad_ref[...]).astype(BF16)
    att_ref[0] = attended
    middle = x + nt(attended, wo_ref[...]) + outb_ref[0:1]
    xhat, inverse = normalize(middle)
    xhat2_ref[0] = xhat.astype(BF16)
    inv2_ref[0] = jnp.broadcast_to(inverse, (ROWS, LANES))
    normed = (xhat * gain_ref[1:2] + shift_ref[1:2]).astype(BF16)
    normed2_ref[0] = normed
    total = middle + outb_ref[1:2]
    step = mlp_ref.shape[1] // (2 * groups)
    for c in range(groups):
        at = slice(step * c, step * (c + 1))
        pre = nn(normed, mlp_ref[:, 2 * step * c : 2 * step * c + step]) + upb_ref[:, at]
        half = 0.5 * (1.0 + lax.erf(pre * 0.7071067811865476))
        hidden = (pre * half).astype(BF16)
        hid_ref[0, :, at] = hidden
        slope_ref[0, :, at] = (half + pre * jnp.exp(-0.5 * pre * pre) * 0.3989422804014327).astype(BF16)
        total = total + nt(hidden, mlp_ref[:, 2 * step * c + step : 2 * step * (c + 1)])
    if last:
        total = total * live_ref[pl.program_id(0)]
    out_ref[0] = total.astype(out_ref.dtype)
    hook(3)


def norm_back(grad, xhat, inverse, gain):
    scaled = grad * gain
    first = row_mean(scaled)
    second = row_mean(scaled * xhat)
    return inverse * (scaled - first - xhat * second)


def add_rows(ref, row, value):
    ref[row : row + 1, : value.shape[1]] += jnp.sum(value, axis=0, keepdims=True)


def scatter_hooks(hook, rest, matrices, outs, scratch):
    here = Place(rest)
    *buffers, load, send, recv = scratch
    copies = Copies(load, send, recv)
    scatter = Scatter(here, copies, scatter_chunks(*matrices, *outs, buffers))
    hook.place(0, scatter.load)
    hook.place(0, here.greet)
    hook.place(0, scatter.begin)
    for due, event in scatter.events():
        hook.place(due / 44.0, event)
    hook.place(1, copies.drain)


def backward_kernel(images, first, following, rest, *refs):
    live_ref, g_ref, attn_ref, mlp_ref, bias_ref, mask_ref, perm_ref, back_ref, gain_ref, *refs = refs
    xhat1_ref, inv1_ref, qkv_ref, lse_ref, xhat2_ref, inv2_ref, slope_ref, *refs = refs
    normed1_ref, att_ref, normed2_ref, hid_ref, *refs = refs
    matrices, refs = (refs[:2], refs[2:]) if following else ((), refs)
    gout_ref, table_ref, small_ref, gattn_ref, gmlp_ref, *refs = refs
    outs, refs = (refs[:2], refs[2:]) if following else ((), refs)
    gap_ref, gpad_ref, wq_ref, wo_ref, gm_ref, gpre_ref, gp_ref, gqkv_ref, *refs = refs
    kept_n1, kept_att, kept_n2, kept_hid, sems, *refs = refs
    hook = Hooks(images, 4)
    if following:
        scatter_hooks(hook, rest, matrices, outs, refs)
    hook(0)
    groups = wo_ref.shape[1] // LANES
    image = pl.program_id(0)
    pairs = ((normed1_ref, kept_n1), (att_ref, kept_att), (normed2_ref, kept_n2), (hid_ref, kept_hid))
    loads = [pltpu.make_async_copy(src, dst, sems.at[k]) for k, (src, dst) in enumerate(pairs)]
    compact(attn_ref, wq_ref, wo_ref)

    @pl.when(image == 0)
    def _():
        table_ref[...] = jnp.zeros_like(table_ref)
        small_ref[...] = jnp.zeros_like(small_ref)
        for load in loads:
            load.start()

    g_res = g_ref[0].astype(F32)
    if first:
        g_res = g_res * live_ref[image]
    add_rows(small_ref, 5, g_res)
    g_m = g_res.astype(BF16)
    gm_ref[image] = g_m
    g_n2 = jnp.zeros_like(g_res)
    step = mlp_ref.shape[1] // (2 * groups)
    for c in range(groups):
        at = slice(step * c, step * (c + 1))
        down = mlp_ref[:, 2 * step * c + step : 2 * step * (c + 1)]
        g_pre = (nn(g_m, down) * slope_ref[0, :, at].astype(F32)).astype(BF16)
        gpre_ref[image, :, at] = g_pre
        add_rows(small_ref, 6 + c, g_pre.astype(F32))
        g_n2 = g_n2 + nt(g_pre, mlp_ref[:, 2 * step * c : 2 * step * c + step])
    hook(1)
    xhat = xhat2_ref[0].astype(F32)
    add_rows(small_ref, 2, g_n2 * xhat)
    add_rows(small_ref, 3, g_n2)
    g_mid = g_res + norm_back(g_n2, xhat, inv2_ref[0, :, 0:1], gain_ref[1:2])
    add_rows(small_ref, 4, g_mid)
    g_p = g_mid.astype(BF16)
    gp_ref[image] = g_p
    g_att = nn(g_p, wo_ref[...]).astype(BF16)
    gap_ref[...] = nn(perm_ref[...], g_att).astype(BF16)

    def attend(g, carry):
        bias = bias_ref[g]
        for w in range(WINDOWS):
            rows = slice(KEYS * w, KEYS * (w + 1))
            query = spread_heads(qkv_ref[0, rows, cols(BLOCK * g, LANES)])
            key = qkv_ref[0, rows, cols(BLOCK * g + LANES, LANES)]
            val = qkv_ref[0, rows, cols(BLOCK * g + 2 * LANES, LANES)]
            grad = spread_heads(gap_ref[rows, cols(LANES * g, LANES)])
            scores = nt(key, query) * SCALE + bias + mask_ref[w]
            probs = jnp.exp(scores - lse_ref[0, pl.ds(WINDOWS * g + w, 1), :])
            g_probs = nt(val, grad)
            g_vals = nn(probs.astype(BF16), grad)
            mean = jnp.sum(g_probs * probs, axis=0, keepdims=True)
            g_scores = (probs * (g_probs - mean)).astype(BF16)
            table_ref[g] += g_scores.astype(F32)
            g_keys = nn(g_scores, query) * SCALE
            g_queries = join_heads(tn(g_scores, key)) * SCALE
            gpad_ref[rows, cols(BLOCK * g, LANES)] = g_queries.astype(BF16)
            gpad_ref[rows, cols(BLOCK * g + LANES, LANES)] = g_keys.astype(BF16)
            gpad_ref[rows, cols(BLOCK * g + 2 * LANES, LANES)] = g_vals.astype(BF16)
        return carry

    hook(2)
    lax.fori_loop(0, groups, attend, 0)
    hook(3)
    g_qkv = nn(back_ref[...], gpad_ref[...]).astype(BF16)
    gqkv_ref[image] = g_qkv
    for g in range(groups):
        for row, at in ((10, BLOCK * g), (11, BLOCK * g + 2 * LANES)):
            part = g_qkv[:, at : at + LANES].astype(F32)
            small_ref[row : row + 1, LANES * g : LANES * (g + 1)] += jnp.sum(part, axis=0, keepdims=True)
    g_n1 = nt(g_qkv, wq_ref[...])
    xhat = xhat1_ref[0].astype(F32)
    add_rows(small_ref, 0, g_n1 * xhat)
    add_rows(small_ref, 1, g_n1)
    gout_ref[0] = g_mid + norm_back(g_n1, xhat, inv1_ref[0, :, 0:1], gain_ref[0:1])

    @pl.when(image == pl.num_programs(0) - 1)
    def _():
        for load in loads:
            load.wait()
        flat = lambda ref: ref.reshape(ref.shape[0] * ref.shape[1], ref.shape[2])

        def product(left_ref, right_ref, size, out_ref, stride, start):
            left = flat(left_ref)[...].T
            for g in range(groups):
                right = flat(right_ref)[:, size * g : size * (g + 1)]
                at = stride * g + start
                out_ref[:, at : at + size] = nn(left, right).astype(BF16)

        product(gm_ref, kept_hid, step, gmlp_ref, 2 * step, step)
        product(kept_n2, gpre_ref, step, gmlp_ref, 2 * step, 0)
        product(gp_ref, kept_att, LANES, gattn_ref, 4 * LANES, BLOCK)
        product(kept_n1, gqkv_ref, BLOCK, gattn_ref, 4 * LANES, 0)


def whole(array):
    zeros = (0,) * array.ndim
    return pl.BlockSpec(array.shape, lambda i: zeros, pipeline_mode=pl.Buffered(1))


def per_image(shape):
    tail = (0,) * (len(shape) - 1)
    return pl.BlockSpec((1,) + tuple(shape[1:]), lambda i: (i,) + tail)


def fixed(shape):
    zeros = (0,) * len(shape)
    return pl.BlockSpec(shape, lambda i: zeros)


def params(**more):
    return pltpu.CompilerParams(dimension_semantics=("arbitrary",), vmem_limit_bytes=60000 * 1024, **more)


def forward_layer(layer, layers, live, x, attn, mlp, tables, rows, shards):
    images = x.shape[0]
    width, units = attn.shape[0], mlp.shape[1] // 2
    groups = width // LANES
    total = groups * BLOCK
    last = layer == layers - 1
    shapes = [
        ((images, ROWS, width), BF16 if last else F32),
        ((images, ROWS, width), BF16),
        ((images, ROWS, LANES), F32),
        ((images, ROWS, width), BF16),
        ((images, PADDED, total), BF16),
        ((images, groups * WINDOWS, WIDE), F32),
        ((images, ROWS, width), BF16),
        ((images, ROWS, width), BF16),
        ((images, ROWS, LANES), F32),
        ((images, ROWS, width), BF16),
        ((images, ROWS, units), BF16),
        ((images, ROWS, units), BF16),
    ]
    fixed_args = (attn, mlp, *tables, *rows)
    rest = lax.axis_size("dp") // LINE
    extra_shapes, own, sems, more = [], [], [], {}
    if last:
        shards = ()
    else:
        extra_shapes, own = gather_shapes(rest, shards)
        sems = gather_sems(chunk_count(shards[2].shape[1]), rest)
        more = dict(collective_id=2 + layer, has_side_effects=True)
    result = pl.pallas_call(
        functools.partial(forward_kernel, images, last, 0 if last else layer + 1, rest),
        grid=(images,),
        in_specs=[SMEM, per_image(x.shape)] + [whole(a) for a in fixed_args] + [ANY] * len(shards),
        out_specs=[per_image(s) for s, _ in shapes] + [ANY] * len(extra_shapes),
        out_shape=[jax.ShapeDtypeStruct(s, d) for s, d in shapes] + extra_shapes,
        scratch_shapes=[
            pltpu.VMEM((PADDED, width), BF16),
            pltpu.VMEM((width, total), BF16),
            pltpu.VMEM((width, width), BF16),
        ]
        + own
        + sems,
        compiler_params=params(**more),
        name="forward_layer",
    )(live, x, *fixed_args, *shards)
    return result[: len(shapes)], [flat_rows(m) for m in result[len(shapes) :]]


def backward_layer(layer, layers, live, g, attn, mlp, tables, gain, saved, operands, following):
    images = g.shape[0]
    width, units = attn.shape[0], mlp.shape[1] // 2
    groups = width // LANES
    total = groups * BLOCK
    sums = [((groups, KEYS, WIDE), F32), ((16, width), F32), (attn.shape, BF16), (mlp.shape, BF16)]
    fixed_args = (attn, mlp, *tables, gain)
    rest = lax.axis_size("dp") // LINE
    matrices, outs, buffers, more = [], [], [], {}
    if following:
        matrices, outs, buffers = scatter_shapes(rest, *following)
        buffers = buffers + scatter_sems(len(buffers) // 7, rest)
        more = dict(collective_id=2 + layers + layer, has_side_effects=True)
    result = pl.pallas_call(
        functools.partial(backward_kernel, images, layer == layers - 1, bool(following), rest),
        grid=(images,),
        in_specs=[SMEM, per_image(g.shape)]
        + [whole(a) for a in fixed_args]
        + [per_image(a.shape) for a in saved]
        + [ANY] * (len(operands) + len(matrices)),
        out_specs=[per_image(g.shape)] + [fixed(s) for s, _ in sums] + [fixed(o.shape) for o in outs],
        out_shape=[jax.ShapeDtypeStruct(g.shape, F32)] + [jax.ShapeDtypeStruct(s, d) for s, d in sums] + outs,
        scratch_shapes=[
            pltpu.VMEM((PADDED, width), BF16),
            pltpu.VMEM((PADDED, total), BF16),
            pltpu.VMEM((width, total), BF16),
            pltpu.VMEM((width, width), BF16),
            pltpu.VMEM((images, ROWS, width), BF16),
            pltpu.VMEM((images, ROWS, units), BF16),
            pltpu.VMEM((images, ROWS, width), BF16),
            pltpu.VMEM((images, ROWS, total), BF16),
        ]
        + [pltpu.VMEM(a.shape, a.dtype) for a in operands]
        + [pltpu.SemaphoreType.DMA((len(operands),))]
        + buffers,
        compiler_params=params(**more),
        name="backward_layer",
    )(live, g, *fixed_args, *saved, *operands, *matrices)
    return result[:5], result[5:]


def to_rows(images):
    slots, width = images.shape[0], images.shape[3]
    flat = jnp.transpose(images, (0, 2, 1, 3)).reshape(slots, TOKENS, width)
    return jnp.pad(flat, ((0, 0), (0, ROWS - TOKENS), (0, 0)))


def from_rows(rows):
    slots, width = rows.shape[0], rows.shape[2]
    return jnp.transpose(rows[:, :TOKENS].reshape(slots, PLACES, WINDOWS, width), (0, 2, 1, 3))


def local(
    activations,
    counts,
    w_qkv,
    w_out,
    w_up,
    w_down,
    qv_bias,
    rel_table,
    up_bias,
    norm_gain,
    norm_bias,
    out_bias,
    cotangent,
):
    slots, width = activations.shape[0], activations.shape[3]
    layers = w_qkv.shape[0]
    shares = lax.axis_size("seq")
    seq = lax.axis_index("seq")
    spot = seq % PLANES * 2 + seq // PLANES
    units = w_up.shape[2]
    heads = rel_table.shape[2]
    live = (seq * slots + jnp.arange(slots) < counts[0]).astype(F32)
    onehot = jnp.asarray(place_onehot())

    table = jnp.pad(jnp.transpose(rel_table, (0, 2, 1)), ((0, 0), (0, 0), (0, 2 * LANES - 169)))
    pieces = [p.astype(F32).reshape(-1, LANES) for p in (qv_bias, up_bias, table)]
    at = np.cumsum([0] + [p.shape[0] for p in pieces])
    shards = (
        jnp.transpose(w_qkv, (0, 2, 1, 3)),
        jnp.transpose(w_out, (0, 2, 1)),
        w_up,
        jnp.transpose(w_down, (0, 2, 1)),
    )
    every, *matrices = gather_weights(jnp.concatenate(pieces), *shards)
    every = jnp.stack([every[PLANES * (p % 2) + p // 2] for p in range(shares)])
    all_qv = every[:, at[0] : at[1]].reshape(shares, layers, 2, LANES)
    all_up = every[:, at[1] : at[2]].reshape(shares, layers, units)
    all_table = every[:, at[2] : at[3]].reshape(shares, layers, heads, 2 * LANES)[..., :169]

    tables, rows = [], []
    for layer in range(layers):
        perm, mask = place_tables(3 if layer % 2 == 1 else 0)
        lookup = jnp.dot(
            onehot, all_table[:, layer].reshape(-1, 169).T, precision=lax.Precision.HIGHEST
        ).reshape(KEYS, KEYS, -1, PER_GROUP)
        bias = jnp.transpose(lookup, (2, 0, 3, 1)).reshape(-1, KEYS, WIDE)
        tables.append((bias, jnp.asarray(mask), jnp.asarray(perm, BF16), jnp.asarray(perm.T, BF16)))
        qv = all_qv[:, layer]
        qvb = jnp.stack([qv[:, 0], jnp.zeros_like(qv[:, 0]), qv[:, 1]], axis=1).reshape(1, -1)
        upb = all_up[:, layer].reshape(1, -1)
        rows.append((qvb, upb, norm_gain[layer], norm_bias[layer], out_bias[layer]))

    residual = to_rows(activations)
    saved, weights = [], []
    for layer in range(layers):
        weights.append(matrices)
        (residual, *kept), matrices = forward_layer(
            layer, layers, live, residual, *matrices, tables[layer], rows[layer], shards
        )
        saved.append(kept)
    out = from_rows(residual)

    grad = to_rows(cotangent)
    smalls, grads, partial = [None] * layers, [None] * layers, ()
    for layer in reversed(range(layers)):
        xhat1, inv1, normed1, qkv, lse, att, xhat2, inv2, normed2, hid, slope = saved[layer]
        (grad, table, small, *partial), sums = backward_layer(
            layer,
            layers,
            live,
            grad,
            *weights[layer],
            tables[layer],
            norm_gain[layer],
            (xhat1, inv1, qkv, lse, xhat2, inv2, slope),
            (normed1, att, normed2, hid),
            partial,
        )
        if layer < layers - 1:
            grads[layer + 1] = sums
        per_head = jnp.transpose(table.reshape(-1, KEYS, PER_GROUP, KEYS), (0, 2, 1, 3)).reshape(-1, KEYS * KEYS)
        grad_table = jnp.dot(per_head, onehot, precision=lax.Precision.HIGHEST)
        grad_table = jnp.pad(grad_table, ((0, 0), (0, 2 * LANES - 169))).reshape(-1, width)
        smalls[layer] = jnp.concatenate([small, grad_table])

    total, *grads[0] = scatter_weights(jnp.stack(smalls), *partial)
    grad_attn, grad_mlp = (jnp.stack(g) for g in zip(*grads))
    mine = lambda value, axis, size: lax.dynamic_slice_in_dim(value, spot * size, size, axis)
    grad_table = mine(total[:, 16:].reshape(layers, -1, 2 * LANES), 1, heads)[..., :169]
    return (
        out,
        from_rows(grad),
        jnp.transpose(grad_attn[..., :BLOCK].reshape(layers, -1, 3, LANES), (0, 1, 2, 3)),
        jnp.transpose(grad_attn[..., BLOCK:], (0, 2, 1)),
        grad_mlp[..., :units],
        jnp.transpose(grad_mlp[..., units:], (0, 2, 1)),
        mine(total[:, 10:12], 2, LANES),
        jnp.transpose(grad_table, (0, 2, 1)),
        mine(total[:, 6:10], 1, 1)[:, 0],
        total[:, 0:3:2],
        total[:, 1:4:2],
        total[:, 4:6],
    )


def solution(mesh):
    slots = P(("dp", "seq"), None, None, None)
    return jax.shard_map(
        local,
        mesh=mesh,
        in_specs=(
            slots,
            P("dp"),
            P(None, "dp", None, "seq"),
            P(None, "seq", "dp"),
            P(None, "dp", "seq"),
            P(None, "seq", "dp"),
            P(None, None, "seq"),
            P(None, None, "seq"),
            P(None, "seq"),
            P(),
            P(),
            P(),
            slots,
        ),
        out_specs=(
            slots,
            slots,
            P(None, "dp", None, "seq"),
            P(None, "seq", "dp"),
            P(None, "dp", "seq"),
            P(None, "seq", "dp"),
            P(None, None, "seq"),
            P(None, None, "seq"),
            P(None, "seq"),
            P(),
            P(),
            P(),
        ),
        check_vma=False,
    )
```

```python
import functools

import jax
import jax.numpy as jnp
import numpy as np
from jax import lax
from jax.experimental import pallas as pl
from jax.experimental.pallas import tpu as pltpu
from jax.sharding import PartitionSpec as P

EPS = 1e-05
F32 = jnp.float32
BF16 = jnp.bfloat16
SIDE = 7
GRID = 14
PLACES = 49
WINDOWS = 4
TOKENS = PLACES * WINDOWS
ROWS = 208
KEYS = 64
PADDED = WINDOWS * KEYS
HEAD = 32
LANES = 128
PER_GROUP = LANES // HEAD
WIDE = PER_GROUP * KEYS
BLOCK = 3 * LANES
SCALE = HEAD**-0.5
TABLE = 169
CENTRE = 84
SPREAD = 88
GAP = 2 * LANES - TABLE


def place_tables(shift):
    perm = np.zeros((PADDED, ROWS), np.float32)
    region = np.zeros((WINDOWS, PLACES), np.int64)
    for w in range(WINDOWS):
        for p in range(PLACES):
            row, col = SIDE * (w // 2) + p // SIDE, SIDE * (w % 2) + p % SIDE
            band = [int(v >= 7) + int(v >= 11) for v in (row, col)]
            region[w, p] = 3 * band[0] + band[1]
            row, col = (row + shift) % GRID, (col + shift) % GRID
            source_w = 2 * (row // SIDE) + col // SIDE
            source_p = SIDE * (row % SIDE) + col % SIDE
            perm[KEYS * w + p, WINDOWS * source_p + source_w] = 1.0
    mask = np.where(region[:, :, None] == region[:, None, :], 0.0, -100.0)
    mask = np.pad(mask, ((0, 0), (0, KEYS - PLACES), (0, KEYS - PLACES))).astype(np.float32)
    return perm, np.tile(mask, (1, 1, PER_GROUP))


def spread_tables():
    rows = np.zeros((2, KEYS, SPREAD), np.float32)
    columns = np.zeros((2, LANES, LANES), np.float32)
    for p in range(PLACES):
        wide = 13 * (p // SIDE) + p % SIDE
        rows[0, p, wide] = 1.0
        rows[1, p, CENTRE - wide] = 1.0
        columns[0, wide, p] = 1.0
        columns[1, wide, KEYS + p] = 1.0
    return jnp.asarray(rows), jnp.asarray(columns)


def nn(a, b):
    return lax.dot_general(a, b, (((1,), (0,)), ((), ())), preferred_element_type=F32)


def nt(a, b):
    return lax.dot_general(a, b, (((1,), (1,)), ((), ())), preferred_element_type=F32)


def tn(a, b):
    return lax.dot_general(a, b, (((0,), (0,)), ((), ())), preferred_element_type=F32)


def exact(a, b, contract):
    return lax.dot_general(
        a, b, (contract, ((), ())), precision=lax.Precision.HIGHEST, preferred_element_type=F32
    )


def head_bias(table_row, rows_ref, columns_ref, out_ref):
    picked = []
    for h in range(PER_GROUP):
        wide = jnp.broadcast_to(table_row(h), (SPREAD, 2 * LANES))
        wide = pltpu.roll(wide, 0, 1, stride=1, stride_axis=0)[:, :LANES]
        picked.append(exact(rows_ref[0], wide, ((1,), (0,))))
    pad = lax.broadcasted_iota(jnp.int32, (KEYS, LANES), 0) >= PLACES
    for c in range(PER_GROUP // 2):
        even = exact(picked[2 * c], columns_ref[0], ((1,), (0,)))
        odd = exact(picked[2 * c + 1], columns_ref[1], ((1,), (0,)))
        out_ref[:, LANES * c : LANES * (c + 1)] = jnp.where(pad, -1e30, even + odd)


def table_grad(grads, rows_ref, columns_ref):
    tables = []
    for h in range(PER_GROUP):
        part = grads[:, LANES * (h // 2) : LANES * (h // 2 + 1)]
        wide = exact(part, columns_ref[h % 2], ((1,), (1,)))
        wide = exact(rows_ref[1], wide, ((0,), (0,)))
        wide = jnp.concatenate([wide, jnp.zeros((SPREAD, LANES), F32)], axis=1)
        wide = pltpu.roll(wide, 0, 1, stride=1, stride_axis=0)
        tables.append(jnp.sum(wide, axis=0, keepdims=True))
    return tables


def row_mean(value):
    return jnp.sum(value, axis=-1, keepdims=True) * (1.0 / value.shape[-1])


def normalize(value):
    centered = value - row_mean(value)
    inverse = lax.rsqrt(row_mean(centered * centered) + EPS)
    return centered * inverse, inverse


def spread_heads(tile):
    head = lax.broadcasted_iota(jnp.int32, tile.shape, 1) // HEAD
    zero = jnp.zeros_like(tile)
    return jnp.concatenate([jnp.where(head == h, tile, zero) for h in range(PER_GROUP)], axis=0)


def join_heads(wide):
    head = lax.broadcasted_iota(jnp.int32, (KEYS, LANES), 1) // HEAD
    total = wide[:KEYS]
    for h in range(1, PER_GROUP):
        total = jnp.where(head == h, wide[KEYS * h : KEYS * (h + 1)], total)
    return total


def cols(at, size):
    return pl.ds(pl.multiple_of(at, LANES), size)


SMEM = pl.BlockSpec(memory_space=pltpu.SMEM)
ANY = pl.BlockSpec(memory_space=pl.ANY)

MESH = pl.DeviceIdType.MESH
LINE = 4
PLANES = 2


class Place:
    def __init__(self, rest):
        dp, seq = lax.axis_index("dp"), lax.axis_index("seq")
        self.rest = rest
        self.z, self.u = dp // rest, dp % rest
        self.x, self.c = seq // PLANES, seq % PLANES

    def at(self, z=0, u=0, x=0, c=0):
        dp = (self.z + z) % LINE * self.rest + (self.u + u) % self.rest
        return (dp, (self.x + x) % 2 * PLANES + (self.c + c) % 2)

    def greet(self, *more):
        near = [self.at(z=k) for k in range(1, LINE)] + [self.at(u=k) for k in range(1, self.rest)]
        peers = near + [self.at(x=1), self.at(c=1), *more]
        barrier = pltpu.get_barrier_semaphore()
        for peer in peers:
            pl.semaphore_signal(barrier, inc=1, device_id=peer, device_id_type=MESH)
        pl.semaphore_wait(barrier, len(peers))


class Copies:
    def __init__(self, load, send, recv):
        self.load, self.send, self.recv = load, send, recv
        self.loads, self.sent = 0, []

    def local(self, src, dst):
        self.loads += 1
        return pltpu.make_async_copy(src, dst, self.load.at[self.loads - 1])

    def remote(self, src, dst, peer):
        at = len(self.sent)
        copy = pltpu.make_async_remote_copy(
            src_ref=src,
            dst_ref=dst,
            send_sem=self.send.at[at],
            recv_sem=self.recv.at[at],
            device_id=peer,
            device_id_type=MESH,
        )
        self.sent.append(copy)
        return copy

    def drain(self):
        for copy in self.sent:
            copy.wait_send()


def start(copies):
    for copy in copies:
        copy.start()


def arrive(copies):
    for copy in copies:
        copy.wait_recv()


def schedule(count, begin, steps, lag=3.0):
    free, ready, plan = {}, [(0.0, k, 0) for k in range(count)], []
    transfers = [begin, *steps]
    while ready:
        ready.sort()
        now, k, s = ready.pop(0)
        if s > 0:
            plan.append((now, s - 1, k))
        if s < len(transfers) and transfers[s]:
            link, total = transfers[s]
            free[link] = max(free.get(link, 0.0), now) + total / count
            ready.append((free[link] + lag, k, s + 1))
    return plan


def row_chunks(rows, least):
    count = max(1, rows // least)
    size = rows // count
    return [(k * size, size) for k in range(count)]


ATTN_ROWS, MLP_ROWS = 32, 16


class Gather:
    def __init__(self, here, copies, fills, chunks):
        self.copies, self.items = copies, []
        self.fills = [copies.local(a, b) for a, b in fills]
        z, u, x, c, rest = here.z, here.u, here.x, here.c, here.rest
        others = range(1, rest)
        for own, full, (at, rows) in chunks:
            width = own.shape[1]
            half = rows // 2
            first, second, both = pl.ds(at, half), pl.ds(at + half, half), pl.ds(at, rows)
            span = [pl.ds(pl.multiple_of((c * 2 + (x + d) % 2) * width, width), width) for d in range(2)]
            pair = pl.ds(pl.multiple_of(c * 2 * width, 2 * width), 2 * width)

            def send(index, **offset):
                return copies.remote(full.at[index], full.at[index], here.at(**offset))

            mine = full.at[z, u, both, span[0]]
            shard = own.at[both, :]
            item = dict(
                local=[copies.local(shard, mine)],
                line=[copies.remote(shard, mine, here.at(z=d)) for d in range(1, LINE)],
            )
            every = slice(None)
            item["a1"] = [send((every, u, first, span[0]), x=1)]
            item["b1"] = [send((every, u, second, span[0]), u=d) for d in others]
            item["d1"] = [send((every, u, both, span[0]), c=1)]
            item["a2"] = [send((every, u, first, pair), u=d) for d in others]
            item["b2"] = [send((every, every, second, span[0]), x=1)]
            item["d2"] = [send((every, u, first, span[1]), c=1)]
            item["d2"] += [send((every, (u + d) % rest, second, span[0]), c=1) for d in others]
            item["d3"] = [send((every, (u + d) % rest, first, pair), c=1) for d in others]
            item["d3"] += [send((every, every, second, span[1]), c=1)]
            self.items.append(item)

    def fill(self):
        start(self.fills)

    def begin(self):
        for copy in self.fills:
            copy.wait()
        for item in self.items:
            start(item["local"] + item["line"])

    def events(self):
        def one(item):
            item["local"][0].wait()
            arrive(item["line"])
            start(item["a1"] + item["b1"] + item["d1"])

        def two(item):
            arrive(item["a1"])
            start(item["a2"])
            arrive(item["b1"])
            start(item["b2"] + item["d2"])

        def three(item):
            arrive(item["a2"] + item["b2"])
            start(item["d3"])

        steps = (one, two, three)
        plan = schedule(len(self.items), ("z", 15.0), [("xy", 8.0), ("xy", 16.0), None])
        return [(t, functools.partial(steps[s], self.items[k])) for t, s, k in plan]

    def finish(self):
        for item in self.items:
            arrive(item["d1"] + item["d2"] + item["d3"])


def gather_sems(chunks, rest, more=0):
    count = chunks * (LINE + 4 + 4 * (rest - 1)) + more
    return [pltpu.SemaphoreType.DMA((n,)) for n in (chunks + 7, count, count)]


def shard_chunks(layer, wq_ref, wo_ref, wu_ref, wd_ref, attn_own, mlp_own, attn_ref, mlp_ref):
    units = wu_ref.shape[2]
    part = lambda ref, at, size: ref.at[:, pl.ds(at, size)]
    fills = [(wq_ref.at[layer, t], part(attn_own, LANES * t, LANES)) for t in range(3)]
    fills += [(wo_ref.at[layer], part(attn_own, BLOCK, LANES))]
    fills += [(wu_ref.at[layer], part(mlp_own, 0, units)), (wd_ref.at[layer], part(mlp_own, units, units))]
    rows = attn_own.shape[0]
    chunks = [(attn_own, attn_ref, r) for r in row_chunks(rows, ATTN_ROWS)]
    chunks += [(mlp_own, mlp_ref, r) for r in row_chunks(rows, MLP_ROWS)]
    return fills, chunks


def chunk_count(rows):
    return len(row_chunks(rows, ATTN_ROWS)) + len(row_chunks(rows, MLP_ROWS))


def gather_kernel(rest, layers, *refs):
    small_ref, rows_ref, columns_ref, wq_ref, wo_ref, wu_ref, wd_ref, *refs = refs
    qvb_ref, upb_ref, bias_ref, attn_ref, mlp_ref, *refs = refs
    all_ref, attn_own, mlp_own, load, send, recv = refs
    here = Place(rest)
    copies = Copies(load, send, recv)
    chunks = shard_chunks(0, wq_ref, wo_ref, wu_ref, wd_ref, attn_own, mlp_own, attn_ref, mlp_ref)
    gather = Gather(here, copies, *chunks)
    gather.fill()
    across = here.at(x=1, c=1)
    here.greet(across)
    spot = here.x * PLANES + here.c
    small = [copies.remote(small_ref, all_ref.at[spot], peer) for peer in (here.at(c=1), here.at(x=1), across)]
    keep = copies.local(small_ref, all_ref.at[spot])
    start(small + [keep])
    gather.begin()
    groups = all_ref.shape[0]
    units = upb_ref.shape[2] // groups

    def biases():
        arrive(small)
        keep.wait()
        qvb_ref[...] = jnp.zeros_like(qvb_ref)
        for l in range(layers):
            for g in range(groups):
                seq = PLANES * (g % 2) + g // 2
                at = BLOCK * g
                qvb_ref[l, :, at : at + LANES] = all_ref[seq, 2 * l : 2 * l + 1]
                qvb_ref[l, :, at + 2 * LANES : at + BLOCK] = all_ref[seq, 2 * l + 1 : 2 * l + 2]
                for i in range(units // LANES):
                    row = 2 * layers + units // LANES * l + i
                    at = units * g + LANES * i
                    upb_ref[l, :, at : at + LANES] = all_ref[seq, row : row + 1]

    def group_bias(l, g):
        seq = PLANES * (g % 2) + g // 2

        def table_row(h):
            row = (2 + units // LANES) * layers + 2 * (PER_GROUP * l + h)
            return jnp.concatenate([all_ref[seq, row : row + 1], all_ref[seq, row + 1 : row + 2]], axis=1)

        head_bias(table_row, rows_ref, columns_ref, bias_ref.at[l, g])

    beside = [biases] + [functools.partial(group_bias, l, g) for l in range(layers) for g in range(groups)]
    for _, event in gather.events():
        event()
        if beside:
            beside.pop(0)()
    for step in beside:
        step()
    gather.finish()
    copies.drain()


def gather_shapes(rest, shards):
    rows, units = shards[2].shape[1:]
    shares = lax.axis_size("seq")
    widths = (4 * LANES, 2 * units)
    whole_shapes = [jax.ShapeDtypeStruct((LINE, rest, rows, shares * w), BF16) for w in widths]
    return whole_shapes, [pltpu.VMEM((rows, w), BF16) for w in widths]


def flat_rows(matrix):
    return matrix.reshape(-1, matrix.shape[-1])


def gather_weights(small, layers, *shards):
    rest = lax.axis_size("dp") // LINE
    groups = lax.axis_size("seq")
    whole_shapes, own = gather_shapes(rest, shards)
    units = shards[2].shape[2]
    rows, columns = spread_tables()
    tables = [(layers, 1, groups * BLOCK), (layers, 1, groups * units), (layers, groups, KEYS, WIDE)]
    vmem = pl.BlockSpec(memory_space=pltpu.VMEM)
    *tables, attn, mlp = pl.pallas_call(
        functools.partial(gather_kernel, rest, layers),
        in_specs=[ANY, vmem, vmem] + [ANY] * 4,
        out_specs=[vmem] * 3 + [ANY] * 2,
        out_shape=[jax.ShapeDtypeStruct(t, F32) for t in tables] + whole_shapes,
        scratch_shapes=[pltpu.VMEM((groups,) + small.shape, F32)]
        + own
        + gather_sems(chunk_count(shards[2].shape[1]), rest, 3),
        compiler_params=pltpu.CompilerParams(collective_id=0, has_side_effects=True),
        name="gather_weights",
    )(small, rows, columns, *shards)
    return *tables, flat_rows(attn), flat_rows(mlp)


def each(count, body):
    def step(i, carry):
        body(i)
        return carry

    lax.fori_loop(0, count, step, 0)


def plus(ref, at, *others):
    total = ref[at].astype(F32)
    for other in others:
        total = total + other.astype(F32)
    ref[at] = total.astype(BF16)


class Scatter:
    def __init__(self, here, copies, chunks):
        self.here, self.copies, self.items = here, copies, []
        z, u, x, c, rest = here.z, here.u, here.x, here.c, here.rest
        others = range(1, rest)
        for full, out, (at, rows), (acc, swap, x1, u1, x2, u2, line) in chunks:
            width = out.shape[1]
            half = rows // 2
            first, second, both = pl.ds(0, half), pl.ds(half, half), pl.ds(0, rows)
            whole_rows = pl.ds(at, rows)
            pair = [pl.ds(pl.multiple_of((c + d) % 2 * 2 * width, 2 * width), 2 * width) for d in range(2)]
            span = [pl.ds(pl.multiple_of((x + d) % 2 * width, width), width) for d in range(2)]
            every = slice(None)
            item = dict(out=out, rows=whole_rows, acc=acc, swap=swap, x1=x1, u1=u1, x2=x2, u2=u2, line=line)
            item.update(first=first, second=second, both=both, mine=span[0])
            item["own"] = copies.local(full.at[:, :, whole_rows, pair[0]], acc)
            item["to_c"] = [copies.remote(full.at[:, :, whole_rows, pair[1]], swap, here.at(c=1))]
            item["to_1"] = [copies.remote(acc.at[:, :, first, span[1]], x1, here.at(x=1))]
            for d in others:
                there = (u + d) % rest
                item["to_1"].append(copies.remote(acc.at[:, there, second, :], u1.at[d - 1], here.at(u=d)))
            item["to_2"] = [copies.remote(acc.at[:, u, second, span[1]], x2, here.at(x=1))]
            for d in others:
                there = (u + d) % rest
                item["to_2"].append(copies.remote(acc.at[:, there, first, span[0]], u2.at[d - 1], here.at(u=d)))
            item["to_z"] = [
                copies.remote(acc.at[(z + d) % LINE, u, both, span[0]], line.at[d - 1], here.at(z=d))
                for d in range(1, LINE)
            ]
            self.items.append(item)

    def load(self):
        for item in self.items:
            item["own"].start()

    def begin(self):
        for item in self.items:
            start(item["to_c"])

    def events(self):
        z, u, rest = self.here.z, self.here.u, self.here.rest
        others = range(1, rest)

        def one(item):
            item["own"].wait()
            arrive(item["to_c"])

            def add(i):
                a, b = i // rest, i % rest
                plus(item["acc"], (a, b), item["swap"][a, b])

            each(LINE * rest, add)
            start(item["to_1"])

        def two(item):
            arrive(item["to_1"])
            first, second, mine = item["first"], item["second"], item["mine"]

            def add(i):
                a, b = i // rest, i % rest
                plus(item["acc"], (a, b, first, mine), item["x1"][a, b])

            each(LINE * rest, add)

            def add_u(a):
                plus(item["acc"], (a, u, second), *(item["u1"][d - 1, a] for d in others))

            each(LINE, add_u)
            start(item["to_2"])

        def three(item):
            arrive(item["to_2"])
            first, second, mine = item["first"], item["second"], item["mine"]

            def add(a):
                plus(item["acc"], (a, u, second, mine), item["x2"][a])
                plus(item["acc"], (a, u, first, mine), *(item["u2"][d - 1, a] for d in others))

            each(LINE, add)
            start(item["to_z"])

        def four(item):
            arrive(item["to_z"])
            total = item["acc"][z, u, item["both"], item["mine"]].astype(F32)
            for d in range(1, LINE):
                total = total + item["line"][d - 1].astype(F32)
            item["out"][item["rows"], :] = total

        steps = (one, two, three, four)
        plan = schedule(len(self.items), ("c", 5.0), [("xy", 16.0), ("xy", 8.0), ("z", 15.0), None])
        return [(t, functools.partial(steps[s], self.items[k])) for t, s, k in plan]


def scatter_sems(chunks, rest, more=0):
    count = chunks * (LINE + 2 + 2 * (rest - 1)) + more
    return [pltpu.SemaphoreType.DMA((n,)) for n in (chunks + 1, count, count)]


def scatter_buffers(rest, rows, width):
    half = rows // 2
    shapes = (
        (LINE, rest, rows, 2 * width),
        (LINE, rest, rows, 2 * width),
        (LINE, rest, half, width),
        (rest - 1, LINE, half, 2 * width),
        (LINE, half, width),
        (rest - 1, LINE, half, width),
        (LINE - 1, rows, width),
    )
    return [pltpu.VMEM(s, BF16) for s in shapes]


def scatter_chunks(attn_ref, mlp_ref, attn_out, mlp_out, scratch):
    chunks, at = [], 0
    for matrix, out, least in ((mlp_ref, mlp_out, MLP_ROWS), (attn_ref, attn_out, ATTN_ROWS)):
        for rows in row_chunks(out.shape[0], least):
            chunks.append((matrix, out, rows, scratch[at : at + 7]))
            at += 7
    return chunks


def scatter_shapes(rest, attn, mlp):
    shares = lax.axis_size("seq")
    rows = attn.shape[0] // (LINE * rest)
    widths = [m.shape[1] // shares for m in (attn, mlp)]
    outs = [jax.ShapeDtypeStruct((rows, w), F32) for w in widths]
    operands = [m.reshape(LINE, rest, rows, -1) for m in (attn, mlp)]
    buffers = []
    for width, least in ((widths[1], MLP_ROWS), (widths[0], ATTN_ROWS)):
        for _, size in row_chunks(rows, least):
            buffers += scatter_buffers(rest, size, width)
    return operands, outs, buffers


def scatter_kernel(rest, layers, *refs):
    small_refs, table_refs, refs = refs[:layers], refs[layers : 2 * layers], refs[2 * layers :]
    rows_ref, columns_ref, attn_ref, mlp_ref, sum_ref, attn_out, mlp_out, *scratch = refs
    *scratch, small_at, small_in, small_u, small_z, load, send, recv = scratch
    here = Place(rest)
    copies = Copies(load, send, recv)
    scatter = Scatter(here, copies, scatter_chunks(attn_ref, mlp_ref, attn_out, mlp_out, scratch))
    scatter.load()
    here.greet()
    u, z = here.u, here.z
    to_c = [copies.remote(small_at.at[0], small_in.at[0], here.at(c=1))]
    to_x = [copies.remote(small_at.at[1], small_in.at[1], here.at(x=1))]
    to_u = [copies.remote(small_u.at[u], small_u.at[u], here.at(u=d)) for d in range(1, rest)]
    to_z = [copies.remote(small_z.at[z], small_z.at[z], here.at(z=d)) for d in range(1, LINE)]
    scatter.begin()
    for l in range(layers):
        count = small_refs[l].shape[0]
        small_at[0, l, :count] = small_refs[l][...]
        for g in range(table_refs[l].shape[0]):
            for h, table in enumerate(table_grad(table_refs[l][g], rows_ref, columns_ref)):
                row, at = count + (PER_GROUP * g + h) // 2, h % 2 * 2 * LANES
                small_at[0, l, row : row + 1, at : at + 2 * LANES] = table
    start(to_c)

    def one():
        arrive(to_c)
        small_at[1] = small_at[0] + small_in[0]
        start(to_x)

    def two():
        arrive(to_x)
        small_u[u] = small_at[1] + small_in[1]
        start(to_u)

    def three():
        arrive(to_u)
        total = small_u[0]
        for d in range(1, rest):
            total = total + small_u[d]
        small_z[z] = total
        start(to_z)

    def four():
        arrive(to_z)
        total = small_z[0]
        for d in range(1, LINE):
            total = total + small_z[d]
        sum_ref[...] = total

    little = [one, two, three, four]
    for _, event in scatter.events():
        event()
        if little:
            little.pop(0)()
    copies.drain()


def scatter_weights(smalls, tables, attn, mlp):
    rest = lax.axis_size("dp") // LINE
    operands, outs, buffers = scatter_shapes(rest, attn, mlp)
    layers, (count, width) = len(smalls), smalls[0].shape
    shape = (layers, count + tables[0].shape[0] * PER_GROUP * 2 * LANES // width, width)
    little = [pltpu.VMEM((n,) + shape, F32) for n in (2, 2, rest, LINE)]
    vmem = pl.BlockSpec(memory_space=pltpu.VMEM)
    return pl.pallas_call(
        functools.partial(scatter_kernel, rest, layers),
        in_specs=[vmem] * (2 * layers + 2) + [ANY] * 2,
        out_specs=[vmem] * 3,
        out_shape=[jax.ShapeDtypeStruct(shape, F32)] + outs,
        scratch_shapes=buffers + little + scatter_sems(len(buffers) // 7, rest, rest + LINE),
        compiler_params=pltpu.CompilerParams(collective_id=1, has_side_effects=True, vmem_limit_bytes=60000 * 1024),
        name="scatter_weights",
    )(*smalls, *tables, *spread_tables(), *operands)


class Hooks:
    def __init__(self, images, points):
        self.images, self.points, self.table = images, points, {}
        self.image = pl.program_id(0)

    def place(self, share, event):
        slot = min(int(share * self.images * self.points), self.images * self.points - 1)
        self.table.setdefault(slot, []).append(event)

    def __call__(self, point):
        for slot in sorted(self.table):
            if slot % self.points == point:

                @pl.when(self.image == slot // self.points)
                def _(slot=slot):
                    for event in self.table[slot]:
                        event()


def compact(attn_ref, wq_ref, wo_ref):
    @pl.when(pl.program_id(0) == 0)
    def _():
        for g in range(wo_ref.shape[1] // LANES):
            at = 4 * LANES * g
            wq_ref[:, BLOCK * g : BLOCK * (g + 1)] = attn_ref[:, at : at + BLOCK]
            wo_ref[:, LANES * g : LANES * (g + 1)] = attn_ref[:, at + BLOCK : at + 4 * LANES]


def gather_hooks(hook, rest, layer, shards, wholes, attn_own, mlp_own, load, send, recv):
    here = Place(rest)
    copies = Copies(load, send, recv)
    gather = Gather(here, copies, *shard_chunks(layer, *shards, attn_own, mlp_own, *wholes))
    hook.place(0, gather.fill)
    hook.place(0, here.greet)
    hook.place(0, gather.begin)
    for due, event in gather.events():
        hook.place(due / 36.0, event)
    hook.place(1, gather.finish)
    hook.place(1, copies.drain)


def load_rows(ref, rows_ref):
    if len(ref.shape) == 3:
        return ref[0].astype(F32)
    rows_ref[:TOKENS] = ref[0].astype(F32).reshape(TOKENS, -1)
    rows_ref[TOKENS:] = jnp.zeros((ROWS - TOKENS, rows_ref.shape[1]), F32)
    return rows_ref[...]


def store_rows(ref, value):
    if len(ref.shape) == 3:
        ref[0] = value
    else:
        ref[0] = value[:TOKENS].reshape(PLACES, WINDOWS, -1).astype(ref.dtype)


def forward_kernel(images, layer, last, shifted, rest, *refs):
    following = 0 if last else layer + 1
    live_ref, x_ref, attn_ref, mlp_ref, bias_ref, mask_ref, perm_ref, back_ref, *refs = refs
    qvb_ref, upb_ref, gain_ref, shift_ref, outb_ref, *refs = refs
    qvb_ref, upb_ref, bias_ref, gain_ref, shift_ref, outb_ref = (
        r.at[layer] for r in (qvb_ref, upb_ref, bias_ref, gain_ref, shift_ref, outb_ref)
    )
    shards, refs = (refs[:4], refs[4:]) if following else ((), refs)
    out_ref, xhat1_ref, inv1_ref, normed1_ref, qkv_ref, lse_ref, *refs = refs
    att_ref, xhat2_ref, inv2_ref, normed2_ref, hid_ref, slope_ref, *refs = refs
    wholes, refs = (refs[:2], refs[2:]) if following else ((), refs)
    pad_ref, wq_ref, wo_ref, rows_ref, *refs = refs
    hook = Hooks(images, 4)
    if following:
        gather_hooks(hook, rest, following, shards, wholes, *refs)
    hook(0)
    groups = wo_ref.shape[1] // LANES
    compact(attn_ref, wq_ref, wo_ref)
    x = load_rows(x_ref, rows_ref)
    xhat, inverse = normalize(x)
    xhat1_ref[0] = xhat.astype(BF16)
    inv1_ref[0] = jnp.broadcast_to(inverse, (ROWS, LANES))
    normed = (xhat * gain_ref[0:1] + shift_ref[0:1]).astype(BF16)
    normed1_ref[0] = normed
    rolled = nn(perm_ref[...], normed).astype(BF16)
    qkv_ref[0] = (nn(rolled, wq_ref[...]) + qvb_ref[...]).astype(BF16)
    hook(1)

    def attend(g, carry):
        bias = bias_ref[g]
        for w in range(WINDOWS):
            rows = slice(KEYS * w, KEYS * (w + 1))
            query = qkv_ref[0, rows, cols(BLOCK * g, LANES)]
            key = qkv_ref[0, rows, cols(BLOCK * g + LANES, LANES)]
            val = qkv_ref[0, rows, cols(BLOCK * g + 2 * LANES, LANES)]
            scores = nt(key, spread_heads(query)) * SCALE + bias
            if shifted:
                scores = scores + mask_ref[w]
            top = jnp.max(scores, axis=0, keepdims=True)
            expo = jnp.exp(scores - top)
            total = jnp.sum(expo, axis=0, keepdims=True)
            probs = (expo * (1.0 / total)).astype(BF16)
            lse_ref[0, pl.ds(WINDOWS * g + w, 1), :] = top + jnp.log(total)
            pad_ref[rows, cols(LANES * g, LANES)] = join_heads(tn(probs, val)).astype(BF16)
        return carry

    lax.fori_loop(0, groups, attend, 0)
    hook(2)
    attended = nn(back_ref[...], pad_ref[...]).astype(BF16)
    att_ref[0] = attended
    middle = x + nt(attended, wo_ref[...]) + outb_ref[0:1]
    xhat, inverse = normalize(middle)
    xhat2_ref[0] = xhat.astype(BF16)
    inv2_ref[0] = jnp.broadcast_to(inverse, (ROWS, LANES))
    normed = (xhat * gain_ref[1:2] + shift_ref[1:2]).astype(BF16)
    normed2_ref[0] = normed
    total = middle + outb_ref[1:2]
    step = mlp_ref.shape[1] // (2 * groups)
    for c in range(groups):
        at = slice(step * c, step * (c + 1))
        pre = nn(normed, mlp_ref[:, 2 * step * c : 2 * step * c + step]) + upb_ref[:, at]
        half = 0.5 + 0.5 * lax.erf(pre * 0.7071067811865476)
        hidden = (pre * half).astype(BF16)
        hid_ref[0, :, at] = hidden
        bell = jnp.exp2(pre * pre * (-0.5 * 1.4426950408889634))
        slope_ref[0, :, at] = (half + pre * 0.3989422804014327 * bell).astype(BF16)
        total = total + nt(hidden, mlp_ref[:, 2 * step * c + step : 2 * step * (c + 1)])
    if last:
        total = total * live_ref[pl.program_id(0)]
    store_rows(out_ref, total)
    hook(3)


def norm_back(grad, xhat, inverse, gain):
    scaled = grad * gain
    first = row_mean(scaled)
    second = row_mean(scaled * xhat)
    return inverse * (scaled - first - xhat * second)


def add_rows(ref, row, value):
    ref[row : row + 1, : value.shape[1]] += jnp.sum(value, axis=0, keepdims=True)


def scatter_hooks(hook, rest, matrices, outs, scratch):
    here = Place(rest)
    *buffers, load, send, recv = scratch
    copies = Copies(load, send, recv)
    scatter = Scatter(here, copies, scatter_chunks(*matrices, *outs, buffers))
    hook.place(0, scatter.load)
    hook.place(0, here.greet)
    hook.place(0, scatter.begin)
    for due, event in scatter.events():
        hook.place(due / 44.0, event)
    hook.place(1, copies.drain)


def backward_kernel(images, layer, first, shifted, following, rest, *refs):
    live_ref, g_ref, attn_ref, mlp_ref, bias_ref, mask_ref, perm_ref, back_ref, gain_ref, *refs = refs
    bias_ref, gain_ref = bias_ref.at[layer], gain_ref.at[layer]
    xhat1_ref, inv1_ref, qkv_ref, lse_ref, xhat2_ref, inv2_ref, slope_ref, *refs = refs
    normed1_ref, att_ref, normed2_ref, hid_ref, *refs = refs
    matrices, refs = (refs[:2], refs[2:]) if following else ((), refs)
    gout_ref, table_ref, small_ref, gattn_ref, gmlp_ref, *refs = refs
    outs, refs = (refs[:2], refs[2:]) if following else ((), refs)
    gap_ref, gpad_ref, wq_ref, wo_ref, gm_ref, gpre_ref, gp_ref, gqkv_ref, *refs = refs
    kept_n1, kept_att, kept_n2, kept_hid, sems, rows_ref, *refs = refs
    hook = Hooks(images, 4)
    if following:
        scatter_hooks(hook, rest, matrices, outs, refs)
    hook(0)
    groups = wo_ref.shape[1] // LANES
    image = pl.program_id(0)
    pairs = ((normed1_ref, kept_n1), (att_ref, kept_att), (normed2_ref, kept_n2), (hid_ref, kept_hid))
    loads = [pltpu.make_async_copy(src, dst, sems.at[k]) for k, (src, dst) in enumerate(pairs)]
    compact(attn_ref, wq_ref, wo_ref)

    @pl.when(image == 0)
    def _():
        table_ref[...] = jnp.zeros_like(table_ref)
        small_ref[...] = jnp.zeros_like(small_ref)
        for load in loads:
            load.start()

    g_res = load_rows(g_ref, rows_ref)
    if first:
        g_res = g_res * live_ref[image]
    add_rows(small_ref, 5, g_res)
    g_m = g_res.astype(BF16)
    gm_ref[image] = g_m
    g_n2 = jnp.zeros_like(g_res)
    step = mlp_ref.shape[1] // (2 * groups)
    for c in range(groups):
        at = slice(step * c, step * (c + 1))
        down = mlp_ref[:, 2 * step * c + step : 2 * step * (c + 1)]
        g_pre = (nn(g_m, down) * slope_ref[0, :, at].astype(F32)).astype(BF16)
        gpre_ref[image, :, at] = g_pre
        add_rows(small_ref, 6 + c, g_pre.astype(F32))
        g_n2 = g_n2 + nt(g_pre, mlp_ref[:, 2 * step * c : 2 * step * c + step])
    hook(1)
    xhat = xhat2_ref[0].astype(F32)
    add_rows(small_ref, 2, g_n2 * xhat)
    add_rows(small_ref, 3, g_n2)
    g_mid = g_res + norm_back(g_n2, xhat, inv2_ref[0, :, 0:1], gain_ref[1:2])
    add_rows(small_ref, 4, g_mid)
    g_p = g_mid.astype(BF16)
    gp_ref[image] = g_p
    g_att = nn(g_p, wo_ref[...]).astype(BF16)
    gap_ref[...] = nn(perm_ref[...], g_att).astype(BF16)

    def attend(g, carry):
        bias = bias_ref[g]
        for w in range(WINDOWS):
            rows = slice(KEYS * w, KEYS * (w + 1))
            query = spread_heads(qkv_ref[0, rows, cols(BLOCK * g, LANES)])
            key = qkv_ref[0, rows, cols(BLOCK * g + LANES, LANES)]
            val = qkv_ref[0, rows, cols(BLOCK * g + 2 * LANES, LANES)]
            grad = spread_heads(gap_ref[rows, cols(LANES * g, LANES)])
            scores = nt(key, query) * SCALE + bias
            if shifted:
                scores = scores + mask_ref[w]
            probs = jnp.exp(scores - lse_ref[0, pl.ds(WINDOWS * g + w, 1), :])
            g_probs = nt(val, grad)
            g_vals = nn(probs.astype(BF16), grad)
            mean = jnp.sum(g_probs * probs, axis=0, keepdims=True)
            g_scores = (probs * (g_probs - mean)).astype(BF16)
            table_ref[g] += g_scores.astype(F32)
            g_keys = nn(g_scores, query) * SCALE
            g_queries = join_heads(tn(g_scores, key)) * SCALE
            gpad_ref[rows, cols(BLOCK * g, LANES)] = g_queries.astype(BF16)
            gpad_ref[rows, cols(BLOCK * g + LANES, LANES)] = g_keys.astype(BF16)
            gpad_ref[rows, cols(BLOCK * g + 2 * LANES, LANES)] = g_vals.astype(BF16)
        return carry

    hook(2)
    lax.fori_loop(0, groups, attend, 0)
    hook(3)
    g_qkv = nn(back_ref[...], gpad_ref[...]).astype(BF16)
    gqkv_ref[image] = g_qkv
    for g in range(groups):
        for row, at in ((10, BLOCK * g), (11, BLOCK * g + 2 * LANES)):
            part = g_qkv[:, at : at + LANES].astype(F32)
            small_ref[row : row + 1, LANES * g : LANES * (g + 1)] += jnp.sum(part, axis=0, keepdims=True)
    g_n1 = nt(g_qkv, wq_ref[...])
    xhat = xhat1_ref[0].astype(F32)
    add_rows(small_ref, 0, g_n1 * xhat)
    add_rows(small_ref, 1, g_n1)
    store_rows(gout_ref, g_mid + norm_back(g_n1, xhat, inv1_ref[0, :, 0:1], gain_ref[0:1]))

    @pl.when(image == pl.num_programs(0) - 1)
    def _():
        for load in loads:
            load.wait()
        flat = lambda ref: ref.reshape(ref.shape[0] * ref.shape[1], ref.shape[2])

        def product(left_ref, right_ref, size, out_ref, stride, start):
            left = flat(left_ref)[...].T
            for g in range(groups):
                right = flat(right_ref)[:, size * g : size * (g + 1)]
                at = stride * g + start
                out_ref[:, at : at + size] = nn(left, right).astype(BF16)

        product(gm_ref, kept_hid, step, gmlp_ref, 2 * step, step)
        product(kept_n2, gpre_ref, step, gmlp_ref, 2 * step, 0)
        product(gp_ref, kept_att, LANES, gattn_ref, 4 * LANES, BLOCK)
        product(kept_n1, gqkv_ref, BLOCK, gattn_ref, 4 * LANES, 0)


def whole(array):
    zeros = (0,) * array.ndim
    return pl.BlockSpec(array.shape, lambda i: zeros, pipeline_mode=pl.Buffered(1))


def per_image(shape):
    tail = (0,) * (len(shape) - 1)
    return pl.BlockSpec((1,) + tuple(shape[1:]), lambda i: (i,) + tail)


def fixed(shape):
    zeros = (0,) * len(shape)
    return pl.BlockSpec(shape, lambda i: zeros)


def params(**more):
    return pltpu.CompilerParams(dimension_semantics=("arbitrary",), vmem_limit_bytes=60000 * 1024, **more)


def forward_layer(layer, layers, live, x, attn, mlp, tables, rows, shards):
    images = x.shape[0]
    width, units = attn.shape[0], mlp.shape[1] // 2
    groups = width // LANES
    total = groups * BLOCK
    last = layer == layers - 1
    shapes = [
        ((images, PLACES, WINDOWS, width), BF16) if last else ((images, ROWS, width), F32),
        ((images, ROWS, width), BF16),
        ((images, ROWS, LANES), F32),
        ((images, ROWS, width), BF16),
        ((images, PADDED, total), BF16),
        ((images, groups * WINDOWS, WIDE), F32),
        ((images, ROWS, width), BF16),
        ((images, ROWS, width), BF16),
        ((images, ROWS, LANES), F32),
        ((images, ROWS, width), BF16),
        ((images, ROWS, units), BF16),
        ((images, ROWS, units), BF16),
    ]
    fixed_args = (attn, mlp, *tables, *rows)
    rest = lax.axis_size("dp") // LINE
    extra_shapes, own, sems, more = [], [], [], {}
    if last:
        shards = ()
    else:
        extra_shapes, own = gather_shapes(rest, shards)
        sems = gather_sems(chunk_count(shards[2].shape[1]), rest)
        more = dict(collective_id=2 + layer, has_side_effects=True)
    result = pl.pallas_call(
        functools.partial(forward_kernel, images, layer, last, layer % 2 == 1, rest),
        grid=(images,),
        in_specs=[SMEM, per_image(x.shape)] + [whole(a) for a in fixed_args] + [ANY] * len(shards),
        out_specs=[per_image(s) for s, _ in shapes] + [ANY] * len(extra_shapes),
        out_shape=[jax.ShapeDtypeStruct(s, d) for s, d in shapes] + extra_shapes,
        scratch_shapes=[
            pltpu.VMEM((PADDED, width), BF16),
            pltpu.VMEM((width, total), BF16),
            pltpu.VMEM((width, width), BF16),
            pltpu.VMEM((ROWS, width), F32),
        ]
        + own
        + sems,
        compiler_params=params(**more),
        name="forward_layer",
    )(live, x, *fixed_args, *shards)
    return result[: len(shapes)], [flat_rows(m) for m in result[len(shapes) :]]


def backward_layer(layer, layers, live, g, attn, mlp, tables, gain, saved, operands, following):
    images = g.shape[0]
    width, units = attn.shape[0], mlp.shape[1] // 2
    groups = width // LANES
    total = groups * BLOCK
    sums = [((groups, KEYS, WIDE), F32), ((16, width), F32), (attn.shape, BF16), (mlp.shape, BF16)]
    fixed_args = (attn, mlp, *tables, gain)
    rest = lax.axis_size("dp") // LINE
    matrices, outs, buffers, more = [], [], [], {}
    result = (images, ROWS, width) if layer else (images, PLACES, WINDOWS, width)
    if following:
        matrices, outs, buffers = scatter_shapes(rest, *following)
        buffers = buffers + scatter_sems(len(buffers) // 7, rest)
        more = dict(collective_id=2 + layers + layer, has_side_effects=True)
    result = pl.pallas_call(
        functools.partial(
            backward_kernel, images, layer, layer == layers - 1, layer % 2 == 1, bool(following), rest
        ),
        grid=(images,),
        in_specs=[SMEM, per_image(g.shape)]
        + [whole(a) for a in fixed_args]
        + [per_image(a.shape) for a in saved]
        + [ANY] * (len(operands) + len(matrices)),
        out_specs=[per_image(result)] + [fixed(s) for s, _ in sums] + [fixed(o.shape) for o in outs],
        out_shape=[jax.ShapeDtypeStruct(result, F32)] + [jax.ShapeDtypeStruct(s, d) for s, d in sums] + outs,
        scratch_shapes=[
            pltpu.VMEM((PADDED, width), BF16),
            pltpu.VMEM((PADDED, total), BF16),
            pltpu.VMEM((width, total), BF16),
            pltpu.VMEM((width, width), BF16),
            pltpu.VMEM((images, ROWS, width), BF16),
            pltpu.VMEM((images, ROWS, units), BF16),
            pltpu.VMEM((images, ROWS, width), BF16),
            pltpu.VMEM((images, ROWS, total), BF16),
        ]
        + [pltpu.VMEM(a.shape, a.dtype) for a in operands]
        + [pltpu.SemaphoreType.DMA((len(operands),)), pltpu.VMEM((ROWS, width), F32)]
        + buffers,
        compiler_params=params(**more),
        name="backward_layer",
    )(live, g, *fixed_args, *saved, *operands, *matrices)
    return result[:5], result[5:]


def swap_windows(images):
    return jnp.transpose(images, (0, 2, 1, 3))


def local(
    activations,
    counts,
    w_qkv,
    w_out,
    w_up,
    w_down,
    qv_bias,
    rel_table,
    up_bias,
    norm_gain,
    norm_bias,
    out_bias,
    cotangent,
):
    slots, width = activations.shape[0], activations.shape[3]
    layers = w_qkv.shape[0]
    shares = lax.axis_size("seq")
    seq = lax.axis_index("seq")
    spot = seq % PLANES * 2 + seq // PLANES
    units = w_up.shape[2]
    heads = rel_table.shape[2]
    live = (seq * slots + jnp.arange(slots) < counts[0]).astype(F32)

    table = jnp.transpose(rel_table, (0, 2, 1))
    table = jnp.concatenate(
        [table[..., CENTRE:], jnp.zeros((layers, heads, GAP), F32), table[..., :CENTRE]], axis=2
    )
    pieces = [p.astype(F32).reshape(-1, LANES) for p in (qv_bias, up_bias, table)]
    shards = (
        jnp.transpose(w_qkv, (0, 2, 1, 3)),
        jnp.transpose(w_out, (0, 2, 1)),
        w_up,
        jnp.transpose(w_down, (0, 2, 1)),
    )
    qvb, upb, bias, *matrices = gather_weights(jnp.concatenate(pieces), layers, *shards)
    rows = (qvb, upb, norm_gain, norm_bias, out_bias)
    tables = []
    for layer in range(layers):
        perm, mask = place_tables(3 if layer % 2 == 1 else 0)
        mask = mask if layer % 2 == 1 else mask[:1, :8, :LANES]
        tables.append((bias, jnp.asarray(mask), jnp.asarray(perm, BF16), jnp.asarray(perm.T, BF16)))

    residual = swap_windows(activations)
    saved, weights = [], []
    for layer in range(layers):
        weights.append(matrices)
        (residual, *kept), matrices = forward_layer(
            layer, layers, live, residual, *matrices, tables[layer], rows, shards
        )
        saved.append(kept)
    out = swap_windows(residual)

    grad = swap_windows(cotangent)
    smalls, scores, grads, partial = [None] * layers, [None] * layers, [None] * layers, ()
    for layer in reversed(range(layers)):
        xhat1, inv1, normed1, qkv, lse, att, xhat2, inv2, normed2, hid, slope = saved[layer]
        (grad, scores[layer], smalls[layer], *partial), sums = backward_layer(
            layer,
            layers,
            live,
            grad,
            *weights[layer],
            tables[layer],
            norm_gain,
            (xhat1, inv1, qkv, lse, xhat2, inv2, slope),
            (normed1, att, normed2, hid),
            partial,
        )
        if layer < layers - 1:
            grads[layer + 1] = sums

    total, *grads[0] = scatter_weights(smalls, scores, *partial)
    grad_attn, grad_mlp = (jnp.stack(g) for g in zip(*grads))
    mine = lambda value, axis, size: lax.dynamic_slice_in_dim(value, spot * size, size, axis)
    grad_table = mine(total[:, 16:].reshape(layers, -1, 2 * LANES), 1, heads)[..., :TABLE]
    return (
        out,
        swap_windows(grad),
        grad_attn[..., :BLOCK].reshape(layers, -1, 3, LANES),
        jnp.transpose(grad_attn[..., BLOCK:], (0, 2, 1)),
        grad_mlp[..., :units],
        jnp.transpose(grad_mlp[..., units:], (0, 2, 1)),
        mine(total[:, 10:12], 2, LANES),
        jnp.transpose(grad_table, (0, 2, 1)),
        mine(total[:, 6:10], 1, 1)[:, 0],
        total[:, 0:3:2],
        total[:, 1:4:2],
        total[:, 4:6],
    )


def solution(mesh):
    slots = P(("dp", "seq"), None, None, None)
    return jax.shard_map(
        local,
        mesh=mesh,
        in_specs=(
            slots,
            P("dp"),
            P(None, "dp", None, "seq"),
            P(None, "seq", "dp"),
            P(None, "dp", "seq"),
            P(None, "seq", "dp"),
            P(None, None, "seq"),
            P(None, None, "seq"),
            P(None, "seq"),
            P(),
            P(),
            P(),
            slots,
        ),
        out_specs=(
            slots,
            slots,
            P(None, "dp", None, "seq"),
            P(None, "seq", "dp"),
            P(None, "dp", "seq"),
            P(None, "seq", "dp"),
            P(None, None, "seq"),
            P(None, None, "seq"),
            P(None, "seq"),
            P(),
            P(),
            P(),
        ),
        check_vma=False,
    )
```

```python
import functools

import jax
import jax.numpy as jnp
import numpy as np
from jax import lax
from jax.experimental import pallas as pl
from jax.experimental.pallas import tpu as pltpu
from jax.sharding import PartitionSpec as P

EPS = 1e-05
F32 = jnp.float32
BF16 = jnp.bfloat16
SIDE = 7
GRID = 14
PLACES = 49
WINDOWS = 4
TOKENS = PLACES * WINDOWS
ROWS = 208
KEYS = 64
PADDED = WINDOWS * KEYS
HEAD = 32
LANES = 128
PER_GROUP = LANES // HEAD
WIDE = PER_GROUP * KEYS
BLOCK = 3 * LANES
SCALE = HEAD**-0.5
TABLE = 169
CENTRE = 84
SPREAD = 88
GAP = 2 * LANES - TABLE


def place_tables(shift):
    perm = np.zeros((PADDED, ROWS), np.float32)
    region = np.zeros((WINDOWS, PLACES), np.int64)
    for w in range(WINDOWS):
        for p in range(PLACES):
            row, col = SIDE * (w // 2) + p // SIDE, SIDE * (w % 2) + p % SIDE
            band = [int(v >= 7) + int(v >= 11) for v in (row, col)]
            region[w, p] = 3 * band[0] + band[1]
            row, col = (row + shift) % GRID, (col + shift) % GRID
            source_w = 2 * (row // SIDE) + col // SIDE
            source_p = SIDE * (row % SIDE) + col % SIDE
            perm[KEYS * w + p, WINDOWS * source_p + source_w] = 1.0
    mask = np.where(region[:, :, None] == region[:, None, :], 0.0, -100.0)
    mask = np.pad(mask, ((0, 0), (0, KEYS - PLACES), (0, KEYS - PLACES))).astype(np.float32)
    return perm, np.tile(mask, (1, 1, PER_GROUP))


def spread_tables():
    rows = np.zeros((2, KEYS, SPREAD), np.float32)
    columns = np.zeros((2, LANES, LANES), np.float32)
    for p in range(PLACES):
        wide = 13 * (p // SIDE) + p % SIDE
        rows[0, p, wide] = 1.0
        rows[1, p, CENTRE - wide] = 1.0
        columns[0, wide, p] = 1.0
        columns[1, wide, KEYS + p] = 1.0
    return jnp.asarray(rows), jnp.asarray(columns)


def nn(a, b):
    return lax.dot_general(a, b, (((1,), (0,)), ((), ())), preferred_element_type=F32)


def nt(a, b):
    return lax.dot_general(a, b, (((1,), (1,)), ((), ())), preferred_element_type=F32)


def tn(a, b):
    return lax.dot_general(a, b, (((0,), (0,)), ((), ())), preferred_element_type=F32)


def exact(a, b, contract):
    return lax.dot_general(
        a, b, (contract, ((), ())), precision=lax.Precision.HIGHEST, preferred_element_type=F32
    )


def head_bias(table_row, rows_ref, columns_ref, out_ref):
    picked = []
    for h in range(PER_GROUP):
        wide = jnp.broadcast_to(table_row(h), (SPREAD, 2 * LANES))
        wide = pltpu.roll(wide, 0, 1, stride=1, stride_axis=0)[:, :LANES]
        picked.append(exact(rows_ref[0], wide, ((1,), (0,))))
    pad = lax.broadcasted_iota(jnp.int32, (KEYS, LANES), 0) >= PLACES
    for c in range(PER_GROUP // 2):
        even = exact(picked[2 * c], columns_ref[0], ((1,), (0,)))
        odd = exact(picked[2 * c + 1], columns_ref[1], ((1,), (0,)))
        out_ref[:, LANES * c : LANES * (c + 1)] = jnp.where(pad, -1e30, even + odd)


def table_grad(grads, rows_ref, columns_ref):
    tables = []
    for h in range(PER_GROUP):
        part = grads[:, LANES * (h // 2) : LANES * (h // 2 + 1)]
        wide = exact(part, columns_ref[h % 2], ((1,), (1,)))
        wide = exact(rows_ref[1], wide, ((0,), (0,)))
        wide = jnp.concatenate([wide, jnp.zeros((SPREAD, LANES), F32)], axis=1)
        wide = pltpu.roll(wide, 0, 1, stride=1, stride_axis=0)
        tables.append(jnp.sum(wide, axis=0, keepdims=True))
    return tables


def row_mean(value):
    return jnp.sum(value, axis=-1, keepdims=True) * (1.0 / value.shape[-1])


def normalize(value):
    centered = value - row_mean(value)
    inverse = lax.rsqrt(row_mean(centered * centered) + EPS)
    return centered * inverse, inverse


def spread_heads(tile):
    head = lax.broadcasted_iota(jnp.int32, tile.shape, 1) // HEAD
    zero = jnp.zeros_like(tile)
    return jnp.concatenate([jnp.where(head == h, tile, zero) for h in range(PER_GROUP)], axis=0)


def join_heads(wide):
    head = lax.broadcasted_iota(jnp.int32, (KEYS, LANES), 1) // HEAD
    total = wide[:KEYS]
    for h in range(1, PER_GROUP):
        total = jnp.where(head == h, wide[KEYS * h : KEYS * (h + 1)], total)
    return total


def cols(at, size):
    return pl.ds(pl.multiple_of(at, LANES), size)


SMEM = pl.BlockSpec(memory_space=pltpu.SMEM)
ANY = pl.BlockSpec(memory_space=pl.ANY)

MESH = pl.DeviceIdType.MESH
LINE = 4
PLANES = 2


class Place:
    def __init__(self, rest):
        dp, seq = lax.axis_index("dp"), lax.axis_index("seq")
        self.rest = rest
        self.z, self.u = dp // rest, dp % rest
        self.x, self.c = seq // PLANES, seq % PLANES

    def at(self, z=0, u=0, x=0, c=0):
        dp = (self.z + z) % LINE * self.rest + (self.u + u) % self.rest
        return (dp, (self.x + x) % 2 * PLANES + (self.c + c) % 2)

    def greet(self, *more):
        near = [self.at(z=k) for k in range(1, LINE)] + [self.at(u=k) for k in range(1, self.rest)]
        peers = near + [self.at(x=1), self.at(c=1), *more]
        barrier = pltpu.get_barrier_semaphore()
        for peer in peers:
            pl.semaphore_signal(barrier, inc=1, device_id=peer, device_id_type=MESH)
        pl.semaphore_wait(barrier, len(peers))


class Copies:
    def __init__(self, load, send, recv):
        self.load, self.send, self.recv = load, send, recv
        self.loads, self.sent = 0, []

    def local(self, src, dst):
        self.loads += 1
        return pltpu.make_async_copy(src, dst, self.load.at[self.loads - 1])

    def remote(self, src, dst, peer):
        at = len(self.sent)
        copy = pltpu.make_async_remote_copy(
            src_ref=src,
            dst_ref=dst,
            send_sem=self.send.at[at],
            recv_sem=self.recv.at[at],
            device_id=peer,
            device_id_type=MESH,
        )
        self.sent.append(copy)
        return copy

    def drain(self):
        for copy in self.sent:
            copy.wait_send()


def start(copies):
    for copy in copies:
        copy.start()


def arrive(copies):
    for copy in copies:
        copy.wait_recv()


def schedule(count, begin, steps, lag=3.0):
    free, ready, plan = {}, [(0.0, k, 0) for k in range(count)], []
    transfers = [begin, *steps]
    while ready:
        ready.sort()
        now, k, s = ready.pop(0)
        if s > 0:
            plan.append((now, s - 1, k))
        if s < len(transfers) and transfers[s]:
            link, total = transfers[s]
            free[link] = max(free.get(link, 0.0), now) + total / count
            ready.append((free[link] + lag, k, s + 1))
    return plan


def row_chunks(rows, least):
    count = max(1, rows // least)
    size = rows // count
    return [(k * size, size) for k in range(count)]


ATTN_ROWS, MLP_ROWS = 32, 16


class Gather:
    def __init__(self, here, copies, fills, chunks):
        self.copies, self.items = copies, []
        self.fills = [copies.local(a, b) for a, b in fills]
        z, u, x, c, rest = here.z, here.u, here.x, here.c, here.rest
        others = range(1, rest)
        for own, full, (at, rows) in chunks:
            width = own.shape[1]
            half = rows // 2
            first, second, both = pl.ds(at, half), pl.ds(at + half, half), pl.ds(at, rows)
            span = [pl.ds(pl.multiple_of((c * 2 + (x + d) % 2) * width, width), width) for d in range(2)]
            pair = pl.ds(pl.multiple_of(c * 2 * width, 2 * width), 2 * width)

            def send(index, **offset):
                return copies.remote(full.at[index], full.at[index], here.at(**offset))

            mine = full.at[z, u, both, span[0]]
            shard = own.at[both, :]
            item = dict(
                local=[copies.local(shard, mine)],
                line=[copies.remote(shard, mine, here.at(z=d)) for d in range(1, LINE)],
            )
            every = slice(None)
            item["a1"] = [send((every, u, first, span[0]), x=1)]
            item["b1"] = [send((every, u, second, span[0]), u=d) for d in others]
            item["d1"] = [send((every, u, both, span[0]), c=1)]
            item["a2"] = [send((every, u, first, pair), u=d) for d in others]
            item["b2"] = [send((every, every, second, span[0]), x=1)]
            item["d2"] = [send((every, u, first, span[1]), c=1)]
            item["d2"] += [send((every, (u + d) % rest, second, span[0]), c=1) for d in others]
            item["d3"] = [send((every, (u + d) % rest, first, pair), c=1) for d in others]
            item["d3"] += [send((every, every, second, span[1]), c=1)]
            self.items.append(item)

    def fill(self):
        start(self.fills)

    def begin(self):
        for copy in self.fills:
            copy.wait()
        for item in self.items:
            start(item["local"] + item["line"])

    def events(self):
        def one(item):
            item["local"][0].wait()
            arrive(item["line"])
            start(item["a1"] + item["b1"] + item["d1"])

        def two(item):
            arrive(item["a1"])
            start(item["a2"])
            arrive(item["b1"])
            start(item["b2"] + item["d2"])

        def three(item):
            arrive(item["a2"] + item["b2"])
            start(item["d3"])

        steps = (one, two, three)
        plan = schedule(len(self.items), ("z", 15.0), [("xy", 8.0), ("xy", 16.0), None])
        return [(t, functools.partial(steps[s], self.items[k])) for t, s, k in plan]

    def finish(self):
        for item in self.items:
            arrive(item["d1"] + item["d2"] + item["d3"])


def gather_sems(chunks, rest, more=0):
    count = chunks * (LINE + 4 + 4 * (rest - 1)) + more
    return [pltpu.SemaphoreType.DMA((n,)) for n in (chunks + 7, count, count)]


def shard_chunks(layer, wq_ref, wo_ref, wu_ref, wd_ref, attn_own, mlp_own, attn_ref, mlp_ref):
    units = wu_ref.shape[2]
    part = lambda ref, at, size: ref.at[:, pl.ds(at, size)]
    fills = [(wq_ref.at[layer, t], part(attn_own, LANES * t, LANES)) for t in range(3)]
    fills += [(wo_ref.at[layer], part(attn_own, BLOCK, LANES))]
    fills += [(wu_ref.at[layer], part(mlp_own, 0, units)), (wd_ref.at[layer], part(mlp_own, units, units))]
    rows = attn_own.shape[0]
    chunks = [(attn_own, attn_ref, r) for r in row_chunks(rows, ATTN_ROWS)]
    chunks += [(mlp_own, mlp_ref, r) for r in row_chunks(rows, MLP_ROWS)]
    return fills, chunks


def chunk_count(rows):
    return len(row_chunks(rows, ATTN_ROWS)) + len(row_chunks(rows, MLP_ROWS))


def gather_kernel(rest, layers, *refs):
    small_ref, rows_ref, columns_ref, wq_ref, wo_ref, wu_ref, wd_ref, *refs = refs
    qvb_ref, upb_ref, bias_ref, attn_ref, mlp_ref, *refs = refs
    all_ref, attn_own, mlp_own, load, send, recv = refs
    here = Place(rest)
    copies = Copies(load, send, recv)
    chunks = shard_chunks(0, wq_ref, wo_ref, wu_ref, wd_ref, attn_own, mlp_own, attn_ref, mlp_ref)
    gather = Gather(here, copies, *chunks)
    gather.fill()
    across = here.at(x=1, c=1)
    here.greet(across)
    spot = here.x * PLANES + here.c
    small = [copies.remote(small_ref, all_ref.at[spot], peer) for peer in (here.at(c=1), here.at(x=1), across)]
    keep = copies.local(small_ref, all_ref.at[spot])
    start(small + [keep])
    gather.begin()
    groups = all_ref.shape[0]
    units = upb_ref.shape[2] // groups

    def biases():
        arrive(small)
        keep.wait()
        qvb_ref[...] = jnp.zeros_like(qvb_ref)
        for l in range(layers):
            for g in range(groups):
                seq = PLANES * (g % 2) + g // 2
                at = BLOCK * g
                qvb_ref[l, :, at : at + LANES] = all_ref[seq, 2 * l : 2 * l + 1]
                qvb_ref[l, :, at + 2 * LANES : at + BLOCK] = all_ref[seq, 2 * l + 1 : 2 * l + 2]
                for i in range(units // LANES):
                    row = 2 * layers + units // LANES * l + i
                    at = units * g + LANES * i
                    upb_ref[l, :, at : at + LANES] = all_ref[seq, row : row + 1]

    def group_bias(l, g):
        seq = PLANES * (g % 2) + g // 2

        def table_row(h):
            row = (2 + units // LANES) * layers + 2 * (PER_GROUP * l + h)
            return jnp.concatenate([all_ref[seq, row : row + 1], all_ref[seq, row + 1 : row + 2]], axis=1)

        head_bias(table_row, rows_ref, columns_ref, bias_ref.at[l, g])

    beside = [biases] + [functools.partial(group_bias, l, g) for l in range(layers) for g in range(groups)]
    for _, event in gather.events():
        event()
        if beside:
            beside.pop(0)()
    for step in beside:
        step()
    gather.finish()
    copies.drain()


def gather_shapes(rest, shards):
    rows, units = shards[2].shape[1:]
    shares = lax.axis_size("seq")
    widths = (4 * LANES, 2 * units)
    whole_shapes = [jax.ShapeDtypeStruct((LINE, rest, rows, shares * w), BF16) for w in widths]
    return whole_shapes, [pltpu.VMEM((rows, w), BF16) for w in widths]


def flat_rows(matrix):
    return matrix.reshape(-1, matrix.shape[-1])


def gather_weights(small, layers, *shards):
    rest = lax.axis_size("dp") // LINE
    groups = lax.axis_size("seq")
    whole_shapes, own = gather_shapes(rest, shards)
    units = shards[2].shape[2]
    rows, columns = spread_tables()
    tables = [(layers, 1, groups * BLOCK), (layers, 1, groups * units), (layers, groups, KEYS, WIDE)]
    vmem = pl.BlockSpec(memory_space=pltpu.VMEM)
    *tables, attn, mlp = pl.pallas_call(
        functools.partial(gather_kernel, rest, layers),
        in_specs=[ANY, vmem, vmem] + [ANY] * 4,
        out_specs=[vmem] * 3 + [ANY] * 2,
        out_shape=[jax.ShapeDtypeStruct(t, F32) for t in tables] + whole_shapes,
        scratch_shapes=[pltpu.VMEM((groups,) + small.shape, F32)]
        + own
        + gather_sems(chunk_count(shards[2].shape[1]), rest, 3),
        compiler_params=pltpu.CompilerParams(collective_id=0, has_side_effects=True),
        name="gather_weights",
    )(small, rows, columns, *shards)
    return *tables, flat_rows(attn), flat_rows(mlp)


def each(count, body):
    def step(i, carry):
        body(i)
        return carry

    lax.fori_loop(0, count, step, 0)


def plus(ref, at, *others):
    total = ref[at].astype(F32)
    for other in others:
        total = total + other.astype(F32)
    ref[at] = total.astype(BF16)


class Scatter:
    def __init__(self, here, copies, chunks):
        self.here, self.copies, self.items = here, copies, []
        z, u, x, c, rest = here.z, here.u, here.x, here.c, here.rest
        others = range(1, rest)
        for full, out, (at, rows), (acc, swap, x1, u1, x2, u2, line) in chunks:
            width = out.shape[1]
            half = rows // 2
            first, second, both = pl.ds(0, half), pl.ds(half, half), pl.ds(0, rows)
            whole_rows = pl.ds(at, rows)
            pair = [pl.ds(pl.multiple_of((c + d) % 2 * 2 * width, 2 * width), 2 * width) for d in range(2)]
            span = [pl.ds(pl.multiple_of((x + d) % 2 * width, width), width) for d in range(2)]
            every = slice(None)
            item = dict(out=out, rows=whole_rows, acc=acc, swap=swap, x1=x1, u1=u1, x2=x2, u2=u2, line=line)
            item.update(first=first, second=second, both=both, mine=span[0])
            item["own"] = copies.local(full.at[:, :, whole_rows, pair[0]], acc)
            item["to_c"] = [copies.remote(full.at[:, :, whole_rows, pair[1]], swap, here.at(c=1))]
            item["to_1"] = [copies.remote(acc.at[:, :, first, span[1]], x1, here.at(x=1))]
            for d in others:
                there = (u + d) % rest
                item["to_1"].append(copies.remote(acc.at[:, there, second, :], u1.at[d - 1], here.at(u=d)))
            item["to_2"] = [copies.remote(acc.at[:, u, second, span[1]], x2, here.at(x=1))]
            for d in others:
                there = (u + d) % rest
                item["to_2"].append(copies.remote(acc.at[:, there, first, span[0]], u2.at[d - 1], here.at(u=d)))
            item["to_z"] = [
                copies.remote(acc.at[(z + d) % LINE, u, both, span[0]], line.at[d - 1], here.at(z=d))
                for d in range(1, LINE)
            ]
            self.items.append(item)

    def load(self):
        for item in self.items:
            item["own"].start()

    def begin(self):
        for item in self.items:
            start(item["to_c"])

    def events(self):
        z, u, rest = self.here.z, self.here.u, self.here.rest
        others = range(1, rest)

        def one(item):
            item["own"].wait()
            arrive(item["to_c"])

            def add(i):
                a, b = i // rest, i % rest
                plus(item["acc"], (a, b), item["swap"][a, b])

            each(LINE * rest, add)
            start(item["to_1"])

        def two(item):
            arrive(item["to_1"])
            first, second, mine = item["first"], item["second"], item["mine"]

            def add(i):
                a, b = i // rest, i % rest
                plus(item["acc"], (a, b, first, mine), item["x1"][a, b])

            each(LINE * rest, add)

            def add_u(a):
                plus(item["acc"], (a, u, second), *(item["u1"][d - 1, a] for d in others))

            each(LINE, add_u)
            start(item["to_2"])

        def three(item):
            arrive(item["to_2"])
            first, second, mine = item["first"], item["second"], item["mine"]

            def add(a):
                plus(item["acc"], (a, u, second, mine), item["x2"][a])
                plus(item["acc"], (a, u, first, mine), *(item["u2"][d - 1, a] for d in others))

            each(LINE, add)
            start(item["to_z"])

        def four(item):
            arrive(item["to_z"])
            total = item["acc"][z, u, item["both"], item["mine"]].astype(F32)
            for d in range(1, LINE):
                total = total + item["line"][d - 1].astype(F32)
            item["out"][item["rows"], :] = total

        steps = (one, two, three, four)
        plan = schedule(len(self.items), ("c", 5.0), [("xy", 16.0), ("xy", 8.0), ("z", 15.0), None])
        return [(t, functools.partial(steps[s], self.items[k])) for t, s, k in plan]


def scatter_sems(chunks, rest, more=0):
    count = chunks * (LINE + 2 + 2 * (rest - 1)) + more
    return [pltpu.SemaphoreType.DMA((n,)) for n in (chunks + 1, count, count)]


def scatter_buffers(rest, rows, width):
    half = rows // 2
    shapes = (
        (LINE, rest, rows, 2 * width),
        (LINE, rest, rows, 2 * width),
        (LINE, rest, half, width),
        (rest - 1, LINE, half, 2 * width),
        (LINE, half, width),
        (rest - 1, LINE, half, width),
        (LINE - 1, rows, width),
    )
    return [pltpu.VMEM(s, BF16) for s in shapes]


def scatter_chunks(attn_ref, mlp_ref, attn_out, mlp_out, scratch):
    chunks, at = [], 0
    for matrix, out, least in ((mlp_ref, mlp_out, MLP_ROWS), (attn_ref, attn_out, ATTN_ROWS)):
        for rows in row_chunks(out.shape[0], least):
            chunks.append((matrix, out, rows, scratch[at : at + 7]))
            at += 7
    return chunks


def scatter_shapes(rest, attn, mlp):
    shares = lax.axis_size("seq")
    rows = attn.shape[0] // (LINE * rest)
    widths = [m.shape[1] // shares for m in (attn, mlp)]
    outs = [jax.ShapeDtypeStruct((rows, w), F32) for w in widths]
    operands = [m.reshape(LINE, rest, rows, -1) for m in (attn, mlp)]
    buffers = []
    for width, least in ((widths[1], MLP_ROWS), (widths[0], ATTN_ROWS)):
        for _, size in row_chunks(rows, least):
            buffers += scatter_buffers(rest, size, width)
    return operands, outs, buffers


def scatter_kernel(rest, layers, *refs):
    small_refs, table_refs, refs = refs[:layers], refs[layers : 2 * layers], refs[2 * layers :]
    rows_ref, columns_ref, attn_ref, mlp_ref, sum_ref, attn_out, mlp_out, *scratch = refs
    *scratch, small_at, small_in, small_u, small_z, load, send, recv = scratch
    here = Place(rest)
    copies = Copies(load, send, recv)
    scatter = Scatter(here, copies, scatter_chunks(attn_ref, mlp_ref, attn_out, mlp_out, scratch))
    scatter.load()
    here.greet()
    u, z = here.u, here.z
    to_c = [copies.remote(small_at.at[0], small_in.at[0], here.at(c=1))]
    to_x = [copies.remote(small_at.at[1], small_in.at[1], here.at(x=1))]
    to_u = [copies.remote(small_u.at[u], small_u.at[u], here.at(u=d)) for d in range(1, rest)]
    to_z = [copies.remote(small_z.at[z], small_z.at[z], here.at(z=d)) for d in range(1, LINE)]
    scatter.begin()
    for l in range(layers):
        count = small_refs[l].shape[0]
        small_at[0, l, :count] = small_refs[l][...]
        for g in range(table_refs[l].shape[0]):
            for h, table in enumerate(table_grad(table_refs[l][g], rows_ref, columns_ref)):
                row, at = count + (PER_GROUP * g + h) // 2, h % 2 * 2 * LANES
                small_at[0, l, row : row + 1, at : at + 2 * LANES] = table
    start(to_c)

    def one():
        arrive(to_c)
        small_at[1] = small_at[0] + small_in[0]
        start(to_x)

    def two():
        arrive(to_x)
        small_u[u] = small_at[1] + small_in[1]
        start(to_u)

    def three():
        arrive(to_u)
        total = small_u[0]
        for d in range(1, rest):
            total = total + small_u[d]
        small_z[z] = total
        start(to_z)

    def four():
        arrive(to_z)
        total = small_z[0]
        for d in range(1, LINE):
            total = total + small_z[d]
        sum_ref[...] = total

    little = [one, two, three, four]
    for _, event in scatter.events():
        event()
        if little:
            little.pop(0)()
    copies.drain()


def scatter_weights(smalls, tables, attn, mlp):
    rest = lax.axis_size("dp") // LINE
    operands, outs, buffers = scatter_shapes(rest, attn, mlp)
    layers, (count, width) = len(smalls), smalls[0].shape
    shape = (layers, count + tables[0].shape[0] * PER_GROUP * 2 * LANES // width, width)
    little = [pltpu.VMEM((n,) + shape, F32) for n in (2, 2, rest, LINE)]
    vmem = pl.BlockSpec(memory_space=pltpu.VMEM)
    return pl.pallas_call(
        functools.partial(scatter_kernel, rest, layers),
        in_specs=[vmem] * (2 * layers + 2) + [ANY] * 2,
        out_specs=[vmem] * 3,
        out_shape=[jax.ShapeDtypeStruct(shape, F32)] + outs,
        scratch_shapes=buffers + little + scatter_sems(len(buffers) // 7, rest, rest + LINE),
        compiler_params=pltpu.CompilerParams(collective_id=1, has_side_effects=True, vmem_limit_bytes=60000 * 1024),
        name="scatter_weights",
    )(*smalls, *tables, *spread_tables(), *operands)


class Hooks:
    def __init__(self, images, points, tail=0):
        self.images, self.points, self.table = images, points, {}
        self.image = pl.program_id(0)
        self.slots = images * points + tail

    def place(self, share, event):
        slot = min(int(share * self.slots), self.slots - 1)
        self.table.setdefault(slot, []).append(event)

    def after(self, point):
        for event in self.table.get(self.images * self.points + point, []):
            event()

    def __call__(self, point):
        for slot in sorted(self.table):
            if slot < self.images * self.points and slot % self.points == point:

                @pl.when(self.image == slot // self.points)
                def _(slot=slot):
                    for event in self.table[slot]:
                        event()


def compact(attn_ref, wq_ref, wo_ref):
    @pl.when(pl.program_id(0) == 0)
    def _():
        for g in range(wo_ref.shape[1] // LANES):
            at = 4 * LANES * g
            wq_ref[:, BLOCK * g : BLOCK * (g + 1)] = attn_ref[:, at : at + BLOCK]
            wo_ref[:, LANES * g : LANES * (g + 1)] = attn_ref[:, at + BLOCK : at + 4 * LANES]


def gather_hooks(hook, rest, layer, shards, wholes, attn_own, mlp_own, load, send, recv):
    here = Place(rest)
    copies = Copies(load, send, recv)
    gather = Gather(here, copies, *shard_chunks(layer, *shards, attn_own, mlp_own, *wholes))
    hook.place(0, gather.fill)
    hook.place(0, here.greet)
    hook.place(0, gather.begin)
    for due, event in gather.events():
        hook.place(due / 36.0, event)
    hook.place(1, gather.finish)
    hook.place(1, copies.drain)


def load_rows(ref, rows_ref):
    if len(ref.shape) == 3:
        return ref[0].astype(F32)
    rows_ref[:TOKENS] = ref[0].astype(F32).reshape(TOKENS, -1)
    rows_ref[TOKENS:] = jnp.zeros((ROWS - TOKENS, rows_ref.shape[1]), F32)
    return rows_ref[...]


def store_rows(ref, value):
    if len(ref.shape) == 3:
        ref[0] = value
    else:
        ref[0] = value[:TOKENS].reshape(PLACES, WINDOWS, -1).astype(ref.dtype)


def forward_kernel(images, layer, last, shifted, rest, *refs):
    following = 0 if last else layer + 1
    live_ref, x_ref, attn_ref, mlp_ref, bias_ref, mask_ref, perm_ref, back_ref, *refs = refs
    qvb_ref, upb_ref, gain_ref, shift_ref, outb_ref, *refs = refs
    qvb_ref, upb_ref, bias_ref, gain_ref, shift_ref, outb_ref = (
        r.at[layer] for r in (qvb_ref, upb_ref, bias_ref, gain_ref, shift_ref, outb_ref)
    )
    shards, refs = (refs[:4], refs[4:]) if following else ((), refs)
    out_ref, xhat1_ref, inv1_ref, normed1_ref, qkv_ref, lse_ref, *refs = refs
    att_ref, xhat2_ref, inv2_ref, normed2_ref, hid_ref, slope_ref, *refs = refs
    wholes, refs = (refs[:2], refs[2:]) if following else ((), refs)
    pad_ref, wq_ref, wo_ref, rows_ref, *refs = refs
    hook = Hooks(images, 4)
    if following:
        gather_hooks(hook, rest, following, shards, wholes, *refs)
    hook(0)
    groups = wo_ref.shape[1] // LANES
    compact(attn_ref, wq_ref, wo_ref)
    x = load_rows(x_ref, rows_ref)
    xhat, inverse = normalize(x)
    xhat1_ref[0] = xhat.astype(BF16)
    inv1_ref[0] = jnp.broadcast_to(inverse, (ROWS, LANES))
    normed = (xhat * gain_ref[0:1] + shift_ref[0:1]).astype(BF16)
    normed1_ref[0] = normed
    rolled = nn(perm_ref[...], normed).astype(BF16)
    qkv_ref[0] = (nn(rolled, wq_ref[...]) + qvb_ref[...]).astype(BF16)
    hook(1)

    def attend(g, carry):
        bias = bias_ref[g]
        for w in range(WINDOWS):
            rows = slice(KEYS * w, KEYS * (w + 1))
            query = qkv_ref[0, rows, cols(BLOCK * g, LANES)]
            key = qkv_ref[0, rows, cols(BLOCK * g + LANES, LANES)]
            val = qkv_ref[0, rows, cols(BLOCK * g + 2 * LANES, LANES)]
            scores = nt(key, spread_heads(query)) * SCALE + bias
            if shifted:
                scores = scores + mask_ref[w]
            top = jnp.max(scores, axis=0, keepdims=True)
            expo = jnp.exp(scores - top)
            total = jnp.sum(expo, axis=0, keepdims=True)
            probs = (expo * (1.0 / total)).astype(BF16)
            lse_ref[0, pl.ds(WINDOWS * g + w, 1), :] = top + jnp.log(total)
            pad_ref[rows, cols(LANES * g, LANES)] = join_heads(tn(probs, val)).astype(BF16)
        return carry

    lax.fori_loop(0, groups, attend, 0, unroll=4)
    hook(2)
    attended = nn(back_ref[...], pad_ref[...]).astype(BF16)
    att_ref[0] = attended
    middle = x + nt(attended, wo_ref[...]) + outb_ref[0:1]
    xhat, inverse = normalize(middle)
    xhat2_ref[0] = xhat.astype(BF16)
    inv2_ref[0] = jnp.broadcast_to(inverse, (ROWS, LANES))
    normed = (xhat * gain_ref[1:2] + shift_ref[1:2]).astype(BF16)
    normed2_ref[0] = normed
    total = middle + outb_ref[1:2]
    step = mlp_ref.shape[1] // (2 * groups)
    for c in range(groups):
        at = slice(step * c, step * (c + 1))
        pre = nn(normed, mlp_ref[:, 2 * step * c : 2 * step * c + step]) + upb_ref[:, at]
        half = 0.5 + 0.5 * lax.erf(pre * 0.7071067811865476)
        hidden = (pre * half).astype(BF16)
        hid_ref[0, :, at] = hidden
        bell = jnp.exp2(pre * pre * (-0.5 * 1.4426950408889634))
        slope_ref[0, :, at] = (half + pre * 0.3989422804014327 * bell).astype(BF16)
        total = total + nt(hidden, mlp_ref[:, 2 * step * c + step : 2 * step * (c + 1)])
    if last:
        total = total * live_ref[pl.program_id(0)]
    store_rows(out_ref, total)
    hook(3)


def norm_back(grad, xhat, inverse, gain):
    scaled = grad * gain
    first = row_mean(scaled)
    second = row_mean(scaled * xhat)
    return inverse * (scaled - first - xhat * second)


def add_rows(ref, row, value):
    ref[row : row + 1, : value.shape[1]] += jnp.sum(value, axis=0, keepdims=True)


def scatter_hooks(hook, rest, matrices, outs, scratch):
    here = Place(rest)
    *buffers, load, send, recv = scratch
    copies = Copies(load, send, recv)
    scatter = Scatter(here, copies, scatter_chunks(*matrices, *outs, buffers))
    hook.place(0, scatter.load)
    hook.place(0, here.greet)
    hook.place(0, scatter.begin)
    for due, event in scatter.events():
        hook.place(due * 1.2 / 55.0, event)
    hook.place(1, copies.drain)


def backward_kernel(images, layer, first, shifted, following, rest, *refs):
    live_ref, g_ref, attn_ref, mlp_ref, bias_ref, mask_ref, perm_ref, back_ref, gain_ref, *refs = refs
    bias_ref, gain_ref = bias_ref.at[layer], gain_ref.at[layer]
    xhat1_ref, inv1_ref, qkv_ref, lse_ref, xhat2_ref, inv2_ref, slope_ref, *refs = refs
    normed1_ref, att_ref, normed2_ref, hid_ref, *refs = refs
    matrices, refs = (refs[:2], refs[2:]) if following else ((), refs)
    gout_ref, table_ref, small_ref, gattn_ref, gmlp_ref, *refs = refs
    outs, refs = (refs[:2], refs[2:]) if following else ((), refs)
    gap_ref, gpad_ref, wq_ref, wo_ref, gm_ref, gpre_ref, gp_ref, gqkv_ref, *refs = refs
    kept_n1, kept_att, kept_n2, kept_hid, sems, rows_ref, *refs = refs
    hook = Hooks(images, 4, 4)
    if following:
        scatter_hooks(hook, rest, matrices, outs, refs)
    hook(0)
    groups = wo_ref.shape[1] // LANES
    image = pl.program_id(0)
    pairs = ((normed1_ref, kept_n1), (att_ref, kept_att), (normed2_ref, kept_n2), (hid_ref, kept_hid))
    loads = [pltpu.make_async_copy(src, dst, sems.at[k]) for k, (src, dst) in enumerate(pairs)]
    compact(attn_ref, wq_ref, wo_ref)

    @pl.when(image == 0)
    def _():
        table_ref[...] = jnp.zeros_like(table_ref)
        small_ref[...] = jnp.zeros_like(small_ref)
        for load in loads:
            load.start()

    g_res = load_rows(g_ref, rows_ref)
    if first:
        g_res = g_res * live_ref[image]
    add_rows(small_ref, 5, g_res)
    g_m = g_res.astype(BF16)
    gm_ref[image] = g_m
    g_n2 = jnp.zeros_like(g_res)
    step = mlp_ref.shape[1] // (2 * groups)
    for c in range(groups):
        at = slice(step * c, step * (c + 1))
        down = mlp_ref[:, 2 * step * c + step : 2 * step * (c + 1)]
        g_pre = (nn(g_m, down) * slope_ref[0, :, at].astype(F32)).astype(BF16)
        gpre_ref[image, :, at] = g_pre
        add_rows(small_ref, 6 + c, g_pre.astype(F32))
        g_n2 = g_n2 + nt(g_pre, mlp_ref[:, 2 * step * c : 2 * step * c + step])
    hook(1)
    xhat = xhat2_ref[0].astype(F32)
    add_rows(small_ref, 2, g_n2 * xhat)
    add_rows(small_ref, 3, g_n2)
    g_mid = g_res + norm_back(g_n2, xhat, inv2_ref[0, :, 0:1], gain_ref[1:2])
    add_rows(small_ref, 4, g_mid)
    g_p = g_mid.astype(BF16)
    gp_ref[image] = g_p
    g_att = nn(g_p, wo_ref[...]).astype(BF16)
    gap_ref[...] = nn(perm_ref[...], g_att).astype(BF16)

    def attend(g, carry):
        bias = bias_ref[g]
        for w in range(WINDOWS):
            rows = slice(KEYS * w, KEYS * (w + 1))
            query = spread_heads(qkv_ref[0, rows, cols(BLOCK * g, LANES)])
            key = qkv_ref[0, rows, cols(BLOCK * g + LANES, LANES)]
            val = qkv_ref[0, rows, cols(BLOCK * g + 2 * LANES, LANES)]
            grad = spread_heads(gap_ref[rows, cols(LANES * g, LANES)])
            scores = nt(key, query) * SCALE + bias
            if shifted:
                scores = scores + mask_ref[w]
            probs = jnp.exp(scores - lse_ref[0, pl.ds(WINDOWS * g + w, 1), :])
            g_probs = nt(val, grad)
            g_vals = nn(probs.astype(BF16), grad)
            mean = jnp.sum(g_probs * probs, axis=0, keepdims=True)
            g_scores = (probs * (g_probs - mean)).astype(BF16)
            table_ref[g] += g_scores.astype(F32)
            g_keys = nn(g_scores, query) * SCALE
            g_queries = join_heads(tn(g_scores, key)) * SCALE
            gpad_ref[rows, cols(BLOCK * g, LANES)] = g_queries.astype(BF16)
            gpad_ref[rows, cols(BLOCK * g + LANES, LANES)] = g_keys.astype(BF16)
            gpad_ref[rows, cols(BLOCK * g + 2 * LANES, LANES)] = g_vals.astype(BF16)
        return carry

    hook(2)
    lax.fori_loop(0, groups, attend, 0, unroll=4)
    hook(3)
    g_qkv = nn(back_ref[...], gpad_ref[...]).astype(BF16)
    gqkv_ref[image] = g_qkv
    for g in range(groups):
        for row, at in ((10, BLOCK * g), (11, BLOCK * g + 2 * LANES)):
            part = g_qkv[:, at : at + LANES].astype(F32)
            small_ref[row : row + 1, LANES * g : LANES * (g + 1)] += jnp.sum(part, axis=0, keepdims=True)
    g_n1 = nt(g_qkv, wq_ref[...])
    xhat = xhat1_ref[0].astype(F32)
    add_rows(small_ref, 0, g_n1 * xhat)
    add_rows(small_ref, 1, g_n1)
    store_rows(gout_ref, g_mid + norm_back(g_n1, xhat, inv1_ref[0, :, 0:1], gain_ref[0:1]))

    @pl.when(image == pl.num_programs(0) - 1)
    def _():
        for load in loads:
            load.wait()
        flat = lambda ref: ref.reshape(ref.shape[0] * ref.shape[1], ref.shape[2])

        def product(left_ref, right_ref, size, out_ref, stride, start):
            left = flat(left_ref)[...].T
            for g in range(groups):
                right = flat(right_ref)[:, size * g : size * (g + 1)]
                at = stride * g + start
                out_ref[:, at : at + size] = nn(left, right).astype(BF16)

        product(gm_ref, kept_hid, step, gmlp_ref, 2 * step, step)
        hook.after(0)
        product(kept_n2, gpre_ref, step, gmlp_ref, 2 * step, 0)
        hook.after(1)
        product(gp_ref, kept_att, LANES, gattn_ref, 4 * LANES, BLOCK)
        hook.after(2)
        product(kept_n1, gqkv_ref, BLOCK, gattn_ref, 4 * LANES, 0)
        hook.after(3)


def whole(array):
    zeros = (0,) * array.ndim
    return pl.BlockSpec(array.shape, lambda i: zeros, pipeline_mode=pl.Buffered(1))


def per_image(shape):
    tail = (0,) * (len(shape) - 1)
    return pl.BlockSpec((1,) + tuple(shape[1:]), lambda i: (i,) + tail)


def fixed(shape):
    zeros = (0,) * len(shape)
    return pl.BlockSpec(shape, lambda i: zeros)


def params(**more):
    return pltpu.CompilerParams(dimension_semantics=("arbitrary",), vmem_limit_bytes=60000 * 1024, **more)


def forward_layer(layer, layers, live, x, attn, mlp, tables, rows, shards):
    images = x.shape[0]
    width, units = attn.shape[0], mlp.shape[1] // 2
    groups = width // LANES
    total = groups * BLOCK
    last = layer == layers - 1
    shapes = [
        ((images, PLACES, WINDOWS, width), BF16) if last else ((images, ROWS, width), F32),
        ((images, ROWS, width), BF16),
        ((images, ROWS, LANES), F32),
        ((images, ROWS, width), BF16),
        ((images, PADDED, total), BF16),
        ((images, groups * WINDOWS, WIDE), F32),
        ((images, ROWS, width), BF16),
        ((images, ROWS, width), BF16),
        ((images, ROWS, LANES), F32),
        ((images, ROWS, width), BF16),
        ((images, ROWS, units), BF16),
        ((images, ROWS, units), BF16),
    ]
    fixed_args = (attn, mlp, *tables, *rows)
    rest = lax.axis_size("dp") // LINE
    extra_shapes, own, sems, more = [], [], [], {}
    if last:
        shards = ()
    else:
        extra_shapes, own = gather_shapes(rest, shards)
        sems = gather_sems(chunk_count(shards[2].shape[1]), rest)
        more = dict(collective_id=2 + layer, has_side_effects=True)
    result = pl.pallas_call(
        functools.partial(forward_kernel, images, layer, last, layer % 2 == 1, rest),
        grid=(images,),
        in_specs=[SMEM, per_image(x.shape)] + [whole(a) for a in fixed_args] + [ANY] * len(shards),
        out_specs=[per_image(s) for s, _ in shapes] + [ANY] * len(extra_shapes),
        out_shape=[jax.ShapeDtypeStruct(s, d) for s, d in shapes] + extra_shapes,
        scratch_shapes=[
            pltpu.VMEM((PADDED, width), BF16),
            pltpu.VMEM((width, total), BF16),
            pltpu.VMEM((width, width), BF16),
            pltpu.VMEM((ROWS, width), F32),
        ]
        + own
        + sems,
        compiler_params=params(**more),
        name="forward_layer",
    )(live, x, *fixed_args, *shards)
    return result[: len(shapes)], [flat_rows(m) for m in result[len(shapes) :]]


def backward_layer(layer, layers, live, g, attn, mlp, tables, gain, saved, operands, following):
    images = g.shape[0]
    width, units = attn.shape[0], mlp.shape[1] // 2
    groups = width // LANES
    total = groups * BLOCK
    sums = [((groups, KEYS, WIDE), F32), ((16, width), F32), (attn.shape, BF16), (mlp.shape, BF16)]
    fixed_args = (attn, mlp, *tables, gain)
    rest = lax.axis_size("dp") // LINE
    matrices, outs, buffers, more = [], [], [], {}
    result = (images, ROWS, width) if layer else (images, PLACES, WINDOWS, width)
    if following:
        matrices, outs, buffers = scatter_shapes(rest, *following)
        buffers = buffers + scatter_sems(len(buffers) // 7, rest)
        more = dict(collective_id=2 + layers + layer, has_side_effects=True)
    result = pl.pallas_call(
        functools.partial(
            backward_kernel, images, layer, layer == layers - 1, layer % 2 == 1, bool(following), rest
        ),
        grid=(images,),
        in_specs=[SMEM, per_image(g.shape)]
        + [whole(a) for a in fixed_args]
        + [per_image(a.shape) for a in saved]
        + [ANY] * (len(operands) + len(matrices)),
        out_specs=[per_image(result)] + [fixed(s) for s, _ in sums] + [fixed(o.shape) for o in outs],
        out_shape=[jax.ShapeDtypeStruct(result, F32)] + [jax.ShapeDtypeStruct(s, d) for s, d in sums] + outs,
        scratch_shapes=[
            pltpu.VMEM((PADDED, width), BF16),
            pltpu.VMEM((PADDED, total), BF16),
            pltpu.VMEM((width, total), BF16),
            pltpu.VMEM((width, width), BF16),
            pltpu.VMEM((images, ROWS, width), BF16),
            pltpu.VMEM((images, ROWS, units), BF16),
            pltpu.VMEM((images, ROWS, width), BF16),
            pltpu.VMEM((images, ROWS, total), BF16),
        ]
        + [pltpu.VMEM(a.shape, a.dtype) for a in operands]
        + [pltpu.SemaphoreType.DMA((len(operands),)), pltpu.VMEM((ROWS, width), F32)]
        + buffers,
        compiler_params=params(**more),
        name="backward_layer",
    )(live, g, *fixed_args, *saved, *operands, *matrices)
    return result[:5], result[5:]


def swap_windows(images):
    return jnp.transpose(images, (0, 2, 1, 3))


def local(
    activations,
    counts,
    w_qkv,
    w_out,
    w_up,
    w_down,
    qv_bias,
    rel_table,
    up_bias,
    norm_gain,
    norm_bias,
    out_bias,
    cotangent,
):
    slots, width = activations.shape[0], activations.shape[3]
    layers = w_qkv.shape[0]
    shares = lax.axis_size("seq")
    seq = lax.axis_index("seq")
    spot = seq % PLANES * 2 + seq // PLANES
    units = w_up.shape[2]
    heads = rel_table.shape[2]
    live = (seq * slots + jnp.arange(slots) < counts[0]).astype(F32)

    table = jnp.transpose(rel_table, (0, 2, 1))
    table = jnp.concatenate(
        [table[..., CENTRE:], jnp.zeros((layers, heads, GAP), F32), table[..., :CENTRE]], axis=2
    )
    pieces = [p.astype(F32).reshape(-1, LANES) for p in (qv_bias, up_bias, table)]
    shards = (
        jnp.transpose(w_qkv, (0, 2, 1, 3)),
        jnp.transpose(w_out, (0, 2, 1)),
        w_up,
        jnp.transpose(w_down, (0, 2, 1)),
    )
    qvb, upb, bias, *matrices = gather_weights(jnp.concatenate(pieces), layers, *shards)
    rows = (qvb, upb, norm_gain, norm_bias, out_bias)
    tables = []
    for layer in range(layers):
        perm, mask = place_tables(3 if layer % 2 == 1 else 0)
        mask = mask if layer % 2 == 1 else mask[:1, :8, :LANES]
        tables.append((bias, jnp.asarray(mask), jnp.asarray(perm, BF16), jnp.asarray(perm.T, BF16)))

    residual = swap_windows(activations)
    saved, weights = [], []
    for layer in range(layers):
        weights.append(matrices)
        (residual, *kept), matrices = forward_layer(
            layer, layers, live, residual, *matrices, tables[layer], rows, shards
        )
        saved.append(kept)
    out = swap_windows(residual)

    grad = swap_windows(cotangent)
    smalls, scores, grads, partial = [None] * layers, [None] * layers, [None] * layers, ()
    for layer in reversed(range(layers)):
        xhat1, inv1, normed1, qkv, lse, att, xhat2, inv2, normed2, hid, slope = saved[layer]
        (grad, scores[layer], smalls[layer], *partial), sums = backward_layer(
            layer,
            layers,
            live,
            grad,
            *weights[layer],
            tables[layer],
            norm_gain,
            (xhat1, inv1, qkv, lse, xhat2, inv2, slope),
            (normed1, att, normed2, hid),
            partial,
        )
        if layer < layers - 1:
            grads[layer + 1] = sums

    total, *grads[0] = scatter_weights(smalls, scores, *partial)
    grad_attn, grad_mlp = (jnp.stack(g) for g in zip(*grads))
    mine = lambda value, axis, size: lax.dynamic_slice_in_dim(value, spot * size, size, axis)
    grad_table = mine(total[:, 16:].reshape(layers, -1, 2 * LANES), 1, heads)[..., :TABLE]
    return (
        out,
        swap_windows(grad),
        grad_attn[..., :BLOCK].reshape(layers, -1, 3, LANES),
        jnp.transpose(grad_attn[..., BLOCK:], (0, 2, 1)),
        grad_mlp[..., :units],
        jnp.transpose(grad_mlp[..., units:], (0, 2, 1)),
        mine(total[:, 10:12], 2, LANES),
        jnp.transpose(grad_table, (0, 2, 1)),
        mine(total[:, 6:10], 1, 1)[:, 0],
        total[:, 0:3:2],
        total[:, 1:4:2],
        total[:, 4:6],
    )


def solution(mesh):
    slots = P(("dp", "seq"), None, None, None)
    return jax.shard_map(
        local,
        mesh=mesh,
        in_specs=(
            slots,
            P("dp"),
            P(None, "dp", None, "seq"),
            P(None, "seq", "dp"),
            P(None, "dp", "seq"),
            P(None, "seq", "dp"),
            P(None, None, "seq"),
            P(None, None, "seq"),
            P(None, "seq"),
            P(),
            P(),
            P(),
            slots,
        ),
        out_specs=(
            slots,
            slots,
            P(None, "dp", None, "seq"),
            P(None, "seq", "dp"),
            P(None, "dp", "seq"),
            P(None, "seq", "dp"),
            P(None, None, "seq"),
            P(None, None, "seq"),
            P(None, "seq"),
            P(),
            P(),
            P(),
        ),
        check_vma=False,
    )
```
